32 devices in a mesh: sec: 4 (over y, core), op: 8 (over z, x).
Axes of the slice: x: 2, y: 2, z: 4, core: 2. Of those that a mesh axis runs over, the one named last changes fastest.
Arguments:
- wavefunction: bfloat16 [4, 512, 1024], P('sec', 'op'), may hold values from -4.5 to 4.5
- op_blocks: bfloat16 [8, 4, 1024, 1024], P('op', 'sec'), may hold values from -6 to 6
- basis_guess: bfloat16 [4, 1024, 512], P('sec'), may hold values from -4.5 to 4.5
- sector_sizes: int32 [4], replicated, may hold values from 768 to 1024
- kept_counts: int32 [4], replicated, may hold values from 256 to 512
- target_map: int32 [8, 4], replicated, may hold values from 0 to 3, as said below
- noise_numerator: int32 [1], replicated, may hold values from 256 to 1024
- noise_denominator: int32 [1], replicated, may hold values from 4194304 to 8388608
Outputs:
- kept_basis: float32 [4, 1024, 512], P('sec', 'op')
- rotated: float32 [8, 4, 512, 512], P('op', 'sec')
The draws below stay inside these ranges and needn't reach their ends.
Inputs may be any that keep to these rules, and one draw needn't show every extreme that they name: For every operator k, target_map[k] is a permutation of the 4 sectors.
All inputs are finite; a program needn't handle non-finite values.
Results may differ from the reference program's by a relative error of at most 0.005.
Values may be sent and summed in bfloat16 or wider, within the bound.
A program may use at most 64 MiB of HBM per device.

```python
import jax
import jax.numpy as jnp
from jax import lax

DIM = 1024
KEEP = 512
COLS = 512
SECTORS = 4
OPS = 8


def draw_target_map(key, part):
    operator_keys = jax.random.split(jax.random.fold_in(key, 17), OPS)
    orders = jax.vmap(lambda operator_key: jax.random.permutation(operator_key, SECTORS))(operator_keys)
    return orders.astype(jnp.int32)


def rough_rows(key, shape):
    values = jax.random.normal(jax.random.fold_in(key, 3), shape, jnp.float32)
    return jnp.clip(values, -4.5, 4.5)


def draw_wavefunction(key, part):
    return rough_rows(jax.random.fold_in(key, 29), (SECTORS, COLS, DIM)).astype(jnp.bfloat16)


def draw_basis_guess(key, part):
    return rough_rows(jax.random.fold_in(key, 31), (SECTORS, DIM, KEEP)).astype(jnp.bfloat16)


def set_ends(result, stream_key, least, high):
    spot = [jax.random.randint(jax.random.fold_in(stream_key, axis), (), 0, length) for axis, length in enumerate(result.shape)]
    widest = result.shape.index(max(result.shape))
    beside = spot[:widest] + [(spot[widest] + 1) % result.shape[widest]] + spot[widest + 1:]
    return result.at[tuple(spot)].set(least).at[tuple(beside)].set(high)


def block_levels(own_key, extent, pieces, smallest, top_value):
    loudness = 1.0
    for dim, parts in pieces:
        steps = jax.random.uniform(jax.random.fold_in(jax.random.fold_in(own_key, 6), dim), (parts,), jnp.float32, smallest / len(pieces), top_value / len(pieces))
        loudness = loudness * jnp.repeat(jnp.exp(steps), extent[dim] // parts).reshape((-1,) + (1,) * (len(extent) - 1 - dim))
    return loudness


def normal_values(own_key, dims, spread, bound, pieces=(), kind=jnp.bfloat16):
    values = spread * jax.random.normal(own_key, dims, jnp.float32)
    if pieces:
        values = values * block_levels(own_key, dims, pieces, -0.22, 0.18)
    return jnp.clip(values, -bound, bound).astype(kind)


def setup_inputs(seed: int = 0) -> dict:
    splits = jax.random.split(jax.random.key(seed), 9)
    return {
        "wavefunction": draw_wavefunction(jax.random.fold_in(splits[8], 71), 0),
        "op_blocks": normal_values(splits[1], (OPS, SECTORS, DIM, DIM), 1.0, 6.0, ((0, 8), (1, 4))),
        "basis_guess": draw_basis_guess(jax.random.fold_in(splits[8], 71), 0),
        "sector_sizes": set_ends(jax.random.randint(splits[3], (SECTORS,), 3 * DIM // 4, DIM + 1), jax.random.fold_in(splits[3], 1), 3 * DIM // 4, DIM).astype(jnp.int32),
        "kept_counts": set_ends(jax.random.randint(splits[4], (SECTORS,), KEEP // 2, KEEP + 1), jax.random.fold_in(splits[4], 1), KEEP // 2, KEEP).astype(jnp.int32),
        "target_map": draw_target_map(jax.random.fold_in(splits[8], 71), 0),
        "noise_numerator": jax.random.randint(splits[6], (1,), 256, 1025).astype(jnp.int32),
        "noise_denominator": jax.random.randint(splits[7], (1,), 4096 * DIM, 8192 * DIM + 1).astype(jnp.int32),
    }


def source_sectors(target_map):
    sectors = jnp.arange(SECTORS, dtype=jnp.int32)
    matches = target_map[:, :, None] == sectors[None, None, :]
    return jnp.sum(jnp.where(matches, sectors[None, :, None], 0), axis=1).astype(jnp.int32)

def reference(wavefunction, op_blocks, basis_guess, sector_sizes, kept_counts, target_map, noise_numerator, noise_denominator):
    highest = lax.Precision.HIGHEST
    noise_weight = noise_numerator[0].astype(jnp.float32) / noise_denominator[0].astype(jnp.float32)
    sources = source_sectors(target_map)
    states = jnp.arange(DIM, dtype=jnp.int32)
    state_mask = states[None, :] < sector_sizes[:, None]
    kept_mask = jnp.arange(KEEP, dtype=jnp.int32)[None, :] < kept_counts[:, None]
    masked = jnp.where(state_mask[:, None, :], wavefunction, jnp.zeros((), wavefunction.dtype))
    masked_wide = masked.astype(jnp.float32)
    base = jnp.einsum('scx,scy->sxy', masked_wide, masked_wide, precision=highest)

    def add_operator(running, inputs):
        blocks, anchor = inputs
        moved = jnp.take(masked_wide, anchor, axis=0)
        perturbed = jnp.einsum('tcx,txy->tcy', moved, blocks.astype(jnp.float32), precision=highest)
        perturbed = lax.optimization_barrier(perturbed.astype(jnp.bfloat16)).astype(jnp.float32)
        return (running + jnp.einsum('tcx,tcy->txy', perturbed, perturbed, precision=highest), None)
    noise_sum, unused = lax.scan(add_operator, jnp.zeros_like(base), (op_blocks, sources))
    density = base + noise_weight * noise_sum
    guess_masked = jnp.where(state_mask[:, :, None], basis_guess, jnp.zeros((), basis_guess.dtype)).astype(jnp.float32)
    image = jnp.einsum('sxy,syk->sxk', density, guess_masked, precision=highest)
    image = jnp.where(state_mask[:, :, None] & kept_mask[:, None, :], image, jnp.float32(0.0))
    padding = jnp.where(kept_mask, jnp.float32(0.0), jnp.float32(1.0))
    correlation = jnp.einsum('sdk,sdm->skm', image, image, precision=highest) + padding[:, :, None] * jnp.eye(KEEP, dtype=jnp.float32)[None]
    factor = jnp.linalg.cholesky(correlation)
    new_basis = lax.linalg.triangular_solve(factor, image, left_side=False, lower=True, transpose_a=True)
    kept_basis = new_basis * DIM ** 0.5
    basis_wide = lax.optimization_barrier(new_basis.astype(jnp.bfloat16)).astype(jnp.float32)

    def rotate(inputs):
        blocks, anchor = inputs
        mapped = jnp.einsum('txy,tyk->txk', blocks.astype(jnp.float32), basis_wide, precision=highest)
        mapped = lax.optimization_barrier(mapped.astype(jnp.bfloat16)).astype(jnp.float32)
        return jnp.einsum('txk,txm->tkm', jnp.take(basis_wide, anchor, axis=0), mapped, precision=highest)
    rotated = lax.map(rotate, (op_blocks, sources))
    return (kept_basis, rotated)
```

```python
import jax
import jax.numpy as jnp
from jax import lax
from jax.experimental import pallas as pl
from jax.experimental.pallas import tpu as pltpu
from jax.sharding import PartitionSpec as P

LANES = 128
ROWS = 8
HIGHEST = lax.Precision.HIGHEST


def dot_ta(a, b):
    return lax.dot_general(
        a, b, (((0,), (0,)), ((), ())), precision=HIGHEST, preferred_element_type=jnp.float32
    )


def dot(a, b):
    return jnp.dot(a, b, precision=HIGHEST, preferred_element_type=jnp.float32)


def eliminate_tile(tile):
    count = LANES // ROWS
    row = lax.broadcasted_iota(jnp.int32, (ROWS, LANES), 0)
    lane = lax.broadcasted_iota(jnp.int32, (ROWS, LANES), 1)
    left = [tile[ROWS * q : ROWS * (q + 1), :] for q in range(count)]
    right = [jnp.where(lane == row + ROWS * q, 1.0, 0.0).astype(jnp.float32) for q in range(count)]
    for p in range(count):
        upper, lower = left[p], right[p]
        columns = [
            jnp.broadcast_to(upper[:, ROWS * p + j : ROWS * p + j + 1], (ROWS, LANES))
            for j in range(ROWS)
        ]
        for j in range(ROWS):
            scale = lax.rsqrt(jnp.broadcast_to(columns[j][j : j + 1, :], (ROWS, LANES)))
            factor = jnp.where(row > j, columns[j] * scale, 0.0)
            for k in range(j + 1, ROWS):
                own = jnp.broadcast_to(columns[k][j : j + 1, :], (ROWS, LANES)) * scale
                columns[k] = columns[k] - factor * own
            own_upper = jnp.broadcast_to(upper[j : j + 1, :], (ROWS, LANES)) * scale
            own_lower = jnp.broadcast_to(lower[j : j + 1, :], (ROWS, LANES)) * scale
            upper = jnp.where(row == j, own_upper, upper - factor * own_upper)
            lower = jnp.where(row == j, own_lower, lower - factor * own_lower)
        right[p] = lower
        if p + 1 < count:
            change = dot_ta(upper, jnp.concatenate([upper, lower], axis=1))
            for q in range(p + 1, count):
                part = change[ROWS * q : ROWS * (q + 1), :]
                left[q] = left[q] - part[:, :LANES]
                right[q] = right[q] - part[:, LANES:]
    return jnp.concatenate(right, axis=0)


def inverse_factor_kernel(matrix_ref, out_ref, work):
    size = matrix_ref.shape[0]
    blocks = size // LANES
    work[:, :size] = matrix_ref[...]
    work[:, size:] = (
        lax.broadcasted_iota(jnp.int32, (size, size), 0)
        == lax.broadcasted_iota(jnp.int32, (size, size), 1)
    ).astype(jnp.float32)

    def step(b, carry):
        rows = pl.ds(pl.multiple_of(b * LANES, LANES), LANES)
        inverse = eliminate_tile(work[rows, rows])
        panel = dot(inverse, work[rows, :])
        work[rows, :] = panel
        out_ref[rows, :] = panel[:, size:]

        def update(i, inner):
            below = pl.ds(pl.multiple_of(i * LANES, LANES), LANES)
            work[below, :] = work[below, :] - dot_ta(work[rows, below], work[rows, :])
            return inner

        lax.fori_loop(b + 1, blocks, update, 0)
        return carry

    lax.fori_loop(0, blocks, step, 0)


def inverse_factor(matrix):
    size = matrix.shape[0]
    return pl.pallas_call(
        inverse_factor_kernel,
        out_shape=jax.ShapeDtypeStruct((size, size), jnp.float32),
        in_specs=[pl.BlockSpec(memory_space=pltpu.VMEM)],
        out_specs=pl.BlockSpec(memory_space=pltpu.VMEM),
        scratch_shapes=[pltpu.VMEM((size, 2 * size), jnp.float32)],
        compiler_params=pltpu.CompilerParams(vmem_limit_bytes=24 * 1024 * 1024),
        cost_estimate=pl.CostEstimate(flops=2 * size**3, bytes_accessed=8 * size * size, transcendentals=size),
        name="inverse_factor",
    )(matrix)


def source_sectors(target_map):
    sectors = jnp.arange(target_map.shape[1], dtype=jnp.int32)
    matches = target_map[:, :, None] == sectors[None, None, :]
    return jnp.sum(jnp.where(matches, sectors[None, :, None], 0), axis=1)


def fetch_pieces(own_slice, wanted_all):
    everyone = lax.all_gather(own_slice, "sec", axis=0, tiled=True)
    outgoing = jnp.take(everyone, wanted_all, axis=0)
    incoming = lax.all_to_all(outgoing, "op", split_axis=1, concat_axis=1, tiled=True)
    return incoming.reshape(
        incoming.shape[0], incoming.shape[1] * incoming.shape[2], incoming.shape[3]
    )


def exchange(value, axis, bit):
    count = lax.axis_size(axis)
    return lax.ppermute(value, axis, [(i, i ^ bit) for i in range(count)])


def halves(value, side):
    half = value.shape[0] // 2
    kept = lax.dynamic_slice_in_dim(value, side * half, half, 0)
    given = lax.dynamic_slice_in_dim(value, (1 - side) * half, half, 0)
    return kept, given


def sum_over_op(value):
    count = lax.axis_size("op")
    index = lax.axis_index("op")
    bits = [1 << b for b in range(count.bit_length() - 1)]
    orders = [bits, bits[1:] + bits[:1]]
    half = value.shape[0] // 2
    held = [value[:half], value[half:]]
    for step in range(len(bits)):
        for color, order in enumerate(orders):
            kept, given = halves(held[color], (index // order[step]) % 2)
            held[color] = kept + exchange(given, "op", order[step])
    for step in reversed(range(len(bits))):
        for color, order in enumerate(orders):
            own = held[color]
            other = exchange(own, "op", order[step])
            first = (index // order[step]) % 2 == 0
            held[color] = jnp.concatenate(
                [jnp.where(first, own, other), jnp.where(first, other, own)], axis=0
            )
    return jnp.concatenate(held, axis=0)


def fetch_sector(own, wanted):
    count = lax.axis_size("sec")
    offset = lax.axis_index("sec") ^ wanted
    held = {0: own}
    bit = count // 2
    while bit:
        for known in list(held):
            held[known ^ bit] = exchange(held[known], "sec", bit)
        bit //= 2
    result = own
    for known, value in held.items():
        result = jnp.where(offset == known, value, result)
    return result


MESH = pl.DeviceIdType.MESH
DEPTH = 4
PAIRS = 6
CROSSED = 4
FLOWS = 2 * PAIRS


def quantize(value):
    top = jnp.maximum(jnp.max(jnp.abs(value), axis=0, keepdims=True), jnp.float32(1e-30))
    levels = jnp.round(value * (jnp.float32(32766.0) / top))
    return levels.astype(jnp.int32).astype(jnp.int16), top * jnp.float32(1.0 / 32766.0)


def sum_kernel(part_ref, out_ref, *refs):
    rows, cols = part_ref.shape
    chunk = rows // 16
    names = ("give", "take", "own", "inner", "final", "cross", "last")
    levels = dict(zip(names, refs[0:7]))
    scales = dict(zip(names, refs[7:14]))
    arrivals = dict(zip(("take", "inner", "final", "cross", "last"), refs[14:19]))
    departures = dict(zip(("give", "own", "outward", "across", "last"), refs[19:24]))
    total_ref = refs[24]
    sec = lax.axis_index("sec")
    op = lax.axis_index("op")
    z, x = op // 2, op % 2
    mid = z % 3 != 0
    w = (z + 1) // 3
    side = (sec, z * 2 + 1 - x)
    other = (sec, (3 - z) * 2 + x)
    outer = (sec, 6 * w + x)
    inward = (sec, (1 + w) * 2 + x)

    barrier = pltpu.get_barrier_semaphore()

    def greet(device):
        pl.semaphore_signal(barrier, inc=1, device_id=device, device_id_type=MESH)

    greet(side)

    @pl.when(mid)
    def _():
        greet(other)
        greet(outer)
        pl.semaphore_wait(barrier, 3)

    @pl.when(jnp.logical_not(mid))
    def _():
        greet(inward)
        pl.semaphore_wait(barrier, 2)

    def message(source, i, target, j, departure, k, device):
        return [
            pltpu.make_async_remote_copy(
                src_ref=bufs[source].at[i],
                dst_ref=bufs[target].at[j],
                send_sem=departures[departure].at[k, n],
                recv_sem=arrivals[target].at[j, n],
                device_id=device,
                device_id_type=MESH,
            )
            for n, bufs in enumerate((levels, scales))
        ]

    def start(*args):
        for copy in message(*args):
            copy.start()

    def sent(*args):
        for copy in message(*args):
            copy.wait_send()

    def arrived(target, j):
        for copy in message(target, j, target, j, "give", 0, side):
            copy.wait_recv()

    def put(name, i, value):
        whole, scale = quantize(value)
        levels[name][i] = whole
        scales[name][i] = scale

    def get(name, i):
        return levels[name][i].astype(jnp.int32).astype(jnp.float32) * scales[name][i]

    def rows_of(p, e):
        first = (8 + 4 * e + p) if p < CROSSED else (4 * x + 2 * e + p - CROSSED)
        return pl.ds(pl.multiple_of(first * chunk, chunk), chunk)

    def halves_of(p, e):
        return pl.ds(pl.multiple_of((2 * e + p - CROSSED) * chunk, chunk), chunk)

    def value(p, e):
        if p < CROSSED:
            return part_ref[rows_of(p, e), :]
        return total_ref[halves_of(p, e), :]

    def give(j):
        put("give", j, part_ref[pl.ds(pl.multiple_of((4 * (1 - x) + j) * chunk, chunk), chunk), :])
        start("give", j, "take", j, "give", j, side)

    def gather(j):
        arrived("take", j)
        mine = part_ref[pl.ds(pl.multiple_of((4 * x + j) * chunk, chunk), chunk), :]
        total_ref[pl.ds(j * chunk, chunk), :] = mine + get("take", j)

    def finish(p, e):
        out_ref[rows_of(p, e), :] = get("final", 2 * p + e)
        if p >= CROSSED:
            slot = 2 * (p - CROSSED) + e
            start("final", 2 * p + e, "last", slot, "last", slot, side)

    @pl.when(jnp.logical_not(mid))
    def _():
        def send(p, e):
            i = 2 * p + e
            put("own", i, value(p, e))
            far = w if e == 0 else 1 - w
            start("own", i, "inner", FLOWS * far + i, "own", i, inward)

        for p in range(CROSSED):
            send(p, 0)
            send(p, 1)
            give(p)
        for j in range(4):
            gather(j)
        for p in range(CROSSED, PAIRS):
            send(p, 0)
            send(p, 1)
        for p in range(PAIRS):
            for e in range(2):
                arrived("final", 2 * p + e)
                finish(p, e)
        for i in range(FLOWS):
            sent("own", i, "inner", i, "own", i, inward)

    @pl.when(mid)
    def _():
        def relay(p):
            i = 2 * p + 1 - w
            arrived("inner", FLOWS + i)
            put("own", i, value(p, 1 - w) + get("inner", FLOWS + i))
            start("own", i, "inner", FLOWS + i, "own", i, other)

        def collect(p):
            i = 2 * p + w
            arrived("inner", i)
            near = value(p, w) + get("inner", i)
            arrived("inner", FLOWS + i)
            near = near + get("inner", FLOWS + i)
            if p < CROSSED:
                put("own", i, near)
                start("own", i, "cross", p, "own", i, side)
            else:
                put("final", i, near)
                spread(p)

        def spread(p):
            i = 2 * p + w
            start("final", i, "final", i, "outward", i, outer)
            start("final", i, "final", i, "across", p, other)
            finish(p, w)

        def merge(p):
            i = 2 * p + w
            arrived("cross", p)
            put("final", i, get("own", i) + get("cross", p))
            spread(p)

        def forward(p):
            i = 2 * p + 1 - w
            arrived("final", i)
            start("final", i, "final", i, "outward", i, outer)
            finish(p, 1 - w)

        for j in range(4):
            give(j)
        for p in range(PAIRS + 2):
            if p < PAIRS:
                relay(p)
                collect(p)
            if 1 <= p <= CROSSED:
                merge(p - 1)
            if p == 1:
                for j in range(4):
                    gather(j)
            if p >= 2:
                forward(p - 2)
        for p in range(PAIRS):
            i = 2 * p + 1 - w
            sent("own", i, "inner", i, "own", i, other)
            if p < CROSSED:
                sent("own", 2 * p + w, "cross", p, "own", 2 * p + w, side)
            for e in range(2):
                sent("final", 2 * p + e, "final", 2 * p + e, "outward", 2 * p + e, outer)
            sent("final", 2 * p + w, "final", 2 * p + w, "across", p, other)

    for j in range(4):
        sent("give", j, "take", j, "give", j, side)
    for p in range(CROSSED, PAIRS):
        for e in range(2):
            slot = 2 * (p - CROSSED) + e
            arrived("last", slot)
            first = 4 * (1 - x) + 2 * e + p - CROSSED
            out_ref[pl.ds(pl.multiple_of(first * chunk, chunk), chunk), :] = get("last", slot)
            sent("final", 2 * p + e, "last", slot, "last", slot, side)


def sum_over_op_kernel(part):
    rows, cols = part.shape
    chunk = rows // 16
    counts = (4, 4, FLOWS, 2 * FLOWS, FLOWS, CROSSED, 4)
    sem = pltpu.SemaphoreType.DMA
    return pl.pallas_call(
        sum_kernel,
        out_shape=jax.ShapeDtypeStruct((rows, cols), jnp.float32),
        in_specs=[pl.BlockSpec(memory_space=pltpu.VMEM)],
        out_specs=pl.BlockSpec(memory_space=pltpu.VMEM),
        scratch_shapes=[pltpu.VMEM((n, chunk, cols), jnp.int16) for n in counts]
        + [pltpu.VMEM((n, 1, cols), jnp.float32) for n in counts]
        + [sem((n, 2)) for n in (4, 2 * FLOWS, FLOWS, CROSSED, 4)]
        + [sem((n, 2)) for n in (4, FLOWS, FLOWS, PAIRS, 4)]
        + [pltpu.VMEM((4 * chunk, cols), jnp.float32)],
        compiler_params=pltpu.CompilerParams(collective_id=1, has_side_effects=True),
        name="sum_over_op",
    )(part)


def body(
    wavefunction,
    op_blocks,
    basis_guess,
    sector_sizes,
    kept_counts,
    target_map,
    noise_numerator,
    noise_denominator,
):
    state_count = wavefunction.shape[2]
    kept_width = basis_guess.shape[2]
    tile_rows = state_count // lax.axis_size("op")
    sec_index = lax.axis_index("sec")
    op_index = lax.axis_index("op")
    noise_weight = noise_numerator[0].astype(jnp.float32) / noise_denominator[0].astype(jnp.float32)
    sources = source_sectors(target_map)
    wanted_all = lax.dynamic_index_in_dim(sources, sec_index, 1, keepdims=False)[None, :]
    wanted = lax.dynamic_index_in_dim(wanted_all[0], op_index, 0, keepdims=False)
    states = jnp.arange(state_count, dtype=jnp.int32)
    own_size = lax.dynamic_index_in_dim(sector_sizes, sec_index, 0, keepdims=False)
    source_size = lax.dynamic_index_in_dim(sector_sizes, wanted, 0, keepdims=False)
    own_count = lax.dynamic_index_in_dim(kept_counts, sec_index, 0, keepdims=False)
    own_kept = jnp.arange(kept_width, dtype=jnp.int32) < own_count
    zero_half = jnp.zeros((), jnp.bfloat16)
    own_rows = jnp.where((states < own_size)[None, :], wavefunction[0], zero_half)
    moved = fetch_pieces(wavefunction, wanted_all)[0]
    moved = jnp.where((states < source_size)[None, :], moved, zero_half)
    blocks = op_blocks[0, 0]
    perturbed = jnp.dot(moved, blocks, preferred_element_type=jnp.float32).astype(jnp.bfloat16)
    guess = jnp.where((states < own_size)[:, None], basis_guess[0], zero_half)
    perturbed_guess = noise_weight * jnp.dot(perturbed, guess, preferred_element_type=jnp.float32)
    own_guess = jnp.dot(own_rows, guess, preferred_element_type=jnp.float32)
    part = lax.dot_general(
        jnp.concatenate([perturbed, own_rows], axis=0).astype(jnp.float32),
        jnp.concatenate([perturbed_guess, own_guess], axis=0),
        (((0,), (0,)), ((), ())),
        precision=lax.Precision.HIGH,
    )
    part = jnp.where((states < own_size)[:, None] & own_kept[None, :], part, jnp.float32(0.0))
    if lax.axis_size("op") == 2 * DEPTH and lax.axis_size("sec") == 4:
        full_image = sum_over_op_kernel(part)
    else:
        full_image = sum_over_op(part)
    padding = jnp.where(own_kept, jnp.float32(0.0), jnp.float32(1.0))
    correlation = dot_ta(full_image, full_image) + padding[:, None] * jnp.eye(
        kept_width, dtype=jnp.float32
    )
    inverse = inverse_factor(correlation)
    new_basis = lax.dot_general(
        full_image, inverse, (((1,), (1,)), ((), ())), precision=lax.Precision.HIGH
    )
    kept_tile = (
        lax.dynamic_slice_in_dim(new_basis, op_index * tile_rows, tile_rows, 0)
        * float(state_count) ** 0.5
    )
    basis_half = new_basis.astype(jnp.bfloat16)
    mapped = jnp.dot(blocks, basis_half, preferred_element_type=jnp.float32).astype(jnp.bfloat16)
    source_basis = fetch_sector(basis_half, wanted)
    rotated = lax.dot_general(
        source_basis, mapped, (((0,), (0,)), ((), ())), preferred_element_type=jnp.float32
    )
    return (kept_tile[None], rotated[None, None])


def solution(mesh):
    placed = (
        P("sec", "op", None),
        P("op", "sec", None, None),
        P("sec", None, None),
        P(),
        P(),
        P(),
        P(),
        P(),
    )
    return jax.shard_map(
        body,
        mesh=mesh,
        in_specs=placed,
        out_specs=(P("sec", "op", None), P("op", "sec", None, None)),
        check_vma=False,
    )
```

```python
import jax
import jax.numpy as jnp
from jax import lax
from jax.experimental import pallas as pl
from jax.experimental.pallas import tpu as pltpu
from jax.sharding import PartitionSpec as P

LANES = 128
ROWS = 8
HIGHEST = lax.Precision.HIGHEST


def dot_ta(a, b):
    return lax.dot_general(
        a, b, (((0,), (0,)), ((), ())), precision=HIGHEST, preferred_element_type=jnp.float32
    )


def dot(a, b):
    return jnp.dot(a, b, precision=HIGHEST, preferred_element_type=jnp.float32)


def eliminate_tile(tile):
    count = LANES // ROWS
    row = lax.broadcasted_iota(jnp.int32, (ROWS, LANES), 0)
    lane = lax.broadcasted_iota(jnp.int32, (ROWS, LANES), 1)
    left = [tile[ROWS * q : ROWS * (q + 1), :] for q in range(count)]
    right = [jnp.where(lane == row + ROWS * q, 1.0, 0.0).astype(jnp.float32) for q in range(count)]
    for p in range(count):
        upper, lower = left[p], right[p]
        columns = [
            jnp.broadcast_to(upper[:, ROWS * p + j : ROWS * p + j + 1], (ROWS, LANES))
            for j in range(ROWS)
        ]
        for j in range(ROWS):
            scale = lax.rsqrt(jnp.broadcast_to(columns[j][j : j + 1, :], (ROWS, LANES)))
            factor = jnp.where(row > j, columns[j] * scale, 0.0)
            for k in range(j + 1, ROWS):
                own = jnp.broadcast_to(columns[k][j : j + 1, :], (ROWS, LANES)) * scale
                columns[k] = columns[k] - factor * own
            own_upper = jnp.broadcast_to(upper[j : j + 1, :], (ROWS, LANES)) * scale
            own_lower = jnp.broadcast_to(lower[j : j + 1, :], (ROWS, LANES)) * scale
            upper = jnp.where(row == j, own_upper, upper - factor * own_upper)
            lower = jnp.where(row == j, own_lower, lower - factor * own_lower)
        right[p] = lower
        if p + 1 < count:
            change = dot_ta(upper, jnp.concatenate([upper, lower], axis=1))
            for q in range(p + 1, count):
                part = change[ROWS * q : ROWS * (q + 1), :]
                left[q] = left[q] - part[:, :LANES]
                right[q] = right[q] - part[:, LANES:]
    return jnp.concatenate(right, axis=0)


def inverse_factor_kernel(matrix_ref, out_ref, work):
    size = matrix_ref.shape[0]
    blocks = size // LANES
    work[:, :size] = matrix_ref[...]
    work[:, size:] = (
        lax.broadcasted_iota(jnp.int32, (size, size), 0)
        == lax.broadcasted_iota(jnp.int32, (size, size), 1)
    ).astype(jnp.float32)

    def step(b, carry):
        rows = pl.ds(pl.multiple_of(b * LANES, LANES), LANES)
        inverse = eliminate_tile(work[rows, rows])
        panel = dot(inverse, work[rows, :])
        work[rows, :] = panel
        out_ref[rows, :] = panel[:, size:]

        def update(i, inner):
            below = pl.ds(pl.multiple_of(i * LANES, LANES), LANES)
            work[below, :] = work[below, :] - dot_ta(work[rows, below], work[rows, :])
            return inner

        lax.fori_loop(b + 1, blocks, update, 0)
        return carry

    lax.fori_loop(0, blocks, step, 0)


def inverse_factor(matrix):
    size = matrix.shape[0]
    return pl.pallas_call(
        inverse_factor_kernel,
        out_shape=jax.ShapeDtypeStruct((size, size), jnp.float32),
        in_specs=[pl.BlockSpec(memory_space=pltpu.VMEM)],
        out_specs=pl.BlockSpec(memory_space=pltpu.VMEM),
        scratch_shapes=[pltpu.VMEM((size, 2 * size), jnp.float32)],
        compiler_params=pltpu.CompilerParams(vmem_limit_bytes=24 * 1024 * 1024),
        cost_estimate=pl.CostEstimate(flops=2 * size**3, bytes_accessed=8 * size * size, transcendentals=size),
        name="inverse_factor",
    )(matrix)


def source_sectors(target_map):
    sectors = jnp.arange(target_map.shape[1], dtype=jnp.int32)
    matches = target_map[:, :, None] == sectors[None, None, :]
    return jnp.sum(jnp.where(matches, sectors[None, :, None], 0), axis=1)


def fetch_pieces(own_slice, wanted_all):
    everyone = lax.all_gather(own_slice, "sec", axis=0, tiled=True)
    outgoing = jnp.take(everyone, wanted_all, axis=0)
    incoming = lax.all_to_all(outgoing, "op", split_axis=1, concat_axis=1, tiled=True)
    return incoming.reshape(
        incoming.shape[0], incoming.shape[1] * incoming.shape[2], incoming.shape[3]
    )


def exchange(value, axis, bit):
    count = lax.axis_size(axis)
    return lax.ppermute(value, axis, [(i, i ^ bit) for i in range(count)])


def halves(value, side):
    half = value.shape[0] // 2
    kept = lax.dynamic_slice_in_dim(value, side * half, half, 0)
    given = lax.dynamic_slice_in_dim(value, (1 - side) * half, half, 0)
    return kept, given


def sum_over_op(value):
    count = lax.axis_size("op")
    index = lax.axis_index("op")
    bits = [1 << b for b in range(count.bit_length() - 1)]
    orders = [bits, bits[1:] + bits[:1]]
    half = value.shape[0] // 2
    held = [value[:half], value[half:]]
    for step in range(len(bits)):
        for color, order in enumerate(orders):
            kept, given = halves(held[color], (index // order[step]) % 2)
            held[color] = kept + exchange(given, "op", order[step])
    for step in reversed(range(len(bits))):
        for color, order in enumerate(orders):
            own = held[color]
            other = exchange(own, "op", order[step])
            first = (index // order[step]) % 2 == 0
            held[color] = jnp.concatenate(
                [jnp.where(first, own, other), jnp.where(first, other, own)], axis=0
            )
    return jnp.concatenate(held, axis=0)


def fetch_sector(own, wanted):
    count = lax.axis_size("sec")
    offset = lax.axis_index("sec") ^ wanted
    held = {0: own}
    bit = count // 2
    while bit:
        for known in list(held):
            held[known ^ bit] = exchange(held[known], "sec", bit)
        bit //= 2
    result = own
    for known, value in held.items():
        result = jnp.where(offset == known, value, result)
    return result


MESH = pl.DeviceIdType.MESH
DEPTH = 4
PAIRS = 6
CROSSED = 4
FLOWS = 2 * PAIRS


def quantize(value):
    top = jnp.maximum(jnp.max(jnp.abs(value), axis=0, keepdims=True), jnp.float32(1e-30))
    levels = jnp.round(value * (jnp.float32(32766.0) / top))
    return levels.astype(jnp.int32).astype(jnp.int16), top * jnp.float32(1.0 / 32766.0)


def sum_kernel(part_ref, out_ref, *refs):
    rows, cols = part_ref.shape
    chunk = rows // 16
    names = ("give", "take", "own", "inner", "final", "cross", "last")
    levels = dict(zip(names, refs[0:7]))
    scales = dict(zip(names, refs[7:14]))
    arrivals = dict(zip(("take", "inner", "final", "cross", "last"), refs[14:19]))
    departures = dict(zip(("give", "own", "outward", "across", "last"), refs[19:24]))
    total_ref = refs[24]
    sec = lax.axis_index("sec")
    op = lax.axis_index("op")
    z, x = op // 2, op % 2
    mid = z % 3 != 0
    w = (z + 1) // 3
    side = (sec, z * 2 + 1 - x)
    other = (sec, (3 - z) * 2 + x)
    outer = (sec, 6 * w + x)
    inward = (sec, (1 + w) * 2 + x)

    barrier = pltpu.get_barrier_semaphore()

    def greet(device):
        pl.semaphore_signal(barrier, inc=1, device_id=device, device_id_type=MESH)

    greet(side)

    @pl.when(mid)
    def _():
        greet(other)
        greet(outer)
        pl.semaphore_wait(barrier, 3)

    @pl.when(jnp.logical_not(mid))
    def _():
        greet(inward)
        pl.semaphore_wait(barrier, 2)

    def message(source, i, target, j, departure, k, device):
        return [
            pltpu.make_async_remote_copy(
                src_ref=bufs[source].at[i],
                dst_ref=bufs[target].at[j],
                send_sem=departures[departure].at[k, n],
                recv_sem=arrivals[target].at[j, n],
                device_id=device,
                device_id_type=MESH,
            )
            for n, bufs in enumerate((levels, scales))
        ]

    def start(*args):
        for copy in message(*args):
            copy.start()

    def sent(*args):
        for copy in message(*args):
            copy.wait_send()

    def arrived(target, j):
        for copy in message(target, j, target, j, "give", 0, side):
            copy.wait_recv()

    def put(name, i, value):
        whole, scale = quantize(value)
        levels[name][i] = whole
        scales[name][i] = scale

    def get(name, i):
        return levels[name][i].astype(jnp.int32).astype(jnp.float32) * scales[name][i]

    def rows_of(p, e):
        first = (8 + 4 * e + p) if p < CROSSED else (4 * x + 2 * e + p - CROSSED)
        return pl.ds(pl.multiple_of(first * chunk, chunk), chunk)

    def halves_of(p, e):
        return pl.ds(pl.multiple_of((2 * e + p - CROSSED) * chunk, chunk), chunk)

    def value(p, e):
        if p < CROSSED:
            return part_ref[rows_of(p, e), :]
        return total_ref[halves_of(p, e), :]

    def give(j):
        put("give", j, part_ref[pl.ds(pl.multiple_of((4 * (1 - x) + j) * chunk, chunk), chunk), :])
        start("give", j, "take", j, "give", j, side)

    def gather(j):
        arrived("take", j)
        mine = part_ref[pl.ds(pl.multiple_of((4 * x + j) * chunk, chunk), chunk), :]
        total_ref[pl.ds(j * chunk, chunk), :] = mine + get("take", j)

    def finish(p, e):
        out_ref[rows_of(p, e), :] = get("final", 2 * p + e)
        if p >= CROSSED:
            slot = 2 * (p - CROSSED) + e
            start("final", 2 * p + e, "last", slot, "last", slot, side)

    @pl.when(jnp.logical_not(mid))
    def _():
        def send(p, e):
            i = 2 * p + e
            put("own", i, value(p, e))
            far = w if e == 0 else 1 - w
            start("own", i, "inner", FLOWS * far + i, "own", i, inward)

        for p in range(CROSSED):
            send(p, 0)
            send(p, 1)
            give(p)
        for j in range(4):
            gather(j)
        for p in range(CROSSED, PAIRS):
            send(p, 0)
            send(p, 1)
        for p in range(PAIRS):
            for e in range(2):
                arrived("final", 2 * p + e)
                finish(p, e)
        for i in range(FLOWS):
            sent("own", i, "inner", i, "own", i, inward)

    @pl.when(mid)
    def _():
        def relay(p):
            i = 2 * p + 1 - w
            arrived("inner", FLOWS + i)
            put("own", i, value(p, 1 - w) + get("inner", FLOWS + i))
            start("own", i, "inner", FLOWS + i, "own", i, other)

        def collect(p):
            i = 2 * p + w
            arrived("inner", i)
            near = value(p, w) + get("inner", i)
            arrived("inner", FLOWS + i)
            near = near + get("inner", FLOWS + i)
            if p < CROSSED:
                put("own", i, near)
                start("own", i, "cross", p, "own", i, side)
            else:
                put("final", i, near)
                spread(p)

        def spread(p):
            i = 2 * p + w
            start("final", i, "final", i, "outward", i, outer)
            start("final", i, "final", i, "across", p, other)
            finish(p, w)

        def merge(p):
            i = 2 * p + w
            arrived("cross", p)
            put("final", i, get("own", i) + get("cross", p))
            spread(p)

        def forward(p):
            i = 2 * p + 1 - w
            arrived("final", i)
            start("final", i, "final", i, "outward", i, outer)
            finish(p, 1 - w)

        for j in range(4):
            give(j)
        for p in range(PAIRS + 2):
            if p < PAIRS:
                relay(p)
                collect(p)
            if 1 <= p <= CROSSED:
                merge(p - 1)
            if p == 1:
                for j in range(4):
                    gather(j)
            if p >= 2:
                forward(p - 2)
        for p in range(PAIRS):
            i = 2 * p + 1 - w
            sent("own", i, "inner", i, "own", i, other)
            if p < CROSSED:
                sent("own", 2 * p + w, "cross", p, "own", 2 * p + w, side)
            for e in range(2):
                sent("final", 2 * p + e, "final", 2 * p + e, "outward", 2 * p + e, outer)
            sent("final", 2 * p + w, "final", 2 * p + w, "across", p, other)

    for j in range(4):
        sent("give", j, "take", j, "give", j, side)
    for p in range(CROSSED, PAIRS):
        for e in range(2):
            slot = 2 * (p - CROSSED) + e
            arrived("last", slot)
            first = 4 * (1 - x) + 2 * e + p - CROSSED
            out_ref[pl.ds(pl.multiple_of(first * chunk, chunk), chunk), :] = get("last", slot)
            sent("final", 2 * p + e, "last", slot, "last", slot, side)


def sum_over_op_kernel(part):
    rows, cols = part.shape
    chunk = rows // 16
    counts = (4, 4, FLOWS, 2 * FLOWS, FLOWS, CROSSED, 4)
    sem = pltpu.SemaphoreType.DMA
    return pl.pallas_call(
        sum_kernel,
        out_shape=jax.ShapeDtypeStruct((rows, cols), jnp.float32),
        in_specs=[pl.BlockSpec(memory_space=pltpu.VMEM)],
        out_specs=pl.BlockSpec(memory_space=pltpu.VMEM),
        scratch_shapes=[pltpu.VMEM((n, chunk, cols), jnp.int16) for n in counts]
        + [pltpu.VMEM((n, 1, cols), jnp.float32) for n in counts]
        + [sem((n, 2)) for n in (4, 2 * FLOWS, FLOWS, CROSSED, 4)]
        + [sem((n, 2)) for n in (4, FLOWS, FLOWS, PAIRS, 4)]
        + [pltpu.VMEM((4 * chunk, cols), jnp.float32)],
        compiler_params=pltpu.CompilerParams(collective_id=1, has_side_effects=True),
        name="sum_over_op",
    )(part)


def fetch_kernel(wanted_ref, own_ref, out_ref, store, picked, landed, line_in, side_in, core_in, core_in2, x_in, line_out, side_out, core_out, core_out2, x_out):
    rows = own_ref.shape[0]
    sec = lax.axis_index("sec")
    op = lax.axis_index("op")
    y, c = sec // 2, sec % 2
    z, x = op // 2, op % 2
    far = z // 2
    zz = z + far * (3 - 2 * z)
    mid = zz == 1
    twin = (y * 2 + 1 - c, op)
    over = ((1 - y) * 2 + c, op)
    side = (sec, z * 2 + 1 - x)
    line_sec = sec
    inner = (sec, (1 + far) * 2 + x)
    end = (sec, 6 * far + x)
    other = (sec, (3 - z) * 2 + x)
    sec_over = (1 - y) * 2 + c
    sec_twin = y * 2 + 1 - c
    sec_cross = (1 - y) * 2 + 1 - c

    barrier = pltpu.get_barrier_semaphore()

    def greet(device):
        pl.semaphore_signal(barrier, inc=1, device_id=device, device_id_type=MESH)

    greet(twin)
    greet(over)
    greet(side)

    @pl.when(mid)
    def _():
        greet(other)
        greet(end)
        pl.semaphore_wait(barrier, 5)

    @pl.when(jnp.logical_not(mid))
    def _():
        greet(inner)
        pl.semaphore_wait(barrier, 4)

    marks = [zz, 1 - zz, 2, 3]
    place = [q + far * (3 - 2 * q) for q in marks]

    def slot(step, sector):
        return store.at[place[step] * 4 + sector]

    def copy(source, target, send, receive, device):
        return pltpu.make_async_remote_copy(
            src_ref=source,
            dst_ref=target,
            send_sem=send,
            recv_sem=receive,
            device_id=device,
            device_id_type=MESH,
        )

    def piece(step):
        return own_ref if step == 0 else slot(step, sec)

    def along(step, lane, device):
        return copy(piece(step), slot(step, sec), line_out.at[step, lane], line_in.at[place[step]], device)

    def across(step):
        return copy(piece(step), slot(step, sec), side_out.at[step], side_in.at[step], over)

    def to_twin(step):
        return copy(piece(step), slot(step, sec), core_out.at[step], core_in.at[step], twin)

    def to_twin_second(step):
        return copy(slot(step, sec_over), slot(step, sec_over), core_out2.at[step], core_in2.at[step], twin)

    def to_side(step):
        return copy(picked.at[step], landed.at[step], x_out.at[step], x_in.at[step], side)

    def first(step):
        if step == 0:
            @pl.when(mid)
            def _():
                along(0, 0, other).start()
                along(0, 1, end).start()

            @pl.when(jnp.logical_not(mid))
            def _():
                along(0, 0, inner).start()
        else:
            copy(slot(step, sec), slot(step, sec), line_out.at[step, 0], line_in.at[place[step]], side).wait_recv()

            @pl.when(mid)
            def _():
                if step == 1:
                    along(1, 0, other).start()
                else:
                    along(step, 0, end).start()

        across(step).start()
        to_twin(step).start()

    def second(step):
        copy(slot(step, sec_over), slot(step, sec_over), side_out.at[step], side_in.at[step], over).wait_recv()
        to_twin_second(step).start()

    def choose(step, wanted):
        base = place[step] * 4
        value = store[base + 3]
        for sector in range(3):
            value = jnp.where(wanted == sector, store[base + sector], value)
        return value

    def third(step):
        copy(slot(step, sec_twin), slot(step, sec_twin), core_out.at[step], core_in.at[step], twin).wait_recv()
        copy(slot(step, sec_cross), slot(step, sec_cross), core_out2.at[step], core_in2.at[step], twin).wait_recv()
        picked[step] = choose(step, wanted_ref[1])
        to_side(step).start()
        out_ref[pl.ds(pl.multiple_of((place[step] * 2 + x) * rows, rows), rows), :] = choose(step, wanted_ref[0])

    store[place[0] * 4 + sec] = own_ref[...]
    for step in range(6):
        if step < 4:
            first(step)
        if 1 <= step < 5:
            second(step - 1)
        if step >= 2:
            third(step - 2)
    for step in range(4):
        to_side(step).wait_recv()
        out_ref[pl.ds(pl.multiple_of((place[step] * 2 + 1 - x) * rows, rows), rows), :] = landed[step]
    for step in range(4):
        across(step).wait_send()
        to_twin(step).wait_send()
        to_twin_second(step).wait_send()
        to_side(step).wait_send()

    @pl.when(mid)
    def _():
        along(0, 0, other).wait_send()
        along(0, 1, end).wait_send()
        along(1, 0, other).wait_send()
        along(2, 0, end).wait_send()
        along(3, 0, end).wait_send()

    @pl.when(jnp.logical_not(mid))
    def _():
        along(0, 0, inner).wait_send()


def fetch_by_kernel(own_slice, wanted):
    rows, cols = own_slice.shape
    sem = pltpu.SemaphoreType.DMA
    half = own_slice.dtype
    return pl.pallas_call(
        fetch_kernel,
        out_shape=jax.ShapeDtypeStruct((rows * lax.axis_size("op"), cols), half),
        in_specs=[pl.BlockSpec(memory_space=pltpu.SMEM), pl.BlockSpec(memory_space=pltpu.VMEM)],
        out_specs=pl.BlockSpec(memory_space=pltpu.VMEM),
        scratch_shapes=[pltpu.VMEM((16, rows, cols), half), pltpu.VMEM((4, rows, cols), half), pltpu.VMEM((4, rows, cols), half)]
        + [sem((4,))] * 5
        + [sem((4, 2))]
        + [sem((4,))] * 4,
        compiler_params=pltpu.CompilerParams(collective_id=2, has_side_effects=True),
        name="fetch_source",
    )(wanted, own_slice)


def body(
    wavefunction,
    op_blocks,
    basis_guess,
    sector_sizes,
    kept_counts,
    target_map,
    noise_numerator,
    noise_denominator,
):
    state_count = wavefunction.shape[2]
    kept_width = basis_guess.shape[2]
    tile_rows = state_count // lax.axis_size("op")
    sec_index = lax.axis_index("sec")
    op_index = lax.axis_index("op")
    small = lax.axis_size("op") == 2 * DEPTH and lax.axis_size("sec") == 4
    noise_weight = noise_numerator[0].astype(jnp.float32) / noise_denominator[0].astype(jnp.float32)
    sources = source_sectors(target_map)
    wanted_all = lax.dynamic_index_in_dim(sources, sec_index, 1, keepdims=False)[None, :]
    wanted = lax.dynamic_index_in_dim(wanted_all[0], op_index, 0, keepdims=False)
    states = jnp.arange(state_count, dtype=jnp.int32)
    own_size = lax.dynamic_index_in_dim(sector_sizes, sec_index, 0, keepdims=False)
    source_size = lax.dynamic_index_in_dim(sector_sizes, wanted, 0, keepdims=False)
    own_count = lax.dynamic_index_in_dim(kept_counts, sec_index, 0, keepdims=False)
    own_kept = jnp.arange(kept_width, dtype=jnp.int32) < own_count
    zero_half = jnp.zeros((), jnp.bfloat16)
    own_rows = jnp.where((states < own_size)[None, :], wavefunction[0], zero_half)
    if small:
        beside = lax.dynamic_index_in_dim(wanted_all[0], op_index + 1 - 2 * (op_index % 2), 0, keepdims=False)
        moved = fetch_by_kernel(wavefunction[0], jnp.stack([wanted, beside]))
    else:
        moved = fetch_pieces(wavefunction, wanted_all)[0]
    moved = jnp.where((states < source_size)[None, :], moved, zero_half)
    blocks = op_blocks[0, 0]
    perturbed = jnp.dot(moved, blocks, preferred_element_type=jnp.float32).astype(jnp.bfloat16)
    guess = jnp.where((states < own_size)[:, None], basis_guess[0], zero_half)
    perturbed_guess = noise_weight * jnp.dot(perturbed, guess, preferred_element_type=jnp.float32)
    own_guess = jnp.dot(own_rows, guess, preferred_element_type=jnp.float32)
    part = lax.dot_general(
        jnp.concatenate([perturbed, own_rows], axis=0).astype(jnp.float32),
        jnp.concatenate([perturbed_guess, own_guess], axis=0),
        (((0,), (0,)), ((), ())),
        precision=lax.Precision.HIGH,
    )
    part = jnp.where((states < own_size)[:, None] & own_kept[None, :], part, jnp.float32(0.0))
    if small:
        full_image = sum_over_op_kernel(part)
    else:
        full_image = sum_over_op(part)
    padding = jnp.where(own_kept, jnp.float32(0.0), jnp.float32(1.0))
    correlation = dot_ta(full_image, full_image) + padding[:, None] * jnp.eye(
        kept_width, dtype=jnp.float32
    )
    inverse = inverse_factor(correlation)
    new_basis = lax.dot_general(
        full_image, inverse, (((1,), (1,)), ((), ())), precision=lax.Precision.HIGH
    )
    kept_tile = (
        lax.dynamic_slice_in_dim(new_basis, op_index * tile_rows, tile_rows, 0)
        * float(state_count) ** 0.5
    )
    basis_half = new_basis.astype(jnp.bfloat16)
    mapped = jnp.dot(blocks, basis_half, preferred_element_type=jnp.float32).astype(jnp.bfloat16)
    source_basis = fetch_sector(basis_half, wanted)
    rotated = lax.dot_general(
        source_basis, mapped, (((0,), (0,)), ((), ())), preferred_element_type=jnp.float32
    )
    return (kept_tile[None], rotated[None, None])


def solution(mesh):
    placed = (
        P("sec", "op", None),
        P("op", "sec", None, None),
        P("sec", None, None),
        P(),
        P(),
        P(),
        P(),
        P(),
    )
    return jax.shard_map(
        body,
        mesh=mesh,
        in_specs=placed,
        out_specs=(P("sec", "op", None), P("op", "sec", None, None)),
        check_vma=False,
    )
```

```python
import jax
import jax.numpy as jnp
from jax import lax
from jax.experimental import pallas as pl
from jax.experimental.pallas import tpu as pltpu
from jax.sharding import PartitionSpec as P

LANES = 128
ROWS = 8
HIGHEST = lax.Precision.HIGHEST


def dot_ta(a, b):
    return lax.dot_general(
        a, b, (((0,), (0,)), ((), ())), precision=HIGHEST, preferred_element_type=jnp.float32
    )


def dot(a, b):
    return jnp.dot(a, b, precision=HIGHEST, preferred_element_type=jnp.float32)


def eliminate_tile(tile):
    count = LANES // ROWS
    row = lax.broadcasted_iota(jnp.int32, (ROWS, LANES), 0)
    lane = lax.broadcasted_iota(jnp.int32, (ROWS, LANES), 1)
    left = [tile[ROWS * q : ROWS * (q + 1), :] for q in range(count)]
    right = [jnp.where(lane == row + ROWS * q, 1.0, 0.0).astype(jnp.float32) for q in range(count)]
    for p in range(count):
        upper, lower = left[p], right[p]
        columns = [
            jnp.broadcast_to(upper[:, ROWS * p + j : ROWS * p + j + 1], (ROWS, LANES))
            for j in range(ROWS)
        ]
        for j in range(ROWS):
            scale = lax.rsqrt(jnp.broadcast_to(columns[j][j : j + 1, :], (ROWS, LANES)))
            factor = jnp.where(row > j, columns[j] * scale, 0.0)
            for k in range(j + 1, ROWS):
                own = jnp.broadcast_to(columns[k][j : j + 1, :], (ROWS, LANES)) * scale
                columns[k] = columns[k] - factor * own
            own_upper = jnp.broadcast_to(upper[j : j + 1, :], (ROWS, LANES)) * scale
            own_lower = jnp.broadcast_to(lower[j : j + 1, :], (ROWS, LANES)) * scale
            upper = jnp.where(row == j, own_upper, upper - factor * own_upper)
            lower = jnp.where(row == j, own_lower, lower - factor * own_lower)
        right[p] = lower
        if p + 1 < count:
            change = dot_ta(upper, jnp.concatenate([upper, lower], axis=1))
            for q in range(p + 1, count):
                part = change[ROWS * q : ROWS * (q + 1), :]
                left[q] = left[q] - part[:, :LANES]
                right[q] = right[q] - part[:, LANES:]
    return jnp.concatenate(right, axis=0)


def inverse_factor_kernel(matrix_ref, out_ref, work):
    size = matrix_ref.shape[0]
    blocks = size // LANES
    work[:, :size] = matrix_ref[...]
    work[:, size:] = (
        lax.broadcasted_iota(jnp.int32, (size, size), 0)
        == lax.broadcasted_iota(jnp.int32, (size, size), 1)
    ).astype(jnp.float32)

    def step(b, carry):
        rows = pl.ds(pl.multiple_of(b * LANES, LANES), LANES)
        inverse = eliminate_tile(work[rows, rows])
        panel = dot(inverse, work[rows, :])
        work[rows, :] = panel
        out_ref[rows, :] = panel[:, size:]

        def update(i, inner):
            below = pl.ds(pl.multiple_of(i * LANES, LANES), LANES)
            work[below, :] = work[below, :] - dot_ta(work[rows, below], work[rows, :])
            return inner

        lax.fori_loop(b + 1, blocks, update, 0)
        return carry

    lax.fori_loop(0, blocks, step, 0)


def inverse_factor(matrix):
    size = matrix.shape[0]
    return pl.pallas_call(
        inverse_factor_kernel,
        out_shape=jax.ShapeDtypeStruct((size, size), jnp.float32),
        in_specs=[pl.BlockSpec(memory_space=pltpu.VMEM)],
        out_specs=pl.BlockSpec(memory_space=pltpu.VMEM),
        scratch_shapes=[pltpu.VMEM((size, 2 * size), jnp.float32)],
        compiler_params=pltpu.CompilerParams(vmem_limit_bytes=24 * 1024 * 1024),
        cost_estimate=pl.CostEstimate(flops=2 * size**3, bytes_accessed=8 * size * size, transcendentals=size),
        name="inverse_factor",
    )(matrix)


def source_sectors(target_map):
    sectors = jnp.arange(target_map.shape[1], dtype=jnp.int32)
    matches = target_map[:, :, None] == sectors[None, None, :]
    return jnp.sum(jnp.where(matches, sectors[None, :, None], 0), axis=1)


def fetch_pieces(own_slice, wanted_all):
    everyone = lax.all_gather(own_slice, "sec", axis=0, tiled=True)
    outgoing = jnp.take(everyone, wanted_all, axis=0)
    incoming = lax.all_to_all(outgoing, "op", split_axis=1, concat_axis=1, tiled=True)
    return incoming.reshape(
        incoming.shape[0], incoming.shape[1] * incoming.shape[2], incoming.shape[3]
    )


def exchange(value, axis, bit):
    count = lax.axis_size(axis)
    return lax.ppermute(value, axis, [(i, i ^ bit) for i in range(count)])


def halves(value, side):
    half = value.shape[0] // 2
    kept = lax.dynamic_slice_in_dim(value, side * half, half, 0)
    given = lax.dynamic_slice_in_dim(value, (1 - side) * half, half, 0)
    return kept, given


def sum_over_op(value):
    count = lax.axis_size("op")
    index = lax.axis_index("op")
    bits = [1 << b for b in range(count.bit_length() - 1)]
    orders = [bits, bits[1:] + bits[:1]]
    half = value.shape[0] // 2
    held = [value[:half], value[half:]]
    for step in range(len(bits)):
        for color, order in enumerate(orders):
            kept, given = halves(held[color], (index // order[step]) % 2)
            held[color] = kept + exchange(given, "op", order[step])
    for step in reversed(range(len(bits))):
        for color, order in enumerate(orders):
            own = held[color]
            other = exchange(own, "op", order[step])
            first = (index // order[step]) % 2 == 0
            held[color] = jnp.concatenate(
                [jnp.where(first, own, other), jnp.where(first, other, own)], axis=0
            )
    return jnp.concatenate(held, axis=0)


def fetch_sector(own, wanted):
    count = lax.axis_size("sec")
    offset = lax.axis_index("sec") ^ wanted
    held = {0: own}
    bit = count // 2
    while bit:
        for known in list(held):
            held[known ^ bit] = exchange(held[known], "sec", bit)
        bit //= 2
    result = own
    for known, value in held.items():
        result = jnp.where(offset == known, value, result)
    return result


MESH = pl.DeviceIdType.MESH
DEPTH = 4
PAIRS = 6
CROSSED = 4
FLOWS = 2 * PAIRS
PARTS = 2
WAVES = DEPTH * PARTS


def quantize(value):
    top = jnp.maximum(jnp.max(jnp.abs(value), axis=0, keepdims=True), jnp.float32(1e-30))
    levels = jnp.round(value * (jnp.float32(32766.0) / top))
    return levels.astype(jnp.int32).astype(jnp.int16), top * jnp.float32(1.0 / 32766.0)


def remote(source, target, send, receive, device):
    return pltpu.make_async_remote_copy(
        src_ref=source,
        dst_ref=target,
        send_sem=send,
        recv_sem=receive,
        device_id=device,
        device_id_type=MESH,
    )


def greet(device):
    pl.semaphore_signal(pltpu.get_barrier_semaphore(), inc=1, device_id=device, device_id_type=MESH)


def source_of(map_ref, op, sec):
    found = jnp.int32(0)
    for sector in range(map_ref.shape[1]):
        found = jnp.where(map_ref[op, sector] == sec, sector, found)
    return found


def before(limit, width, dtype):
    lane = lax.broadcasted_iota(jnp.int32, (1, width), 1)
    return jnp.where(lane < limit, 1.0, 0.0).astype(jnp.float32).astype(dtype)


def image_kernel(sizes_ref, counts_ref, map_ref, top_ref, bottom_ref, own_ref, blocks_hbm, guess_hbm, out_ref, *refs):
    rows = own_ref.shape[0]
    states = own_ref.shape[1]
    kept = out_ref.shape[1]
    chunk = states // 16
    band = rows // PARTS
    sec = lax.axis_index("sec")
    op = lax.axis_index("op")
    y, c = sec // 2, sec % 2
    z, x = op // 2, op % 2
    w = z // 2
    zz = z + w * (3 - 2 * z)
    mid = zz == 1
    leaf = jnp.logical_not(mid)
    sec_over = (1 - y) * 2 + c
    sec_twin = y * 2 + 1 - c
    sec_cross = (1 - y) * 2 + 1 - c
    twin = (sec_twin, op)
    over = (sec_over, op)
    side = (sec, z * 2 + 1 - x)
    inner = (sec, (1 + w) * 2 + x)
    outer = (sec, 6 * w + x)
    other = (sec, (3 - z) * 2 + x)

    (store, picked, landed, moved, blocks, guess, left, high, low) = refs[:9]
    (line_in, side_in, core_in, cross_in, x_in, line_out, side_out, core_out, cross_out, x_out, load) = refs[9:20]
    refs = refs[20:]
    names = ("give", "take", "own", "inner", "final", "cross", "last")
    levels = dict(zip(names, refs[0:7]))
    scales = dict(zip(names, refs[7:14]))
    arrivals = dict(zip(("take", "inner", "final", "cross", "last"), refs[14:19]))
    departures = dict(zip(("give", "own", "outward", "across", "last"), refs[19:24]))
    part_ref, total_ref = refs[24:26]

    load_blocks = pltpu.make_async_copy(blocks_hbm, blocks, load.at[0])
    load_guess = pltpu.make_async_copy(guess_hbm, guess, load.at[1])
    load_blocks.start()
    load_guess.start()
    barrier = pltpu.get_barrier_semaphore()
    greet(twin)
    greet(over)
    greet(side)

    @pl.when(mid)
    def _():
        greet(other)
        greet(outer)
        pl.semaphore_wait(barrier, 5)

    @pl.when(leaf)
    def _():
        greet(inner)
        pl.semaphore_wait(barrier, 4)

    wanted = source_of(map_ref, op, sec)
    beside = source_of(map_ref, op + 1 - 2 * x, sec)
    source_mask = before(sizes_ref[wanted], states, jnp.bfloat16)
    own_size = sizes_ref[sec]
    own_mask = before(own_size, states, jnp.bfloat16)

    marks = [zz, 1 - zz, 2, 3]
    place = [q + w * (3 - 2 * q) for q in marks]

    def slot(v, sector):
        return store.at[(place[v // PARTS] * 4 + sector) * PARTS + v % PARTS]

    def piece(v):
        if v < PARTS:
            return own_ref.at[pl.ds(v * band, band)]
        return slot(v, sec)

    def line_sem(v):
        return line_in.at[place[v // PARTS] * PARTS + v % PARTS]

    def along(v, lane, device):
        return remote(piece(v), slot(v, sec), line_out.at[v, lane], line_sem(v), device)

    def across(v):
        return remote(piece(v), slot(v, sec), side_out.at[v], side_in.at[v], over)

    def to_twin(v):
        return remote(piece(v), slot(v, sec), core_out.at[v], core_in.at[v], twin)

    def to_twin_second(v):
        return remote(slot(v, sec_over), slot(v, sec_over), cross_out.at[v], cross_in.at[v], twin)

    def to_side(v):
        return remote(picked.at[v], landed.at[v], x_out.at[v], x_in.at[v], side)

    def first(v):
        step = v // PARTS
        if step == 0:

            @pl.when(mid)
            def _():
                along(v, 0, other).start()
                along(v, 1, outer).start()

            @pl.when(leaf)
            def _():
                along(v, 0, inner).start()
        else:
            remote(slot(v, sec), slot(v, sec), line_out.at[v, 0], line_sem(v), side).wait_recv()

            @pl.when(mid)
            def _():
                along(v, 0, other if step == 1 else outer).start()

        across(v).start()
        to_twin(v).start()

    def second(v):
        remote(slot(v, sec_over), slot(v, sec_over), side_out.at[v], side_in.at[v], over).wait_recv()
        to_twin_second(v).start()

    def choose(v, sector_wanted):
        base = place[v // PARTS] * 4
        value = store[(base + 3) * PARTS + v % PARTS]
        for sector in range(3):
            value = jnp.where(sector_wanted == sector, store[(base + sector) * PARTS + v % PARTS], value)
        return value

    def third(v):
        remote(slot(v, sec_twin), slot(v, sec_twin), core_out.at[v], core_in.at[v], twin).wait_recv()
        remote(slot(v, sec_cross), slot(v, sec_cross), core_out.at[v], cross_in.at[v], twin).wait_recv()
        picked[v] = choose(v, beside)
        to_side(v).start()
        moved[pl.ds(v * band, band), :] = choose(v, wanted) * source_mask

    def perturb(half):
        span = pl.ds(half * DEPTH * rows, DEPTH * rows)

        def step(n, carry):
            lanes = pl.ds(pl.multiple_of(n * 256, 256), 256)
            value = jnp.dot(moved[span, :], blocks[:, lanes], preferred_element_type=jnp.float32)
            lane = lax.broadcasted_iota(jnp.int32, (1, 256), 1) + n * 256
            keep = jnp.where(lane < own_size, 1.0, 0.0).astype(jnp.float32).astype(jnp.bfloat16)
            left[span, lanes] = value.astype(jnp.bfloat16) * keep
            return carry

        lax.fori_loop(0, states // 256, step, 0)

    for v in range(PARTS):
        store[(place[0] * 4 + sec) * PARTS + v] = own_ref[pl.ds(v * band, band), :]
    left[pl.ds(2 * DEPTH * rows, rows), :] = own_ref[...] * own_mask
    first(0)
    for v in range(1, WAVES + 1):
        if v < WAVES:
            first(v)
        second(v - 1)
        third(v - 1)
    load_blocks.wait()
    load_guess.wait()
    perturb(0)
    for v in range(WAVES):
        to_side(v).wait_recv()
        moved[pl.ds(DEPTH * rows + v * band, band), :] = landed[v] * source_mask
    perturb(1)
    weight = jnp.full((1, kept), top_ref[0], jnp.int32).astype(jnp.float32) / jnp.full(
        (1, kept), bottom_ref[0], jnp.int32
    ).astype(jnp.float32)
    kept_mask = before(counts_ref[sec], kept, jnp.float32)

    def project(first_row, count, factor):
        span = pl.ds(first_row, count)
        value = jnp.dot(left[span, :], guess[...], preferred_element_type=jnp.float32) * factor
        top_half = value.astype(jnp.bfloat16)
        high[span, :] = top_half
        low[span, :] = (value - top_half.astype(jnp.float32)).astype(jnp.bfloat16)

    project(0, DEPTH * rows, weight * kept_mask)
    project(DEPTH * rows, DEPTH * rows, weight * kept_mask)
    project(2 * DEPTH * rows, rows, kept_mask)

    def product(n):
        lanes = pl.ds(pl.multiple_of(n * 256, 256), 256)
        dims = (((0,), (0,)), ((), ()))
        value = lax.dot_general(left[:, lanes], high[...], dims, preferred_element_type=jnp.float32)
        part_ref[lanes, :] = value + lax.dot_general(
            left[:, lanes], low[...], dims, preferred_element_type=jnp.float32
        )

    def products(start_tile):
        def step(n, carry):
            product(start_tile + n)
            return carry

        lax.fori_loop(0, states // 512, step, 0)

    def message(source, i, target, j, departure, k, device):
        return [
            remote(bufs[source].at[i], bufs[target].at[j], departures[departure].at[k, n], arrivals[target].at[j, n], device)
            for n, bufs in enumerate((levels, scales))
        ]

    def start(*args):
        for copy in message(*args):
            copy.start()

    def sent(*args):
        for copy in message(*args):
            copy.wait_send()

    def arrived(target, j):
        for copy in message(target, j, target, j, "give", 0, side):
            copy.wait_recv()

    def put(name, i, value):
        whole, scale = quantize(value)
        levels[name][i] = whole
        scales[name][i] = scale

    def get(name, i):
        return levels[name][i].astype(jnp.int32).astype(jnp.float32) * scales[name][i]

    def rows_of(p, e):
        start_chunk = (8 + 4 * e + p) if p < CROSSED else (4 * x + 2 * e + p - CROSSED)
        return pl.ds(pl.multiple_of(start_chunk * chunk, chunk), chunk)

    def halves_of(p, e):
        return pl.ds(pl.multiple_of((2 * e + p - CROSSED) * chunk, chunk), chunk)

    def value(p, e):
        if p < CROSSED:
            return part_ref[rows_of(p, e), :]
        return total_ref[halves_of(p, e), :]

    def give(j):
        put("give", j, part_ref[pl.ds(pl.multiple_of((4 * (1 - x) + j) * chunk, chunk), chunk), :])
        start("give", j, "take", j, "give", j, side)

    def gather(j):
        arrived("take", j)
        mine = part_ref[pl.ds(pl.multiple_of((4 * x + j) * chunk, chunk), chunk), :]
        total_ref[pl.ds(j * chunk, chunk), :] = mine + get("take", j)

    def finish(p, e):
        out_ref[rows_of(p, e), :] = get("final", 2 * p + e)
        if p >= CROSSED:
            place_last = 2 * (p - CROSSED) + e
            start("final", 2 * p + e, "last", place_last, "last", place_last, side)

    products(states // 512)

    @pl.when(leaf)
    def _():
        def send(p, e):
            i = 2 * p + e
            put("own", i, value(p, e))
            far = w if e == 0 else 1 - w
            start("own", i, "inner", FLOWS * far + i, "own", i, inner)

        for p in range(CROSSED):
            send(p, 0)
            send(p, 1)
        products(0)
        for j in range(4):
            give(j)
        for j in range(4):
            gather(j)
        for p in range(CROSSED, PAIRS):
            send(p, 0)
            send(p, 1)
        for p in range(PAIRS):
            for e in range(2):
                arrived("final", 2 * p + e)
                finish(p, e)
        for i in range(FLOWS):
            sent("own", i, "inner", i, "own", i, inner)

    @pl.when(mid)
    def _():
        def relay(p):
            i = 2 * p + 1 - w
            arrived("inner", FLOWS + i)
            put("own", i, value(p, 1 - w) + get("inner", FLOWS + i))
            start("own", i, "inner", FLOWS + i, "own", i, other)

        def collect(p):
            i = 2 * p + w
            arrived("inner", i)
            near = value(p, w) + get("inner", i)
            arrived("inner", FLOWS + i)
            near = near + get("inner", FLOWS + i)
            if p < CROSSED:
                put("own", i, near)
                start("own", i, "cross", p, "own", i, side)
            else:
                put("final", i, near)
                spread(p)

        def spread(p):
            i = 2 * p + w
            start("final", i, "final", i, "outward", i, outer)
            start("final", i, "final", i, "across", p, other)
            finish(p, w)

        def merge(p):
            i = 2 * p + w
            arrived("cross", p)
            put("final", i, get("own", i) + get("cross", p))
            spread(p)

        def forward(p):
            i = 2 * p + 1 - w
            arrived("final", i)
            start("final", i, "final", i, "outward", i, outer)
            finish(p, 1 - w)

        products(0)
        for j in range(4):
            give(j)
        for p in range(PAIRS + 3):
            if p < PAIRS:
                relay(p)
            if 1 <= p <= PAIRS:
                collect(p - 1)
            if 2 <= p < CROSSED + 2:
                merge(p - 2)
            if p == 2:
                for j in range(4):
                    gather(j)
            if p >= 3:
                forward(p - 3)
        for p in range(PAIRS):
            i = 2 * p + 1 - w
            sent("own", i, "inner", i, "own", i, other)
            if p < CROSSED:
                sent("own", 2 * p + w, "cross", p, "own", 2 * p + w, side)
            for e in range(2):
                sent("final", 2 * p + e, "final", 2 * p + e, "outward", 2 * p + e, outer)
            sent("final", 2 * p + w, "final", 2 * p + w, "across", p, other)

    for j in range(4):
        sent("give", j, "take", j, "give", j, side)
    for p in range(CROSSED, PAIRS):
        for e in range(2):
            place_last = 2 * (p - CROSSED) + e
            arrived("last", place_last)
            start_chunk = 4 * (1 - x) + 2 * e + p - CROSSED
            out_ref[pl.ds(pl.multiple_of(start_chunk * chunk, chunk), chunk), :] = get("last", place_last)
            sent("final", 2 * p + e, "last", place_last, "last", place_last, side)
    for v in range(WAVES):
        across(v).wait_send()
        to_twin(v).wait_send()
        to_twin_second(v).wait_send()
        to_side(v).wait_send()

    @pl.when(mid)
    def _():
        for v in range(WAVES):
            if v < PARTS:
                along(v, 0, other).wait_send()
                along(v, 1, outer).wait_send()
            else:
                along(v, 0, other if v < 2 * PARTS else outer).wait_send()

    @pl.when(leaf)
    def _():
        for v in range(PARTS):
            along(v, 0, inner).wait_send()


def reduced_image(own, blocks, guess, sizes, counts, target_map, top, bottom):
    rows, states = own.shape
    kept = guess.shape[1]
    chunk = states // 16
    lengths = (4, 4, FLOWS, 2 * FLOWS, FLOWS, CROSSED, 4)
    sem = pltpu.SemaphoreType.DMA
    half = own.dtype
    total = 2 * DEPTH * rows
    return pl.pallas_call(
        image_kernel,
        out_shape=jax.ShapeDtypeStruct((states, kept), jnp.float32),
        in_specs=[pl.BlockSpec(memory_space=pltpu.SMEM)] * 5
        + [pl.BlockSpec(memory_space=pltpu.VMEM)]
        + [pl.BlockSpec(memory_space=pl.ANY)] * 2,
        out_specs=pl.BlockSpec(memory_space=pltpu.VMEM),
        scratch_shapes=[
            pltpu.VMEM((16 * PARTS, rows // PARTS, states), half),
            pltpu.VMEM((WAVES, rows // PARTS, states), half),
            pltpu.VMEM((WAVES, rows // PARTS, states), half),
            pltpu.VMEM((total, states), half),
            pltpu.VMEM((states, states), half),
            pltpu.VMEM((states, kept), half),
            pltpu.VMEM((total + rows, states), half),
            pltpu.VMEM((total + rows, kept), half),
            pltpu.VMEM((total + rows, kept), half),
        ]
        + [sem((WAVES,))] * 5
        + [sem((WAVES, 2))]
        + [sem((WAVES,))] * 4
        + [sem((2,))]
        + [pltpu.VMEM((n, chunk, kept), jnp.int16) for n in lengths]
        + [pltpu.VMEM((n, 1, kept), jnp.float32) for n in lengths]
        + [sem((n, 2)) for n in (4, 2 * FLOWS, FLOWS, CROSSED, 4)]
        + [sem((n, 2)) for n in (4, FLOWS, FLOWS, PAIRS, 4)]
        + [pltpu.VMEM((states, kept), jnp.float32), pltpu.VMEM((4 * chunk, kept), jnp.float32)],
        compiler_params=pltpu.CompilerParams(
            collective_id=1, has_side_effects=True, vmem_limit_bytes=48 * 1024 * 1024
        ),
        name="reduced_image",
    )(sizes, counts, target_map, top, bottom, own, blocks, guess)


def body(
    wavefunction,
    op_blocks,
    basis_guess,
    sector_sizes,
    kept_counts,
    target_map,
    noise_numerator,
    noise_denominator,
):
    state_count = wavefunction.shape[2]
    kept_width = basis_guess.shape[2]
    tile_rows = state_count // lax.axis_size("op")
    sec_index = lax.axis_index("sec")
    op_index = lax.axis_index("op")
    noise_weight = noise_numerator[0].astype(jnp.float32) / noise_denominator[0].astype(jnp.float32)
    sources = source_sectors(target_map)
    wanted_all = lax.dynamic_index_in_dim(sources, sec_index, 1, keepdims=False)[None, :]
    wanted = lax.dynamic_index_in_dim(wanted_all[0], op_index, 0, keepdims=False)
    states = jnp.arange(state_count, dtype=jnp.int32)
    own_size = lax.dynamic_index_in_dim(sector_sizes, sec_index, 0, keepdims=False)
    source_size = lax.dynamic_index_in_dim(sector_sizes, wanted, 0, keepdims=False)
    own_count = lax.dynamic_index_in_dim(kept_counts, sec_index, 0, keepdims=False)
    own_kept = jnp.arange(kept_width, dtype=jnp.int32) < own_count
    zero_half = jnp.zeros((), jnp.bfloat16)
    own_rows = jnp.where((states < own_size)[None, :], wavefunction[0], zero_half)
    blocks = op_blocks[0, 0]
    if lax.axis_size("op") == 2 * DEPTH and lax.axis_size("sec") == 4:
        full_image = reduced_image(
            wavefunction[0],
            blocks,
            basis_guess[0],
            sector_sizes,
            kept_counts,
            target_map,
            noise_numerator,
            noise_denominator,
        )
    else:
        moved = fetch_pieces(wavefunction, wanted_all)[0]
        moved = jnp.where((states < source_size)[None, :], moved, zero_half)
        perturbed = jnp.dot(moved, blocks, preferred_element_type=jnp.float32).astype(jnp.bfloat16)
        guess = jnp.where((states < own_size)[:, None], basis_guess[0], zero_half)
        perturbed_guess = noise_weight * jnp.dot(perturbed, guess, preferred_element_type=jnp.float32)
        own_guess = jnp.dot(own_rows, guess, preferred_element_type=jnp.float32)
        part = lax.dot_general(
            jnp.concatenate([perturbed, own_rows], axis=0).astype(jnp.float32),
            jnp.concatenate([perturbed_guess, own_guess], axis=0),
            (((0,), (0,)), ((), ())),
            precision=lax.Precision.HIGH,
        )
        part = jnp.where((states < own_size)[:, None] & own_kept[None, :], part, jnp.float32(0.0))
        full_image = sum_over_op(part)
    padding = jnp.where(own_kept, jnp.float32(0.0), jnp.float32(1.0))
    correlation = dot_ta(full_image, full_image) + padding[:, None] * jnp.eye(
        kept_width, dtype=jnp.float32
    )
    inverse = inverse_factor(correlation)
    new_basis = lax.dot_general(
        full_image, inverse, (((1,), (1,)), ((), ())), precision=lax.Precision.HIGH
    )
    kept_tile = (
        lax.dynamic_slice_in_dim(new_basis, op_index * tile_rows, tile_rows, 0)
        * float(state_count) ** 0.5
    )
    basis_half = new_basis.astype(jnp.bfloat16)
    mapped = jnp.dot(blocks, basis_half, preferred_element_type=jnp.float32).astype(jnp.bfloat16)
    source_basis = fetch_sector(basis_half, wanted)
    rotated = lax.dot_general(
        source_basis, mapped, (((0,), (0,)), ((), ())), preferred_element_type=jnp.float32
    )
    return (kept_tile[None], rotated[None, None])


def solution(mesh):
    placed = (
        P("sec", "op", None),
        P("op", "sec", None, None),
        P("sec", None, None),
        P(),
        P(),
        P(),
        P(),
        P(),
    )
    return jax.shard_map(
        body,
        mesh=mesh,
        in_specs=placed,
        out_specs=(P("sec", "op", None), P("op", "sec", None, None)),
        check_vma=False,
    )
```

```python
import jax
import jax.numpy as jnp
from jax import lax
from jax.experimental import pallas as pl
from jax.experimental.pallas import tpu as pltpu
from jax.sharding import PartitionSpec as P

LANES = 128
ROWS = 8
HIGHEST = lax.Precision.HIGHEST


def dot_ta(a, b):
    return lax.dot_general(
        a, b, (((0,), (0,)), ((), ())), precision=HIGHEST, preferred_element_type=jnp.float32
    )


def dot(a, b):
    return jnp.dot(a, b, precision=HIGHEST, preferred_element_type=jnp.float32)


def eliminate_tile(tile):
    count = LANES // ROWS
    row = lax.broadcasted_iota(jnp.int32, (ROWS, LANES), 0)
    lane = lax.broadcasted_iota(jnp.int32, (ROWS, LANES), 1)
    left = [tile[ROWS * q : ROWS * (q + 1), :] for q in range(count)]
    right = [jnp.where(lane == row + ROWS * q, 1.0, 0.0).astype(jnp.float32) for q in range(count)]
    for p in range(count):
        upper, lower = left[p], right[p]
        columns = [
            jnp.broadcast_to(upper[:, ROWS * p + j : ROWS * p + j + 1], (ROWS, LANES))
            for j in range(ROWS)
        ]
        for j in range(ROWS):
            scale = lax.rsqrt(jnp.broadcast_to(columns[j][j : j + 1, :], (ROWS, LANES)))
            factor = jnp.where(row > j, columns[j] * scale, 0.0)
            for k in range(j + 1, ROWS):
                own = jnp.broadcast_to(columns[k][j : j + 1, :], (ROWS, LANES)) * scale
                columns[k] = columns[k] - factor * own
            own_upper = jnp.broadcast_to(upper[j : j + 1, :], (ROWS, LANES)) * scale
            own_lower = jnp.broadcast_to(lower[j : j + 1, :], (ROWS, LANES)) * scale
            upper = jnp.where(row == j, own_upper, upper - factor * own_upper)
            lower = jnp.where(row == j, own_lower, lower - factor * own_lower)
        right[p] = lower
        if p + 1 < count:
            change = dot_ta(upper, jnp.concatenate([upper, lower], axis=1))
            for q in range(p + 1, count):
                part = change[ROWS * q : ROWS * (q + 1), :]
                left[q] = left[q] - part[:, :LANES]
                right[q] = right[q] - part[:, LANES:]
    return jnp.concatenate(right, axis=0)


def inverse_factor_kernel(matrix_ref, out_ref, work):
    size = matrix_ref.shape[0]
    blocks = size // LANES
    work[:, :size] = matrix_ref[...]
    work[:, size:] = (
        lax.broadcasted_iota(jnp.int32, (size, size), 0)
        == lax.broadcasted_iota(jnp.int32, (size, size), 1)
    ).astype(jnp.float32)

    def step(b, carry):
        rows = pl.ds(pl.multiple_of(b * LANES, LANES), LANES)
        inverse = eliminate_tile(work[rows, rows])
        panel = dot(inverse, work[rows, :])
        work[rows, :] = panel
        out_ref[rows, :] = panel[:, size:]

        def update(i, inner):
            below = pl.ds(pl.multiple_of(i * LANES, LANES), LANES)
            work[below, :] = work[below, :] - dot_ta(work[rows, below], work[rows, :])
            return inner

        lax.fori_loop(b + 1, blocks, update, 0)
        return carry

    lax.fori_loop(0, blocks, step, 0)


def inverse_factor(matrix):
    size = matrix.shape[0]
    return pl.pallas_call(
        inverse_factor_kernel,
        out_shape=jax.ShapeDtypeStruct((size, size), jnp.float32),
        in_specs=[pl.BlockSpec(memory_space=pltpu.VMEM)],
        out_specs=pl.BlockSpec(memory_space=pltpu.VMEM),
        scratch_shapes=[pltpu.VMEM((size, 2 * size), jnp.float32)],
        compiler_params=pltpu.CompilerParams(vmem_limit_bytes=24 * 1024 * 1024),
        cost_estimate=pl.CostEstimate(flops=2 * size**3, bytes_accessed=8 * size * size, transcendentals=size),
        name="inverse_factor",
    )(matrix)


def source_sectors(target_map):
    sectors = jnp.arange(target_map.shape[1], dtype=jnp.int32)
    matches = target_map[:, :, None] == sectors[None, None, :]
    return jnp.sum(jnp.where(matches, sectors[None, :, None], 0), axis=1)


def fetch_pieces(own_slice, wanted_all):
    everyone = lax.all_gather(own_slice, "sec", axis=0, tiled=True)
    outgoing = jnp.take(everyone, wanted_all, axis=0)
    incoming = lax.all_to_all(outgoing, "op", split_axis=1, concat_axis=1, tiled=True)
    return incoming.reshape(
        incoming.shape[0], incoming.shape[1] * incoming.shape[2], incoming.shape[3]
    )


def exchange(value, axis, bit):
    count = lax.axis_size(axis)
    return lax.ppermute(value, axis, [(i, i ^ bit) for i in range(count)])


def halves(value, side):
    half = value.shape[0] // 2
    kept = lax.dynamic_slice_in_dim(value, side * half, half, 0)
    given = lax.dynamic_slice_in_dim(value, (1 - side) * half, half, 0)
    return kept, given


def sum_over_op(value):
    count = lax.axis_size("op")
    index = lax.axis_index("op")
    bits = [1 << b for b in range(count.bit_length() - 1)]
    orders = [bits, bits[1:] + bits[:1]]
    half = value.shape[0] // 2
    held = [value[:half], value[half:]]
    for step in range(len(bits)):
        for color, order in enumerate(orders):
            kept, given = halves(held[color], (index // order[step]) % 2)
            held[color] = kept + exchange(given, "op", order[step])
    for step in reversed(range(len(bits))):
        for color, order in enumerate(orders):
            own = held[color]
            other = exchange(own, "op", order[step])
            first = (index // order[step]) % 2 == 0
            held[color] = jnp.concatenate(
                [jnp.where(first, own, other), jnp.where(first, other, own)], axis=0
            )
    return jnp.concatenate(held, axis=0)


def fetch_sector(own, wanted):
    count = lax.axis_size("sec")
    offset = lax.axis_index("sec") ^ wanted
    held = {0: own}
    bit = count // 2
    while bit:
        for known in list(held):
            held[known ^ bit] = exchange(held[known], "sec", bit)
        bit //= 2
    result = own
    for known, value in held.items():
        result = jnp.where(offset == known, value, result)
    return result


MESH = pl.DeviceIdType.MESH
DEPTH = 4
PAIRS = 6
KINDS = (0, 1, 2, 8, 9, 3)
FLOWS = 2 * PAIRS
PARTS = 2
WAVES = DEPTH * PARTS


def quantize(value):
    top = jnp.maximum(jnp.max(jnp.abs(value), axis=0, keepdims=True), jnp.float32(1e-30))
    levels = jnp.round(value * (jnp.float32(32766.0) / top))
    return levels.astype(jnp.int32).astype(jnp.int16), top * jnp.float32(1.0 / 32766.0)


def remote(source, target, send, receive, device):
    return pltpu.make_async_remote_copy(
        src_ref=source,
        dst_ref=target,
        send_sem=send,
        recv_sem=receive,
        device_id=device,
        device_id_type=MESH,
    )


def greet(device):
    pl.semaphore_signal(pltpu.get_barrier_semaphore(), inc=1, device_id=device, device_id_type=MESH)


def source_of(map_ref, op, sec):
    found = jnp.int32(0)
    for sector in range(map_ref.shape[1]):
        found = jnp.where(map_ref[op, sector] == sec, sector, found)
    return found


def before(limit, width, dtype):
    lane = lax.broadcasted_iota(jnp.int32, (1, width), 1)
    return jnp.where(lane < limit, 1.0, 0.0).astype(jnp.float32).astype(dtype)


def image_kernel(sizes_hbm, counts_hbm, map_hbm, top_hbm, bottom_hbm, own_ref, blocks_hbm, guess_hbm, out_ref, *refs):
    rows = own_ref.shape[0]
    states = own_ref.shape[1]
    kept = out_ref.shape[1]
    chunk = states // 16
    band = rows // PARTS
    sec = lax.axis_index("sec")
    op = lax.axis_index("op")
    y, c = sec // 2, sec % 2
    z, x = op // 2, op % 2
    w = z // 2
    zz = z + w * (3 - 2 * z)
    mid = zz == 1
    leaf = jnp.logical_not(mid)
    sec_over = (1 - y) * 2 + c
    sec_twin = y * 2 + 1 - c
    sec_cross = (1 - y) * 2 + 1 - c
    twin = (sec_twin, op)
    over = (sec_over, op)
    side = (sec, z * 2 + 1 - x)
    inner = (sec, (1 + w) * 2 + x)
    outer = (sec, 6 * w + x)
    other = (sec, (3 - z) * 2 + x)

    (store, picked, landed, moved, blocks, guess, left, high, low) = refs[:9]
    (line_in, side_in, core_in, cross_in, x_in, line_out, side_out, core_out, cross_out, x_out, load) = refs[9:20]
    refs = refs[20:]
    names = ("give", "take", "own", "inner", "final", "cross", "last")
    levels = dict(zip(names, refs[0:7]))
    scales = dict(zip(names, refs[7:14]))
    arrivals = dict(zip(("take", "inner", "final", "cross", "last"), refs[14:19]))
    departures = dict(zip(("give", "own", "outward", "across", "last"), refs[19:24]))
    part_ref, total_ref = refs[24:26]
    scalars = refs[26:31]
    sizes_ref, counts_ref, map_ref, top_ref, bottom_ref = scalars
    loads = [
        pltpu.make_async_copy(source, target, load.at[2 + i])
        for i, (source, target) in enumerate(zip((sizes_hbm, counts_hbm, map_hbm, top_hbm, bottom_hbm), scalars))
    ]
    for copy in loads:
        copy.start()

    load_blocks = pltpu.make_async_copy(blocks_hbm, blocks, load.at[0])
    load_guess = pltpu.make_async_copy(guess_hbm, guess, load.at[1])
    load_blocks.start()
    load_guess.start()
    barrier = pltpu.get_barrier_semaphore()
    greet(twin)
    greet(over)
    greet(side)

    @pl.when(mid)
    def _():
        greet(other)
        greet(outer)
        pl.semaphore_wait(barrier, 5)

    @pl.when(leaf)
    def _():
        greet(inner)
        pl.semaphore_wait(barrier, 4)

    for copy in loads:
        copy.wait()
    wanted = source_of(map_ref, op, sec)
    beside = source_of(map_ref, op + 1 - 2 * x, sec)
    source_mask = before(sizes_ref[wanted], states, jnp.bfloat16)
    own_size = sizes_ref[sec]
    own_mask = before(own_size, states, jnp.bfloat16)

    marks = [zz, 1 - zz, 2, 3]
    place = [q + w * (3 - 2 * q) for q in marks]

    def slot(v, sector):
        return store.at[(place[v // PARTS] * 4 + sector) * PARTS + v % PARTS]

    def piece(v):
        if v < PARTS:
            return own_ref.at[pl.ds(v * band, band)]
        return slot(v, sec)

    def line_sem(v):
        return line_in.at[place[v // PARTS] * PARTS + v % PARTS]

    def along(v, lane, device):
        return remote(piece(v), slot(v, sec), line_out.at[v, lane], line_sem(v), device)

    def across(v):
        return remote(piece(v), slot(v, sec), side_out.at[v], side_in.at[v], over)

    def to_twin(v):
        return remote(piece(v), slot(v, sec), core_out.at[v], core_in.at[v], twin)

    def to_twin_second(v):
        return remote(slot(v, sec_over), slot(v, sec_over), cross_out.at[v], cross_in.at[v], twin)

    def to_side(v):
        return remote(picked.at[v], landed.at[v], x_out.at[v], x_in.at[v], side)

    def first(v):
        step = v // PARTS
        if step == 0:

            @pl.when(mid)
            def _():
                along(v, 0, other).start()
                along(v, 1, outer).start()

            @pl.when(leaf)
            def _():
                along(v, 0, inner).start()
        else:
            remote(slot(v, sec), slot(v, sec), line_out.at[v, 0], line_sem(v), side).wait_recv()

            @pl.when(mid)
            def _():
                along(v, 0, other if step == 1 else outer).start()

        across(v).start()
        to_twin(v).start()

    def second(v):
        remote(slot(v, sec_over), slot(v, sec_over), side_out.at[v], side_in.at[v], over).wait_recv()
        to_twin_second(v).start()

    def choose(v, sector_wanted):
        base = place[v // PARTS] * 4
        value = store[(base + 3) * PARTS + v % PARTS]
        for sector in range(3):
            value = jnp.where(sector_wanted == sector, store[(base + sector) * PARTS + v % PARTS], value)
        return value

    def third(v):
        remote(slot(v, sec_twin), slot(v, sec_twin), core_out.at[v], core_in.at[v], twin).wait_recv()
        remote(slot(v, sec_cross), slot(v, sec_cross), core_out.at[v], cross_in.at[v], twin).wait_recv()
        picked[v] = choose(v, beside)
        to_side(v).start()
        moved[pl.ds(v * band, band), :] = choose(v, wanted) * source_mask

    def perturb(half):
        span = pl.ds(half * DEPTH * rows, DEPTH * rows)

        def step(n, carry):
            lanes = pl.ds(pl.multiple_of(n * 256, 256), 256)
            value = jnp.dot(moved[span, :], blocks[:, lanes], preferred_element_type=jnp.float32)
            lane = lax.broadcasted_iota(jnp.int32, (1, 256), 1) + n * 256
            keep = jnp.where(lane < own_size, 1.0, 0.0).astype(jnp.float32).astype(jnp.bfloat16)
            left[span, lanes] = value.astype(jnp.bfloat16) * keep
            return carry

        lax.fori_loop(0, states // 256, step, 0)

    for v in range(PARTS):
        store[(place[0] * 4 + sec) * PARTS + v] = own_ref[pl.ds(v * band, band), :]
    left[pl.ds(2 * DEPTH * rows, rows), :] = own_ref[...] * own_mask
    for v in range(WAVES + 2):
        if v < WAVES:
            first(v)
        if 1 <= v <= WAVES:
            second(v - 1)
        if v >= 2:
            third(v - 2)
    load_blocks.wait()
    load_guess.wait()
    perturb(0)
    for v in range(WAVES):
        to_side(v).wait_recv()
        moved[pl.ds(DEPTH * rows + v * band, band), :] = landed[v] * source_mask
    perturb(1)
    weight = jnp.full((1, kept), top_ref[0], jnp.int32).astype(jnp.float32) / jnp.full(
        (1, kept), bottom_ref[0], jnp.int32
    ).astype(jnp.float32)
    kept_mask = before(counts_ref[sec], kept, jnp.float32)

    def project(first_row, count, factor):
        span = pl.ds(first_row, count)
        value = jnp.dot(left[span, :], guess[...], preferred_element_type=jnp.float32) * factor
        top_half = value.astype(jnp.bfloat16)
        high[span, :] = top_half
        low[span, :] = (value - top_half.astype(jnp.float32)).astype(jnp.bfloat16)

    project(0, DEPTH * rows, weight * kept_mask)
    project(DEPTH * rows, DEPTH * rows, weight * kept_mask)
    project(2 * DEPTH * rows, rows, kept_mask)

    def product(n):
        lanes = pl.ds(pl.multiple_of(n * 256, 256), 256)
        dims = (((0,), (0,)), ((), ()))
        value = lax.dot_general(left[:, lanes], high[...], dims, preferred_element_type=jnp.float32)
        part_ref[lanes, :] = value + lax.dot_general(
            left[:, lanes], low[...], dims, preferred_element_type=jnp.float32
        )

    def products(start_tile):
        def step(n, carry):
            product(start_tile + n)
            return carry

        lax.fori_loop(0, states // 512, step, 0)

    def message(source, i, target, j, departure, k, device):
        return [
            remote(bufs[source].at[i], bufs[target].at[j], departures[departure].at[k, n], arrivals[target].at[j, n], device)
            for n, bufs in enumerate((levels, scales))
        ]

    def start(*args):
        for copy in message(*args):
            copy.start()

    def sent(*args):
        for copy in message(*args):
            copy.wait_send()

    def arrived(target, j):
        for copy in message(target, j, target, j, "give", 0, side):
            copy.wait_recv()

    def put(name, i, value):
        whole, scale = quantize(value)
        levels[name][i] = whole
        scales[name][i] = scale

    def get(name, i):
        return levels[name][i].astype(jnp.int32).astype(jnp.float32) * scales[name][i]

    def rows_of(p, e):
        kind = KINDS[p]
        start_chunk = (8 + 4 * e + kind) if kind < 8 else (4 * x + 2 * e + kind - 8)
        return pl.ds(pl.multiple_of(start_chunk * chunk, chunk), chunk)

    def halves_of(p, e):
        return pl.ds(pl.multiple_of((2 * e + KINDS[p] - 8) * chunk, chunk), chunk)

    def value(p, e):
        if KINDS[p] < 8:
            return part_ref[rows_of(p, e), :]
        return total_ref[halves_of(p, e), :]

    def give(j):
        put("give", j, part_ref[pl.ds(pl.multiple_of((4 * (1 - x) + j) * chunk, chunk), chunk), :])
        start("give", j, "take", j, "give", j, side)

    def gather(j):
        arrived("take", j)
        mine = part_ref[pl.ds(pl.multiple_of((4 * x + j) * chunk, chunk), chunk), :]
        total_ref[pl.ds(j * chunk, chunk), :] = mine + get("take", j)

    def finish(p, e):
        out_ref[rows_of(p, e), :] = get("final", 2 * p + e)
        if KINDS[p] >= 8:
            place_last = 2 * (KINDS[p] - 8) + e
            start("final", 2 * p + e, "last", place_last, "last", place_last, side)

    products(states // 512)

    @pl.when(leaf)
    def _():
        def send(p, e):
            i = 2 * p + e
            put("own", i, value(p, e))
            far = w if e == 0 else 1 - w
            start("own", i, "inner", FLOWS * far + i, "own", i, inner)

        for p in range(PAIRS):
            if p == 3:
                products(0)
                for j in range(4):
                    give(j)
                for j in range(4):
                    gather(j)
            send(p, 0)
            send(p, 1)
        for p in range(PAIRS):
            for e in range(2):
                arrived("final", 2 * p + e)
                finish(p, e)
        for i in range(FLOWS):
            sent("own", i, "inner", i, "own", i, inner)

    @pl.when(mid)
    def _():
        def relay(p):
            i = 2 * p + 1 - w
            arrived("inner", FLOWS + i)
            put("own", i, value(p, 1 - w) + get("inner", FLOWS + i))
            start("own", i, "inner", FLOWS + i, "own", i, other)

        def collect(p):
            i = 2 * p + w
            arrived("inner", i)
            near = value(p, w) + get("inner", i)
            arrived("inner", FLOWS + i)
            near = near + get("inner", FLOWS + i)
            if KINDS[p] < 8:
                put("own", i, near)
                start("own", i, "cross", p, "own", i, side)
            else:
                put("final", i, near)
                spread(p)

        def spread(p):
            i = 2 * p + w
            start("final", i, "final", i, "outward", i, outer)
            start("final", i, "final", i, "across", p, other)
            finish(p, w)

        def merge(p):
            i = 2 * p + w
            arrived("cross", p)
            put("final", i, get("own", i) + get("cross", p))
            spread(p)

        def forward(p):
            i = 2 * p + 1 - w
            arrived("final", i)
            start("final", i, "final", i, "outward", i, outer)
            finish(p, 1 - w)

        products(0)
        for j in range(4):
            give(j)
        for p in range(PAIRS + 3):
            if p == 3:
                for j in range(4):
                    gather(j)
            if p < PAIRS:
                relay(p)
            if 1 <= p <= PAIRS:
                collect(p - 1)
            if 2 <= p < PAIRS + 2 and KINDS[p - 2] < 8:
                merge(p - 2)
            if p >= 3:
                forward(p - 3)
        for p in range(PAIRS):
            i = 2 * p + 1 - w
            sent("own", i, "inner", i, "own", i, other)
            if KINDS[p] < 8:
                sent("own", 2 * p + w, "cross", p, "own", 2 * p + w, side)
            for e in range(2):
                sent("final", 2 * p + e, "final", 2 * p + e, "outward", 2 * p + e, outer)
            sent("final", 2 * p + w, "final", 2 * p + w, "across", p, other)

    for j in range(4):
        sent("give", j, "take", j, "give", j, side)
    for p in range(PAIRS):
        for e in range(2):
            if KINDS[p] < 8:
                continue
            place_last = 2 * (KINDS[p] - 8) + e
            arrived("last", place_last)
            start_chunk = 4 * (1 - x) + 2 * e + KINDS[p] - 8
            out_ref[pl.ds(pl.multiple_of(start_chunk * chunk, chunk), chunk), :] = get("last", place_last)
            sent("final", 2 * p + e, "last", place_last, "last", place_last, side)
    for v in range(WAVES):
        across(v).wait_send()
        to_twin(v).wait_send()
        to_twin_second(v).wait_send()
        to_side(v).wait_send()

    @pl.when(mid)
    def _():
        for v in range(WAVES):
            if v < PARTS:
                along(v, 0, other).wait_send()
                along(v, 1, outer).wait_send()
            else:
                along(v, 0, other if v < 2 * PARTS else outer).wait_send()

    @pl.when(leaf)
    def _():
        for v in range(PARTS):
            along(v, 0, inner).wait_send()


def reduced_image(own, blocks, guess, sizes, counts, target_map, top, bottom):
    rows, states = own.shape
    kept = guess.shape[1]
    chunk = states // 16
    lengths = (4, 4, FLOWS, 2 * FLOWS, FLOWS, PAIRS, 4)
    sem = pltpu.SemaphoreType.DMA
    half = own.dtype
    total = 2 * DEPTH * rows
    return pl.pallas_call(
        image_kernel,
        out_shape=jax.ShapeDtypeStruct((states, kept), jnp.float32),
        in_specs=[pl.BlockSpec(memory_space=pl.ANY)] * 5
        + [pl.BlockSpec(memory_space=pltpu.VMEM)]
        + [pl.BlockSpec(memory_space=pl.ANY)] * 2,
        out_specs=pl.BlockSpec(memory_space=pltpu.VMEM),
        scratch_shapes=[
            pltpu.VMEM((16 * PARTS, rows // PARTS, states), half),
            pltpu.VMEM((WAVES, rows // PARTS, states), half),
            pltpu.VMEM((WAVES, rows // PARTS, states), half),
            pltpu.VMEM((total, states), half),
            pltpu.VMEM((states, states), half),
            pltpu.VMEM((states, kept), half),
            pltpu.VMEM((total + rows, states), half),
            pltpu.VMEM((total + rows, kept), half),
            pltpu.VMEM((total + rows, kept), half),
        ]
        + [sem((WAVES,))] * 5
        + [sem((WAVES, 2))]
        + [sem((WAVES,))] * 4
        + [sem((7,))]
        + [pltpu.VMEM((n, chunk, kept), jnp.int16) for n in lengths]
        + [pltpu.VMEM((n, 1, kept), jnp.float32) for n in lengths]
        + [sem((n, 2)) for n in (4, 2 * FLOWS, FLOWS, PAIRS, 4)]
        + [sem((n, 2)) for n in (4, FLOWS, FLOWS, PAIRS, 4)]
        + [pltpu.VMEM((states, kept), jnp.float32), pltpu.VMEM((4 * chunk, kept), jnp.float32)]
        + [pltpu.SMEM(a.shape, jnp.int32) for a in (sizes, counts, target_map, top, bottom)],
        compiler_params=pltpu.CompilerParams(
            collective_id=1, has_side_effects=True, vmem_limit_bytes=48 * 1024 * 1024
        ),
        name="reduced_image",
    )(sizes, counts, target_map, top, bottom, own, blocks, guess)


def body(
    wavefunction,
    op_blocks,
    basis_guess,
    sector_sizes,
    kept_counts,
    target_map,
    noise_numerator,
    noise_denominator,
):
    state_count = wavefunction.shape[2]
    kept_width = basis_guess.shape[2]
    tile_rows = state_count // lax.axis_size("op")
    sec_index = lax.axis_index("sec")
    op_index = lax.axis_index("op")
    noise_weight = noise_numerator[0].astype(jnp.float32) / noise_denominator[0].astype(jnp.float32)
    sources = source_sectors(target_map)
    wanted_all = lax.dynamic_index_in_dim(sources, sec_index, 1, keepdims=False)[None, :]
    wanted = lax.dynamic_index_in_dim(wanted_all[0], op_index, 0, keepdims=False)
    states = jnp.arange(state_count, dtype=jnp.int32)
    own_size = lax.dynamic_index_in_dim(sector_sizes, sec_index, 0, keepdims=False)
    source_size = lax.dynamic_index_in_dim(sector_sizes, wanted, 0, keepdims=False)
    own_count = lax.dynamic_index_in_dim(kept_counts, sec_index, 0, keepdims=False)
    own_kept = jnp.arange(kept_width, dtype=jnp.int32) < own_count
    zero_half = jnp.zeros((), jnp.bfloat16)
    own_rows = jnp.where((states < own_size)[None, :], wavefunction[0], zero_half)
    blocks = op_blocks[0, 0]
    if lax.axis_size("op") == 2 * DEPTH and lax.axis_size("sec") == 4:
        full_image = reduced_image(
            wavefunction[0],
            blocks,
            basis_guess[0],
            sector_sizes,
            kept_counts,
            target_map,
            noise_numerator,
            noise_denominator,
        )
    else:
        moved = fetch_pieces(wavefunction, wanted_all)[0]
        moved = jnp.where((states < source_size)[None, :], moved, zero_half)
        perturbed = jnp.dot(moved, blocks, preferred_element_type=jnp.float32).astype(jnp.bfloat16)
        guess = jnp.where((states < own_size)[:, None], basis_guess[0], zero_half)
        perturbed_guess = noise_weight * jnp.dot(perturbed, guess, preferred_element_type=jnp.float32)
        own_guess = jnp.dot(own_rows, guess, preferred_element_type=jnp.float32)
        part = lax.dot_general(
            jnp.concatenate([perturbed, own_rows], axis=0).astype(jnp.float32),
            jnp.concatenate([perturbed_guess, own_guess], axis=0),
            (((0,), (0,)), ((), ())),
            precision=lax.Precision.HIGH,
        )
        part = jnp.where((states < own_size)[:, None] & own_kept[None, :], part, jnp.float32(0.0))
        full_image = sum_over_op(part)
    padding = jnp.where(own_kept, jnp.float32(0.0), jnp.float32(1.0))
    correlation = dot_ta(full_image, full_image) + padding[:, None] * jnp.eye(
        kept_width, dtype=jnp.float32
    )
    inverse = inverse_factor(correlation)
    new_basis = lax.dot_general(
        full_image, inverse, (((1,), (1,)), ((), ())), precision=lax.Precision.HIGH
    )
    kept_tile = (
        lax.dynamic_slice_in_dim(new_basis, op_index * tile_rows, tile_rows, 0)
        * float(state_count) ** 0.5
    )
    basis_half = new_basis.astype(jnp.bfloat16)
    mapped = jnp.dot(blocks, basis_half, preferred_element_type=jnp.float32).astype(jnp.bfloat16)
    source_basis = fetch_sector(basis_half, wanted)
    rotated = lax.dot_general(
        source_basis, mapped, (((0,), (0,)), ((), ())), preferred_element_type=jnp.float32
    )
    return (kept_tile[None], rotated[None, None])


def solution(mesh):
    placed = (
        P("sec", "op", None),
        P("op", "sec", None, None),
        P("sec", None, None),
        P(),
        P(),
        P(),
        P(),
        P(),
    )
    return jax.shard_map(
        body,
        mesh=mesh,
        in_specs=placed,
        out_specs=(P("sec", "op", None), P("op", "sec", None, None)),
        check_vma=False,
    )
```

```python
import jax
import jax.numpy as jnp
from jax import lax
from jax.experimental import pallas as pl
from jax.experimental.pallas import tpu as pltpu
from jax.sharding import PartitionSpec as P

LANES = 128
ROWS = 8
HIGHEST = lax.Precision.HIGHEST


def dot_ta(a, b):
    return lax.dot_general(
        a, b, (((0,), (0,)), ((), ())), precision=HIGHEST, preferred_element_type=jnp.float32
    )


def dot(a, b):
    return jnp.dot(a, b, precision=HIGHEST, preferred_element_type=jnp.float32)


def eliminate_tile(tile):
    count = LANES // ROWS
    row = lax.broadcasted_iota(jnp.int32, (ROWS, LANES), 0)
    lane = lax.broadcasted_iota(jnp.int32, (ROWS, LANES), 1)
    left = [tile[ROWS * q : ROWS * (q + 1), :] for q in range(count)]
    right = [jnp.where(lane == row + ROWS * q, 1.0, 0.0).astype(jnp.float32) for q in range(count)]
    for p in range(count):
        upper, lower = left[p], right[p]
        columns = [
            jnp.broadcast_to(upper[:, ROWS * p + j : ROWS * p + j + 1], (ROWS, LANES))
            for j in range(ROWS)
        ]
        for j in range(ROWS):
            scale = lax.rsqrt(jnp.broadcast_to(columns[j][j : j + 1, :], (ROWS, LANES)))
            factor = jnp.where(row > j, columns[j] * scale, 0.0)
            for k in range(j + 1, ROWS):
                own = jnp.broadcast_to(columns[k][j : j + 1, :], (ROWS, LANES)) * scale
                columns[k] = columns[k] - factor * own
            own_upper = jnp.broadcast_to(upper[j : j + 1, :], (ROWS, LANES)) * scale
            own_lower = jnp.broadcast_to(lower[j : j + 1, :], (ROWS, LANES)) * scale
            upper = jnp.where(row == j, own_upper, upper - factor * own_upper)
            lower = jnp.where(row == j, own_lower, lower - factor * own_lower)
        right[p] = lower
        if p + 1 < count:
            change = dot_ta(upper, jnp.concatenate([upper, lower], axis=1))
            for q in range(p + 1, count):
                part = change[ROWS * q : ROWS * (q + 1), :]
                left[q] = left[q] - part[:, :LANES]
                right[q] = right[q] - part[:, LANES:]
    return jnp.concatenate(right, axis=0)


def inverse_factor_kernel(matrix_ref, out_ref, work):
    size = matrix_ref.shape[0]
    blocks = size // LANES
    work[:, :size] = matrix_ref[...]
    work[:, size:] = (
        lax.broadcasted_iota(jnp.int32, (size, size), 0)
        == lax.broadcasted_iota(jnp.int32, (size, size), 1)
    ).astype(jnp.float32)

    def step(b, carry):
        rows = pl.ds(pl.multiple_of(b * LANES, LANES), LANES)
        inverse = eliminate_tile(work[rows, rows])
        panel = dot(inverse, work[rows, :])
        work[rows, :] = panel
        out_ref[rows, :] = panel[:, size:]

        def update(i, inner):
            below = pl.ds(pl.multiple_of(i * LANES, LANES), LANES)
            work[below, :] = work[below, :] - dot_ta(work[rows, below], work[rows, :])
            return inner

        lax.fori_loop(b + 1, blocks, update, 0)
        return carry

    lax.fori_loop(0, blocks, step, 0)


def inverse_factor(matrix):
    size = matrix.shape[0]
    return pl.pallas_call(
        inverse_factor_kernel,
        out_shape=jax.ShapeDtypeStruct((size, size), jnp.float32),
        in_specs=[pl.BlockSpec(memory_space=pltpu.VMEM)],
        out_specs=pl.BlockSpec(memory_space=pltpu.VMEM),
        scratch_shapes=[pltpu.VMEM((size, 2 * size), jnp.float32)],
        compiler_params=pltpu.CompilerParams(vmem_limit_bytes=24 * 1024 * 1024),
        cost_estimate=pl.CostEstimate(flops=2 * size**3, bytes_accessed=8 * size * size, transcendentals=size),
        name="inverse_factor",
    )(matrix)


def source_sectors(target_map):
    sectors = jnp.arange(target_map.shape[1], dtype=jnp.int32)
    matches = target_map[:, :, None] == sectors[None, None, :]
    return jnp.sum(jnp.where(matches, sectors[None, :, None], 0), axis=1)


def fetch_pieces(own_slice, wanted_all):
    everyone = lax.all_gather(own_slice, "sec", axis=0, tiled=True)
    outgoing = jnp.take(everyone, wanted_all, axis=0)
    incoming = lax.all_to_all(outgoing, "op", split_axis=1, concat_axis=1, tiled=True)
    return incoming.reshape(
        incoming.shape[0], incoming.shape[1] * incoming.shape[2], incoming.shape[3]
    )


def exchange(value, axis, bit):
    count = lax.axis_size(axis)
    return lax.ppermute(value, axis, [(i, i ^ bit) for i in range(count)])


def halves(value, side):
    half = value.shape[0] // 2
    kept = lax.dynamic_slice_in_dim(value, side * half, half, 0)
    given = lax.dynamic_slice_in_dim(value, (1 - side) * half, half, 0)
    return kept, given


def sum_over_op(value):
    count = lax.axis_size("op")
    index = lax.axis_index("op")
    bits = [1 << b for b in range(count.bit_length() - 1)]
    orders = [bits, bits[1:] + bits[:1]]
    half = value.shape[0] // 2
    held = [value[:half], value[half:]]
    for step in range(len(bits)):
        for color, order in enumerate(orders):
            kept, given = halves(held[color], (index // order[step]) % 2)
            held[color] = kept + exchange(given, "op", order[step])
    for step in reversed(range(len(bits))):
        for color, order in enumerate(orders):
            own = held[color]
            other = exchange(own, "op", order[step])
            first = (index // order[step]) % 2 == 0
            held[color] = jnp.concatenate(
                [jnp.where(first, own, other), jnp.where(first, other, own)], axis=0
            )
    return jnp.concatenate(held, axis=0)


def fetch_sector(own, wanted):
    count = lax.axis_size("sec")
    offset = lax.axis_index("sec") ^ wanted
    held = {0: own}
    bit = count // 2
    while bit:
        for known in list(held):
            held[known ^ bit] = exchange(held[known], "sec", bit)
        bit //= 2
    result = own
    for known, value in held.items():
        result = jnp.where(offset == known, value, result)
    return result


MESH = pl.DeviceIdType.MESH
DEPTH = 4
PAIRS = 6
KINDS = (0, 1, 2, 8, 9, 3)
FLOWS = 2 * PAIRS
PARTS = 2
WAVES = DEPTH * PARTS


def quantize(value):
    top = jnp.maximum(jnp.max(jnp.abs(value), axis=0, keepdims=True), jnp.float32(1e-30))
    levels = jnp.round(value * (jnp.float32(32766.0) / top))
    return levels.astype(jnp.int32).astype(jnp.int16), top * jnp.float32(1.0 / 32766.0)


def remote(source, target, send, receive, device):
    return pltpu.make_async_remote_copy(
        src_ref=source,
        dst_ref=target,
        send_sem=send,
        recv_sem=receive,
        device_id=device,
        device_id_type=MESH,
    )


def greet(device):
    pl.semaphore_signal(pltpu.get_barrier_semaphore(), inc=1, device_id=device, device_id_type=MESH)


def source_of(map_ref, op, sec):
    found = jnp.int32(0)
    for sector in range(map_ref.shape[1]):
        found = jnp.where(map_ref[op, sector] == sec, sector, found)
    return found


def before(limit, width, dtype):
    lane = lax.broadcasted_iota(jnp.int32, (1, width), 1)
    return jnp.where(lane < limit, 1.0, 0.0).astype(jnp.float32).astype(dtype)


def split(value, parts):
    pieces = []
    for _ in range(parts):
        piece = value.astype(jnp.bfloat16)
        value = value - piece.astype(jnp.float32)
        pieces.append(piece)
    return pieces


def left_terms(value, axis, parts=3):
    p = split(value, parts)
    order = (p[0], p[0], p[1]) if parts == 2 else (p[0], p[0], p[1], p[0], p[2], p[1])
    return jnp.concatenate(order, axis=axis)


def right_terms(value, axis, parts=3):
    p = split(value, parts)
    order = (p[0], p[1], p[0]) if parts == 2 else (p[0], p[1], p[0], p[2], p[0], p[1])
    return jnp.concatenate(order, axis=axis)


def contract(a, b, i, j):
    return lax.dot_general(a, b, (((i,), (j,)), ((), ())), preferred_element_type=jnp.float32)


def eliminate_pairs(tile):
    count = LANES // ROWS
    row = lax.broadcasted_iota(jnp.int32, (ROWS, LANES), 0)
    lane = lax.broadcasted_iota(jnp.int32, (ROWS, LANES), 1)
    left = [tile[ROWS * q : ROWS * (q + 1), :] for q in range(count)]
    right = [jnp.where(lane == row + ROWS * q, 1.0, 0.0).astype(jnp.float32) for q in range(count)]

    def lane_of(value, j):
        return jnp.broadcast_to(value[:, j : j + 1], (ROWS, LANES))

    def row_of(value, j):
        return jnp.broadcast_to(value[j : j + 1, :], (ROWS, LANES))

    for s in range(count // 2):
        base = 2 * ROWS * s
        ua, la, ub, lb = left[2 * s], right[2 * s], left[2 * s + 1], right[2 * s + 1]
        ca = [lane_of(ua, base + j) for j in range(ROWS)]
        cb = [lane_of(ub, base + j) for j in range(2 * ROWS)]
        for j in range(ROWS):
            scale = lax.rsqrt(row_of(ca[j], j))
            fa = jnp.where(row > j, ca[j] * scale, 0.0)
            fb = cb[j] * scale
            for k in range(j + 1, ROWS):
                own = row_of(ca[k], j) * scale
                ca[k] = ca[k] - fa * own
                cb[k] = cb[k] - fb * own
            for k in range(ROWS):
                cb[ROWS + k] = cb[ROWS + k] - fb * row_of(fb, k)
            own_u = row_of(ua, j) * scale
            own_l = row_of(la, j) * scale
            ua = jnp.where(row == j, own_u, ua - fa * own_u)
            la = jnp.where(row == j, own_l, la - fa * own_l)
            ub = ub - fb * own_u
            lb = lb - fb * own_l
        cb = cb[ROWS:]
        for j in range(ROWS):
            scale = lax.rsqrt(row_of(cb[j], j))
            fb = jnp.where(row > j, cb[j] * scale, 0.0)
            for k in range(j + 1, ROWS):
                cb[k] = cb[k] - fb * (row_of(cb[k], j) * scale)
            own_u = row_of(ub, j) * scale
            own_l = row_of(lb, j) * scale
            ub = jnp.where(row == j, own_u, ub - fb * own_u)
            lb = jnp.where(row == j, own_l, lb - fb * own_l)
        right[2 * s], right[2 * s + 1] = la, lb
        if 2 * s + 2 < count:
            upper = jnp.concatenate([ua, ub], axis=0)
            lower = jnp.concatenate([la, lb], axis=0)
            both = jnp.concatenate([right_terms(upper, 0), right_terms(lower, 0)], axis=1)
            change = contract(left_terms(upper, 0), both, 0, 0)
            for q in range(2 * s + 2, count):
                part = change[ROWS * q : ROWS * (q + 1), :]
                left[q] = left[q] - part[:, :LANES]
                right[q] = right[q] - part[:, LANES:]
    return jnp.concatenate(right, axis=0)


def image_kernel(sizes_hbm, counts_hbm, map_hbm, top_hbm, bottom_hbm, own_hbm, blocks_hbm, guess_hbm, tile_ref, rotated_ref, *refs):
    rows, states = own_hbm.shape
    kept = guess_hbm.shape[1]
    chunk = states // 16
    band = rows // PARTS
    sec = lax.axis_index("sec")
    op = lax.axis_index("op")
    y, c = sec // 2, sec % 2
    z, x = op // 2, op % 2
    w = z // 2
    zz = z + w * (3 - 2 * z)
    mid = zz == 1
    leaf = jnp.logical_not(mid)
    sec_over = (1 - y) * 2 + c
    sec_twin = y * 2 + 1 - c
    sec_cross = (1 - y) * 2 + 1 - c
    twin = (sec_twin, op)
    over = (sec_over, op)
    side = (sec, z * 2 + 1 - x)
    inner = (sec, (1 + w) * 2 + x)
    outer = (sec, 6 * w + x)
    other = (sec, (3 - z) * 2 + x)

    (store, picked, landed, moved, blocks, guess, left, high, low) = refs[:9]
    (line_in, side_in, core_in, cross_in, x_in, line_out, side_out, core_out, cross_out, x_out, load) = refs[9:20]
    refs = refs[20:]
    names = ("give", "take", "own", "inner", "final", "cross", "last")
    levels = dict(zip(names, refs[0:7]))
    scales = dict(zip(names, refs[7:14]))
    arrivals = dict(zip(("take", "inner", "final", "cross", "last"), refs[14:19]))
    departures = dict(zip(("give", "own", "outward", "across", "last"), refs[19:24]))
    part_ref, total_ref = refs[24:26]
    scalars = refs[26:31]
    own_ref, out_ref, work, near_terms, far_terms, basis, basis_mid, basis_full, mapped, q_in, q_out = refs[31:42]
    load_own = pltpu.make_async_copy(own_hbm, own_ref, load.at[7])
    load_own.start()
    sizes_ref, counts_ref, map_ref, top_ref, bottom_ref = scalars
    loads = [
        pltpu.make_async_copy(source, target, load.at[2 + i])
        for i, (source, target) in enumerate(zip((sizes_hbm, counts_hbm, map_hbm, top_hbm, bottom_hbm), scalars))
    ]
    for copy in loads:
        copy.start()

    load_blocks = pltpu.make_async_copy(blocks_hbm, blocks, load.at[0])
    load_guess = pltpu.make_async_copy(guess_hbm, guess, load.at[1])
    load_blocks.start()
    load_guess.start()
    barrier = pltpu.get_barrier_semaphore()
    greet(twin)
    greet(over)
    greet(side)

    @pl.when(mid)
    def _():
        greet(other)
        greet(outer)
        pl.semaphore_wait(barrier, 5)

    @pl.when(leaf)
    def _():
        greet(inner)
        pl.semaphore_wait(barrier, 4)

    for copy in loads:
        copy.wait()
    wanted = source_of(map_ref, op, sec)
    beside = source_of(map_ref, op + 1 - 2 * x, sec)
    source_mask = before(sizes_ref[wanted], states, jnp.bfloat16)
    own_size = sizes_ref[sec]
    own_mask = before(own_size, states, jnp.bfloat16)

    marks = [zz, 1 - zz, 2, 3]
    place = [q + w * (3 - 2 * q) for q in marks]

    def slot(v, sector):
        return store.at[(place[v // PARTS] * 4 + sector) * PARTS + v % PARTS]

    def piece(v):
        if v < PARTS:
            return own_ref.at[pl.ds(v * band, band)]
        return slot(v, sec)

    def line_sem(v):
        return line_in.at[place[v // PARTS] * PARTS + v % PARTS]

    def along(v, lane, device):
        return remote(piece(v), slot(v, sec), line_out.at[v, lane], line_sem(v), device)

    def across(v):
        return remote(piece(v), slot(v, sec), side_out.at[v], side_in.at[v], over)

    def to_twin(v):
        return remote(piece(v), slot(v, sec), core_out.at[v], core_in.at[v], twin)

    def to_twin_second(v):
        return remote(slot(v, sec_over), slot(v, sec_over), cross_out.at[v], cross_in.at[v], twin)

    def to_side(v):
        return remote(picked.at[v], landed.at[v], x_out.at[v], x_in.at[v], side)

    def first(v):
        step = v // PARTS
        if step == 0:

            @pl.when(mid)
            def _():
                along(v, 0, other).start()
                along(v, 1, outer).start()

            @pl.when(leaf)
            def _():
                along(v, 0, inner).start()
        else:
            remote(slot(v, sec), slot(v, sec), line_out.at[v, 0], line_sem(v), side).wait_recv()

            @pl.when(mid)
            def _():
                along(v, 0, other if step == 1 else outer).start()

        across(v).start()
        to_twin(v).start()

    def second(v):
        remote(slot(v, sec_over), slot(v, sec_over), side_out.at[v], side_in.at[v], over).wait_recv()
        to_twin_second(v).start()

    def choose(v, sector_wanted):
        base = place[v // PARTS] * 4
        value = store[(base + 3) * PARTS + v % PARTS]
        for sector in range(3):
            value = jnp.where(sector_wanted == sector, store[(base + sector) * PARTS + v % PARTS], value)
        return value

    def third(v):
        remote(slot(v, sec_twin), slot(v, sec_twin), core_out.at[v], core_in.at[v], twin).wait_recv()
        remote(slot(v, sec_cross), slot(v, sec_cross), core_out.at[v], cross_in.at[v], twin).wait_recv()
        picked[v] = choose(v, beside)
        to_side(v).start()
        moved[pl.ds(v * band, band), :] = choose(v, wanted) * source_mask

    def perturb(half):
        span = pl.ds(half * DEPTH * rows, DEPTH * rows)

        def step(n, carry):
            lanes = pl.ds(pl.multiple_of(n * 256, 256), 256)
            value = jnp.dot(moved[span, :], blocks[:, lanes], preferred_element_type=jnp.float32)
            lane = lax.broadcasted_iota(jnp.int32, (1, 256), 1) + n * 256
            keep = jnp.where(lane < own_size, 1.0, 0.0).astype(jnp.float32).astype(jnp.bfloat16)
            left[span, lanes] = value.astype(jnp.bfloat16) * keep
            return carry

        lax.fori_loop(0, states // 256, step, 0)

    load_own.wait()
    for v in range(PARTS):
        store[(place[0] * 4 + sec) * PARTS + v] = own_ref[pl.ds(v * band, band), :]
    left[pl.ds(2 * DEPTH * rows, rows), :] = own_ref[...] * own_mask
    for v in range(WAVES + 2):
        if v < WAVES:
            first(v)
        if 1 <= v <= WAVES:
            second(v - 1)
        if v >= 2:
            third(v - 2)
    load_blocks.wait()
    load_guess.wait()
    perturb(0)
    for v in range(WAVES):
        to_side(v).wait_recv()
        moved[pl.ds(DEPTH * rows + v * band, band), :] = landed[v] * source_mask
    perturb(1)
    weight = jnp.full((1, kept), top_ref[0], jnp.int32).astype(jnp.float32) / jnp.full(
        (1, kept), bottom_ref[0], jnp.int32
    ).astype(jnp.float32)
    kept_mask = before(counts_ref[sec], kept, jnp.float32)

    def project(first_row, count, factor):
        span = pl.ds(first_row, count)
        value = jnp.dot(left[span, :], guess[...], preferred_element_type=jnp.float32) * factor
        top_half = value.astype(jnp.bfloat16)
        high[span, :] = top_half
        low[span, :] = (value - top_half.astype(jnp.float32)).astype(jnp.bfloat16)

    project(0, DEPTH * rows, weight * kept_mask)
    project(DEPTH * rows, DEPTH * rows, weight * kept_mask)
    project(2 * DEPTH * rows, rows, kept_mask)

    def product(n):
        lanes = pl.ds(pl.multiple_of(n * 256, 256), 256)
        dims = (((0,), (0,)), ((), ()))
        value = lax.dot_general(left[:, lanes], high[...], dims, preferred_element_type=jnp.float32)
        part_ref[lanes, :] = value + lax.dot_general(
            left[:, lanes], low[...], dims, preferred_element_type=jnp.float32
        )

    def products(start_tile):
        def step(n, carry):
            product(start_tile + n)
            return carry

        lax.fori_loop(0, states // 512, step, 0)

    def message(source, i, target, j, departure, k, device):
        return [
            remote(bufs[source].at[i], bufs[target].at[j], departures[departure].at[k, n], arrivals[target].at[j, n], device)
            for n, bufs in enumerate((levels, scales))
        ]

    def start(*args):
        for copy in message(*args):
            copy.start()

    def sent(*args):
        for copy in message(*args):
            copy.wait_send()

    def arrived(target, j):
        for copy in message(target, j, target, j, "give", 0, side):
            copy.wait_recv()

    def put(name, i, value):
        whole, scale = quantize(value)
        levels[name][i] = whole
        scales[name][i] = scale

    def get(name, i):
        return levels[name][i].astype(jnp.int32).astype(jnp.float32) * scales[name][i]

    def rows_of(p, e):
        kind = KINDS[p]
        start_chunk = (8 + 4 * e + kind) if kind < 8 else (4 * x + 2 * e + kind - 8)
        return pl.ds(pl.multiple_of(start_chunk * chunk, chunk), chunk)

    def halves_of(p, e):
        return pl.ds(pl.multiple_of((2 * e + KINDS[p] - 8) * chunk, chunk), chunk)

    def value(p, e):
        if KINDS[p] < 8:
            return part_ref[rows_of(p, e), :]
        return total_ref[halves_of(p, e), :]

    def give(j):
        put("give", j, part_ref[pl.ds(pl.multiple_of((4 * (1 - x) + j) * chunk, chunk), chunk), :])
        start("give", j, "take", j, "give", j, side)

    def gather(j):
        arrived("take", j)
        mine = part_ref[pl.ds(pl.multiple_of((4 * x + j) * chunk, chunk), chunk), :]
        total_ref[pl.ds(j * chunk, chunk), :] = mine + get("take", j)

    def finish(p, e):
        out_ref[rows_of(p, e), :] = get("final", 2 * p + e)
        if KINDS[p] >= 8:
            place_last = 2 * (KINDS[p] - 8) + e
            start("final", 2 * p + e, "last", place_last, "last", place_last, side)

    products(states // 512)

    @pl.when(leaf)
    def _():
        def send(p, e):
            i = 2 * p + e
            put("own", i, value(p, e))
            far = w if e == 0 else 1 - w
            start("own", i, "inner", FLOWS * far + i, "own", i, inner)

        for p in range(PAIRS):
            if p == 3:
                products(0)
                for j in range(4):
                    give(j)
                for j in range(4):
                    gather(j)
            send(p, 0)
            send(p, 1)
        for p in range(PAIRS):
            for e in range(2):
                arrived("final", 2 * p + e)
                finish(p, e)
        for i in range(FLOWS):
            sent("own", i, "inner", i, "own", i, inner)

    @pl.when(mid)
    def _():
        def relay(p):
            i = 2 * p + 1 - w
            arrived("inner", FLOWS + i)
            put("own", i, value(p, 1 - w) + get("inner", FLOWS + i))
            start("own", i, "inner", FLOWS + i, "own", i, other)

        def collect(p):
            i = 2 * p + w
            arrived("inner", i)
            near = value(p, w) + get("inner", i)
            arrived("inner", FLOWS + i)
            near = near + get("inner", FLOWS + i)
            if KINDS[p] < 8:
                put("own", i, near)
                start("own", i, "cross", p, "own", i, side)
            else:
                put("final", i, near)
                spread(p)

        def spread(p):
            i = 2 * p + w
            start("final", i, "final", i, "outward", i, outer)
            start("final", i, "final", i, "across", p, other)
            finish(p, w)

        def merge(p):
            i = 2 * p + w
            arrived("cross", p)
            put("final", i, get("own", i) + get("cross", p))
            spread(p)

        def forward(p):
            i = 2 * p + 1 - w
            arrived("final", i)
            start("final", i, "final", i, "outward", i, outer)
            finish(p, 1 - w)

        products(0)
        for j in range(4):
            give(j)
        for p in range(PAIRS + 3):
            if p == 3:
                for j in range(4):
                    gather(j)
            if p < PAIRS:
                relay(p)
            if 1 <= p <= PAIRS:
                collect(p - 1)
            if 2 <= p < PAIRS + 2 and KINDS[p - 2] < 8:
                merge(p - 2)
            if p >= 3:
                forward(p - 3)
        for p in range(PAIRS):
            i = 2 * p + 1 - w
            sent("own", i, "inner", i, "own", i, other)
            if KINDS[p] < 8:
                sent("own", 2 * p + w, "cross", p, "own", 2 * p + w, side)
            for e in range(2):
                sent("final", 2 * p + e, "final", 2 * p + e, "outward", 2 * p + e, outer)
            sent("final", 2 * p + w, "final", 2 * p + w, "across", p, other)

    for j in range(4):
        sent("give", j, "take", j, "give", j, side)
    for p in range(PAIRS):
        for e in range(2):
            if KINDS[p] < 8:
                continue
            place_last = 2 * (KINDS[p] - 8) + e
            arrived("last", place_last)
            start_chunk = 4 * (1 - x) + 2 * e + KINDS[p] - 8
            out_ref[pl.ds(pl.multiple_of(start_chunk * chunk, chunk), chunk), :] = get("last", place_last)
            sent("final", 2 * p + e, "last", place_last, "last", place_last, side)
    for v in range(WAVES):
        across(v).wait_send()
        to_twin(v).wait_send()
        to_twin_second(v).wait_send()
        to_side(v).wait_send()

    @pl.when(mid)
    def _():
        for v in range(WAVES):
            if v < PARTS:
                along(v, 0, other).wait_send()
                along(v, 1, outer).wait_send()
            else:
                along(v, 0, other if v < 2 * PARTS else outer).wait_send()

    @pl.when(leaf)
    def _():
        for v in range(PARTS):
            along(v, 0, inner).wait_send()


    span = LANES
    blocks_count = kept // span
    tall = states // 4

    def correlate(n, carry):
        image = out_ref[pl.ds(pl.multiple_of(n * tall, tall), tall), :]
        change = contract(left_terms(image, 0), right_terms(image, 0), 0, 0)
        work[...] = work[...] + change
        return carry

    diagonal = lax.broadcasted_iota(jnp.int32, (kept, kept), 0) == lax.broadcasted_iota(jnp.int32, (kept, kept), 1)
    work[...] = jnp.where(diagonal, 1.0 - kept_mask, 0.0)
    lax.fori_loop(0, 4, correlate, 0)

    def q_over(b):
        return remote(basis.at[0, b], basis.at[1, b], q_out.at[0, b], q_in.at[0, b], over)

    def q_twin(b):
        return remote(basis.at[0, b], basis.at[2, b], q_out.at[1, b], q_in.at[1, b], twin)

    def q_cross(b):
        return remote(basis.at[1, b], basis.at[3, b], q_out.at[2, b], q_in.at[2, b], twin)

    def pass_on(b):
        q_over(b).wait_recv()
        q_cross(b).start()

    def factor_step(b, carry):
        lanes = pl.ds(pl.multiple_of(b * span, span), span)
        inverse = eliminate_pairs(work[lanes, lanes])
        panel = contract(left_terms(inverse, 1), right_terms(work[lanes, :], 0), 1, 0)
        inverse_terms = right_terms(inverse, 1, 2)
        panel_terms = right_terms(panel, 0, 2)
        near_terms[...] = left_terms(panel, 0)
        far_terms[...] = right_terms(panel, 0)

        def orthogonal(n, inner):
            some = pl.ds(pl.multiple_of(n * tall, tall), tall)
            columns = contract(left_terms(out_ref[some, lanes], 1, 2), inverse_terms, 1, 1)
            basis_full[some, :] = columns
            whole = columns.astype(jnp.bfloat16)
            basis[0, b, some, :] = whole
            basis_mid[some, :] = (columns - whole.astype(jnp.float32)).astype(jnp.bfloat16)
            return inner

        lax.fori_loop(0, 4, orthogonal, 0)
        q_over(b).start()
        q_twin(b).start()

        def update(i, inner):
            below = pl.ds(pl.multiple_of(i * span, span), span)
            work[below, :] = work[below, :] - contract(near_terms[:, below], far_terms[...], 0, 0)
            return inner

        lax.fori_loop(b + 1, blocks_count, update, 0)
        height = tile_ref.shape[0]
        mine = pl.ds(pl.multiple_of(op * height, height), height)
        tile_ref[:, lanes] = basis_full[mine, :] * float(states) ** 0.5

        def spread_out(n, inner):
            some = pl.ds(pl.multiple_of(n * tall, tall), tall)
            whole = basis[0, b, some, :]
            terms = jnp.concatenate([whole, whole, basis_mid[some, :]], axis=1)
            out_ref[some, :] = out_ref[some, :] - contract(terms, panel_terms, 1, 0)
            return inner

        @pl.when(b + 1 < blocks_count)
        def _():
            lax.fori_loop(0, 4, spread_out, 0)

        def apply(n, inner):
            some = pl.ds(pl.multiple_of(n * tall, tall), tall)
            mapped[some, lanes] = contract(blocks[some, :], basis[0, b], 1, 0).astype(jnp.bfloat16)
            return inner

        lax.fori_loop(0, 4, apply, 0)

        @pl.when(b > 0)
        def _():
            pass_on(b - 1)

        return carry

    lax.fori_loop(0, blocks_count, factor_step, 0)

    def rotate(b):
        q_twin(b).wait_recv()
        q_cross(b).wait_recv()
        value = basis[0, b]
        for n, sector in enumerate((sec_over, sec_twin, sec_cross)):
            value = jnp.where(wanted == sector, basis[n + 1, b], value)
        rotated_ref[pl.ds(b * span, span), :] = contract(value, mapped[...], 0, 0)

    for b in range(blocks_count - 1):
        rotate(b)
    pass_on(blocks_count - 1)
    rotate(blocks_count - 1)
    for b in range(blocks_count):
        q_over(b).wait_send()
        q_twin(b).wait_send()
        q_cross(b).wait_send()


def whole_kernel(own, blocks, guess, sizes, counts, target_map, top, bottom):
    rows, states = own.shape
    kept = guess.shape[1]
    chunk = states // 16
    lengths = (4, 4, FLOWS, 2 * FLOWS, FLOWS, PAIRS, 4)
    sem = pltpu.SemaphoreType.DMA
    half = own.dtype
    total = 2 * DEPTH * rows
    pieces = kept // LANES
    scratch = [
        pltpu.VMEM((16 * PARTS, rows // PARTS, states), half),
        pltpu.VMEM((WAVES, rows // PARTS, states), half),
        pltpu.VMEM((WAVES, rows // PARTS, states), half),
        pltpu.VMEM((total, states), half),
        pltpu.VMEM((states, states), half),
        pltpu.VMEM((states, kept), half),
        pltpu.VMEM((total + rows, states), half),
        pltpu.VMEM((total + rows, kept), half),
        pltpu.VMEM((total + rows, kept), half),
    ]
    scratch += [sem((WAVES,))] * 5 + [sem((WAVES, 2))] + [sem((WAVES,))] * 4 + [sem((8,))]
    scratch += [pltpu.VMEM((n, chunk, kept), jnp.int16) for n in lengths]
    scratch += [pltpu.VMEM((n, 1, kept), jnp.float32) for n in lengths]
    scratch += [sem((n, 2)) for n in (4, 2 * FLOWS, FLOWS, PAIRS, 4)]
    scratch += [sem((n, 2)) for n in (4, FLOWS, FLOWS, PAIRS, 4)]
    scratch += [pltpu.VMEM((states, kept), jnp.float32), pltpu.VMEM((4 * chunk, kept), jnp.float32)]
    scratch += [pltpu.SMEM(a.shape, jnp.int32) for a in (sizes, counts, target_map, top, bottom)]
    scratch += [
        pltpu.VMEM((rows, states), half),
        pltpu.VMEM((states, kept), jnp.float32),
        pltpu.VMEM((kept, kept), jnp.float32),
        pltpu.VMEM((6 * LANES, kept), half),
        pltpu.VMEM((6 * LANES, kept), half),
        pltpu.VMEM((4, pieces, states, LANES), half),
        pltpu.VMEM((states, LANES), half),
        pltpu.VMEM((states, LANES), jnp.float32),
        pltpu.VMEM((states, kept), half),
        sem((3, pieces)),
        sem((3, pieces)),
    ]
    return pl.pallas_call(
        image_kernel,
        out_shape=(
            jax.ShapeDtypeStruct((states // lax.axis_size("op"), kept), jnp.float32),
            jax.ShapeDtypeStruct((kept, kept), jnp.float32),
        ),
        in_specs=[pl.BlockSpec(memory_space=pltpu.HBM)] * 8,
        out_specs=[pl.BlockSpec(memory_space=pltpu.VMEM)] * 2,
        scratch_shapes=scratch,
        compiler_params=pltpu.CompilerParams(
            collective_id=1, has_side_effects=True, vmem_limit_bytes=60 * 1024 * 1024
        ),
        name="truncate_and_rotate",
    )(sizes, counts, target_map, top, bottom, own, blocks, guess)


def body(
    wavefunction,
    op_blocks,
    basis_guess,
    sector_sizes,
    kept_counts,
    target_map,
    noise_numerator,
    noise_denominator,
):
    if lax.axis_size("op") == 2 * DEPTH and lax.axis_size("sec") == 4:
        tile, rotated = whole_kernel(
            wavefunction[0],
            op_blocks[0, 0],
            basis_guess[0],
            sector_sizes,
            kept_counts,
            target_map,
            noise_numerator,
            noise_denominator,
        )
        return (tile[None], rotated[None, None])
    state_count = wavefunction.shape[2]
    kept_width = basis_guess.shape[2]
    tile_rows = state_count // lax.axis_size("op")
    sec_index = lax.axis_index("sec")
    op_index = lax.axis_index("op")
    noise_weight = noise_numerator[0].astype(jnp.float32) / noise_denominator[0].astype(jnp.float32)
    sources = source_sectors(target_map)
    wanted_all = lax.dynamic_index_in_dim(sources, sec_index, 1, keepdims=False)[None, :]
    wanted = lax.dynamic_index_in_dim(wanted_all[0], op_index, 0, keepdims=False)
    states = jnp.arange(state_count, dtype=jnp.int32)
    own_size = lax.dynamic_index_in_dim(sector_sizes, sec_index, 0, keepdims=False)
    source_size = lax.dynamic_index_in_dim(sector_sizes, wanted, 0, keepdims=False)
    own_count = lax.dynamic_index_in_dim(kept_counts, sec_index, 0, keepdims=False)
    own_kept = jnp.arange(kept_width, dtype=jnp.int32) < own_count
    zero_half = jnp.zeros((), jnp.bfloat16)
    own_rows = jnp.where((states < own_size)[None, :], wavefunction[0], zero_half)
    moved = fetch_pieces(wavefunction, wanted_all)[0]
    moved = jnp.where((states < source_size)[None, :], moved, zero_half)
    blocks = op_blocks[0, 0]
    perturbed = jnp.dot(moved, blocks, preferred_element_type=jnp.float32).astype(jnp.bfloat16)
    guess = jnp.where((states < own_size)[:, None], basis_guess[0], zero_half)
    perturbed_guess = noise_weight * jnp.dot(perturbed, guess, preferred_element_type=jnp.float32)
    own_guess = jnp.dot(own_rows, guess, preferred_element_type=jnp.float32)
    part = lax.dot_general(
        jnp.concatenate([perturbed, own_rows], axis=0).astype(jnp.float32),
        jnp.concatenate([perturbed_guess, own_guess], axis=0),
        (((0,), (0,)), ((), ())),
        precision=lax.Precision.HIGH,
    )
    part = jnp.where((states < own_size)[:, None] & own_kept[None, :], part, jnp.float32(0.0))
    full_image = sum_over_op(part)
    padding = jnp.where(own_kept, jnp.float32(0.0), jnp.float32(1.0))
    correlation = dot_ta(full_image, full_image) + padding[:, None] * jnp.eye(
        kept_width, dtype=jnp.float32
    )
    inverse = inverse_factor(correlation)
    new_basis = lax.dot_general(
        full_image, inverse, (((1,), (1,)), ((), ())), precision=lax.Precision.HIGH
    )
    kept_tile = (
        lax.dynamic_slice_in_dim(new_basis, op_index * tile_rows, tile_rows, 0)
        * float(state_count) ** 0.5
    )
    basis_half = new_basis.astype(jnp.bfloat16)
    mapped = jnp.dot(blocks, basis_half, preferred_element_type=jnp.float32).astype(jnp.bfloat16)
    source_basis = fetch_sector(basis_half, wanted)
    rotated = lax.dot_general(
        source_basis, mapped, (((0,), (0,)), ((), ())), preferred_element_type=jnp.float32
    )
    return (kept_tile[None], rotated[None, None])


def solution(mesh):
    placed = (
        P("sec", "op", None),
        P("op", "sec", None, None),
        P("sec", None, None),
        P(),
        P(),
        P(),
        P(),
        P(),
    )
    return jax.shard_map(
        body,
        mesh=mesh,
        in_specs=placed,
        out_specs=(P("sec", "op", None), P("op", "sec", None, None)),
        check_vma=False,
    )
```

```python
import jax
import jax.numpy as jnp
from jax import lax
from jax.experimental import pallas as pl
from jax.experimental.pallas import tpu as pltpu
from jax.sharding import PartitionSpec as P

LANES = 128
ROWS = 8
HIGHEST = lax.Precision.HIGHEST


def dot_ta(a, b):
    return lax.dot_general(
        a, b, (((0,), (0,)), ((), ())), precision=HIGHEST, preferred_element_type=jnp.float32
    )


def dot(a, b):
    return jnp.dot(a, b, precision=HIGHEST, preferred_element_type=jnp.float32)


def eliminate_tile(tile):
    count = LANES // ROWS
    row = lax.broadcasted_iota(jnp.int32, (ROWS, LANES), 0)
    lane = lax.broadcasted_iota(jnp.int32, (ROWS, LANES), 1)
    left = [tile[ROWS * q : ROWS * (q + 1), :] for q in range(count)]
    right = [jnp.where(lane == row + ROWS * q, 1.0, 0.0).astype(jnp.float32) for q in range(count)]
    for p in range(count):
        upper, lower = left[p], right[p]
        columns = [
            jnp.broadcast_to(upper[:, ROWS * p + j : ROWS * p + j + 1], (ROWS, LANES))
            for j in range(ROWS)
        ]
        for j in range(ROWS):
            scale = lax.rsqrt(jnp.broadcast_to(columns[j][j : j + 1, :], (ROWS, LANES)))
            factor = jnp.where(row > j, columns[j] * scale, 0.0)
            for k in range(j + 1, ROWS):
                own = jnp.broadcast_to(columns[k][j : j + 1, :], (ROWS, LANES)) * scale
                columns[k] = columns[k] - factor * own
            own_upper = jnp.broadcast_to(upper[j : j + 1, :], (ROWS, LANES)) * scale
            own_lower = jnp.broadcast_to(lower[j : j + 1, :], (ROWS, LANES)) * scale
            upper = jnp.where(row == j, own_upper, upper - factor * own_upper)
            lower = jnp.where(row == j, own_lower, lower - factor * own_lower)
        right[p] = lower
        if p + 1 < count:
            change = dot_ta(upper, jnp.concatenate([upper, lower], axis=1))
            for q in range(p + 1, count):
                part = change[ROWS * q : ROWS * (q + 1), :]
                left[q] = left[q] - part[:, :LANES]
                right[q] = right[q] - part[:, LANES:]
    return jnp.concatenate(right, axis=0)


def inverse_factor_kernel(matrix_ref, out_ref, work):
    size = matrix_ref.shape[0]
    blocks = size // LANES
    work[:, :size] = matrix_ref[...]
    work[:, size:] = (
        lax.broadcasted_iota(jnp.int32, (size, size), 0)
        == lax.broadcasted_iota(jnp.int32, (size, size), 1)
    ).astype(jnp.float32)

    def step(b, carry):
        rows = pl.ds(pl.multiple_of(b * LANES, LANES), LANES)
        inverse = eliminate_tile(work[rows, rows])
        panel = dot(inverse, work[rows, :])
        work[rows, :] = panel
        out_ref[rows, :] = panel[:, size:]

        def update(i, inner):
            below = pl.ds(pl.multiple_of(i * LANES, LANES), LANES)
            work[below, :] = work[below, :] - dot_ta(work[rows, below], work[rows, :])
            return inner

        lax.fori_loop(b + 1, blocks, update, 0)
        return carry

    lax.fori_loop(0, blocks, step, 0)


def inverse_factor(matrix):
    size = matrix.shape[0]
    return pl.pallas_call(
        inverse_factor_kernel,
        out_shape=jax.ShapeDtypeStruct((size, size), jnp.float32),
        in_specs=[pl.BlockSpec(memory_space=pltpu.VMEM)],
        out_specs=pl.BlockSpec(memory_space=pltpu.VMEM),
        scratch_shapes=[pltpu.VMEM((size, 2 * size), jnp.float32)],
        compiler_params=pltpu.CompilerParams(vmem_limit_bytes=24 * 1024 * 1024),
        cost_estimate=pl.CostEstimate(flops=2 * size**3, bytes_accessed=8 * size * size, transcendentals=size),
        name="inverse_factor",
    )(matrix)


def source_sectors(target_map):
    sectors = jnp.arange(target_map.shape[1], dtype=jnp.int32)
    matches = target_map[:, :, None] == sectors[None, None, :]
    return jnp.sum(jnp.where(matches, sectors[None, :, None], 0), axis=1)


def fetch_pieces(own_slice, wanted_all):
    everyone = lax.all_gather(own_slice, "sec", axis=0, tiled=True)
    outgoing = jnp.take(everyone, wanted_all, axis=0)
    incoming = lax.all_to_all(outgoing, "op", split_axis=1, concat_axis=1, tiled=True)
    return incoming.reshape(
        incoming.shape[0], incoming.shape[1] * incoming.shape[2], incoming.shape[3]
    )


def exchange(value, axis, bit):
    count = lax.axis_size(axis)
    return lax.ppermute(value, axis, [(i, i ^ bit) for i in range(count)])


def halves(value, side):
    half = value.shape[0] // 2
    kept = lax.dynamic_slice_in_dim(value, side * half, half, 0)
    given = lax.dynamic_slice_in_dim(value, (1 - side) * half, half, 0)
    return kept, given


def sum_over_op(value):
    count = lax.axis_size("op")
    index = lax.axis_index("op")
    bits = [1 << b for b in range(count.bit_length() - 1)]
    orders = [bits, bits[1:] + bits[:1]]
    half = value.shape[0] // 2
    held = [value[:half], value[half:]]
    for step in range(len(bits)):
        for color, order in enumerate(orders):
            kept, given = halves(held[color], (index // order[step]) % 2)
            held[color] = kept + exchange(given, "op", order[step])
    for step in reversed(range(len(bits))):
        for color, order in enumerate(orders):
            own = held[color]
            other = exchange(own, "op", order[step])
            first = (index // order[step]) % 2 == 0
            held[color] = jnp.concatenate(
                [jnp.where(first, own, other), jnp.where(first, other, own)], axis=0
            )
    return jnp.concatenate(held, axis=0)


def fetch_sector(own, wanted):
    count = lax.axis_size("sec")
    offset = lax.axis_index("sec") ^ wanted
    held = {0: own}
    bit = count // 2
    while bit:
        for known in list(held):
            held[known ^ bit] = exchange(held[known], "sec", bit)
        bit //= 2
    result = own
    for known, value in held.items():
        result = jnp.where(offset == known, value, result)
    return result


MESH = pl.DeviceIdType.MESH
DEPTH = 4
PAIRS = 8
LAG = 2
FLOWS = 2 * PAIRS
PARTS = 4
WAVES = DEPTH * PARTS


def steps(stage, step):
    return [(stage, step * PARTS + h) for h in range(PARTS)]


def mixed(*lists):
    return [item for group in zip(*lists) for item in group]


def leaf_order():
    order = steps(0, 0) + mixed(steps(1, 0), steps(0, 1)) + steps(2, 0)
    order += mixed(steps(1, 1), steps(0, 2)) + steps(2, 1) + steps(1, 2)
    return order + steps(0, 3) + steps(2, 2) + steps(1, 3) + steps(2, 3)


def mid_order():
    order = steps(0, 0) + steps(0, 1) + steps(0, 2) + steps(1, 0) + steps(2, 0) + steps(0, 3)
    return order + steps(1, 1) + mixed(steps(2, 1), steps(1, 2)) + mixed(steps(2, 2), steps(1, 3)) + steps(2, 3)


def quantize(value):
    top = jnp.maximum(jnp.max(jnp.abs(value), axis=0, keepdims=True), jnp.float32(1e-30))
    levels = jnp.round(value * (jnp.float32(32766.0) / top))
    return levels.astype(jnp.int32).astype(jnp.int16), top * jnp.float32(1.0 / 32766.0)


def remote(source, target, send, receive, device):
    return pltpu.make_async_remote_copy(
        src_ref=source,
        dst_ref=target,
        send_sem=send,
        recv_sem=receive,
        device_id=device,
        device_id_type=MESH,
    )


def greet(device):
    pl.semaphore_signal(pltpu.get_barrier_semaphore(), inc=1, device_id=device, device_id_type=MESH)


def source_of(map_ref, op, sec):
    found = jnp.int32(0)
    for sector in range(map_ref.shape[0]):
        found = jnp.where(map_ref[sector, op] == sec, sector, found)
    return found


def before(limit, width, dtype):
    lane = lax.broadcasted_iota(jnp.int32, (1, width), 1)
    return jnp.where(lane < limit, 1.0, 0.0).astype(jnp.float32).astype(dtype)


def split(value, parts):
    pieces = []
    for _ in range(parts):
        piece = value.astype(jnp.bfloat16)
        value = value - piece.astype(jnp.float32)
        pieces.append(piece)
    return pieces


def left_terms(value, axis, parts=3):
    p = split(value, parts)
    order = (p[0], p[0], p[1]) if parts == 2 else (p[0], p[0], p[1], p[0], p[2], p[1])
    return jnp.concatenate(order, axis=axis)


def right_terms(value, axis, parts=3):
    p = split(value, parts)
    order = (p[0], p[1], p[0]) if parts == 2 else (p[0], p[1], p[0], p[2], p[0], p[1])
    return jnp.concatenate(order, axis=axis)


def contract(a, b, i, j):
    return lax.dot_general(a, b, (((i,), (j,)), ((), ())), preferred_element_type=jnp.float32)


def eliminate_pairs(tile):
    count = LANES // ROWS
    row = lax.broadcasted_iota(jnp.int32, (ROWS, LANES), 0)
    lane = lax.broadcasted_iota(jnp.int32, (ROWS, LANES), 1)
    left = [tile[ROWS * q : ROWS * (q + 1), :] for q in range(count)]
    right = [jnp.where(lane == row + ROWS * q, 1.0, 0.0).astype(jnp.float32) for q in range(count)]

    def lane_of(value, j):
        return jnp.broadcast_to(value[:, j : j + 1], (ROWS, LANES))

    def row_of(value, j):
        return jnp.broadcast_to(value[j : j + 1, :], (ROWS, LANES))

    for s in range(count // 2):
        base = 2 * ROWS * s
        ua, la, ub, lb = left[2 * s], right[2 * s], left[2 * s + 1], right[2 * s + 1]
        ca = [lane_of(ua, base + j) for j in range(ROWS)]
        cb = [lane_of(ub, base + j) for j in range(2 * ROWS)]
        for j in range(ROWS):
            scale = lax.rsqrt(row_of(ca[j], j))
            fa = jnp.where(row > j, ca[j] * scale, 0.0)
            fb = cb[j] * scale
            for k in range(j + 1, ROWS):
                own = row_of(ca[k], j) * scale
                ca[k] = ca[k] - fa * own
                cb[k] = cb[k] - fb * own
            for k in range(ROWS):
                cb[ROWS + k] = cb[ROWS + k] - fb * row_of(fb, k)
            own_u = row_of(ua, j) * scale
            own_l = row_of(la, j) * scale
            ua = jnp.where(row == j, own_u, ua - fa * own_u)
            la = jnp.where(row == j, own_l, la - fa * own_l)
            ub = ub - fb * own_u
            lb = lb - fb * own_l
        cb = cb[ROWS:]
        for j in range(ROWS):
            scale = lax.rsqrt(row_of(cb[j], j))
            fb = jnp.where(row > j, cb[j] * scale, 0.0)
            for k in range(j + 1, ROWS):
                cb[k] = cb[k] - fb * (row_of(cb[k], j) * scale)
            own_u = row_of(ub, j) * scale
            own_l = row_of(lb, j) * scale
            ub = jnp.where(row == j, own_u, ub - fb * own_u)
            lb = jnp.where(row == j, own_l, lb - fb * own_l)
        right[2 * s], right[2 * s + 1] = la, lb
        if 2 * s + 2 < count:
            upper = jnp.concatenate([ua, ub], axis=0)
            lower = jnp.concatenate([la, lb], axis=0)
            both = jnp.concatenate([right_terms(upper, 0), right_terms(lower, 0)], axis=1)
            flipped = left_terms(upper, 0).T
            for first, last in ((2 * s + 2, 2 * s + 4), (2 * s + 4, count)):
                if first == last:
                    continue
                change = contract(flipped[ROWS * first : ROWS * last, :], both, 1, 0)
                for q in range(first, last):
                    part = change[ROWS * (q - first) : ROWS * (q - first + 1), :]
                    left[q] = left[q] - part[:, :LANES]
                    right[q] = right[q] - part[:, LANES:]
    return jnp.concatenate(right, axis=0)


def image_kernel(sizes_hbm, counts_hbm, map_hbm, top_hbm, bottom_hbm, own_hbm, blocks_hbm, guess_hbm, tile_ref, rotated_ref, *refs):
    rows, states = own_hbm.shape
    kept = guess_hbm.shape[1]
    chunk = states // (2 * FLOWS)
    band = rows // PARTS
    sec = lax.axis_index("sec")
    op = lax.axis_index("op")
    y, c = sec // 2, sec % 2
    z, x = op // 2, op % 2
    w = z // 2
    zz = z + w * (3 - 2 * z)
    mid = zz == 1
    leaf = jnp.logical_not(mid)
    sec_over = (1 - y) * 2 + c
    sec_twin = y * 2 + 1 - c
    sec_cross = (1 - y) * 2 + 1 - c
    twin = (sec_twin, op)
    over = (sec_over, op)
    side = (sec, z * 2 + 1 - x)
    inner = (sec, (1 + w) * 2 + x)
    outer = (sec, 6 * w + x)
    other = (sec, (3 - z) * 2 + x)

    (store, picked, landed, moved, blocks, guess, left, high, low) = refs[:9]
    (line_in, side_in, core_in, cross_in, x_in, fetch_out, load) = refs[9:16]
    refs = refs[16:]
    names = ("give", "take", "own", "inner", "final", "last")
    levels = dict(zip(names, refs[0:6]))
    scales = dict(zip(names, refs[6:12]))
    arrivals = dict(zip(("take", "inner", "final", "last"), refs[12:16]))
    departures, measure_ref, part_ref = refs[16:19]
    scalars = refs[19:24]
    own_ref, out_ref, work, near_terms, far_terms, basis, basis_mid, basis_full, mapped, panel_ref, q_in, q_out = refs[24:36]
    load_own = pltpu.make_async_copy(own_hbm, own_ref, load.at[7])
    load_own.start()
    sizes_ref, counts_ref, map_ref, top_ref, bottom_ref = scalars
    loads = [
        pltpu.make_async_copy(source, target, load.at[2 + i])
        for i, (source, target) in enumerate(zip((sizes_hbm, counts_hbm, map_hbm, top_hbm, bottom_hbm), scalars))
    ]
    for copy in loads:
        copy.start()

    load_blocks = pltpu.make_async_copy(blocks_hbm, blocks, load.at[0])
    load_guess = pltpu.make_async_copy(guess_hbm, guess, load.at[1])
    load_blocks.start()
    load_guess.start()
    barrier = pltpu.get_barrier_semaphore()
    greet(twin)
    greet(over)
    greet(side)

    @pl.when(mid)
    def _():
        greet(other)
        greet(outer)
        pl.semaphore_wait(barrier, 5)

    @pl.when(leaf)
    def _():
        greet(inner)
        pl.semaphore_wait(barrier, 4)

    for copy in loads:
        copy.wait()
    wanted = source_of(map_ref, op, sec)
    beside = source_of(map_ref, op + 1 - 2 * x, sec)
    source_mask = before(sizes_ref[wanted], states, jnp.bfloat16)
    own_size = sizes_ref[sec]
    own_mask = before(own_size, states, jnp.bfloat16)

    marks = [zz, 1 - zz, 2, 3]
    place = [q + w * (3 - 2 * q) for q in marks]

    def slot(v, sector):
        return store.at[(place[v // PARTS] * 4 + sector) * PARTS + v % PARTS]

    def piece(v):
        if v < PARTS:
            return own_ref.at[pl.ds(v * band, band)]
        return slot(v, sec)

    def line_sem(v):
        return line_in.at[place[v // PARTS] * PARTS + v % PARTS]

    def along(v, device):
        return remote(piece(v), slot(v, sec), fetch_out.at[0], line_sem(v), device)

    def across(v):
        return remote(piece(v), slot(v, sec), fetch_out.at[1], side_in.at[v], over)

    def to_twin(v):
        return remote(piece(v), slot(v, sec), fetch_out.at[1], core_in.at[v], twin)

    def to_twin_second(v):
        return remote(slot(v, sec_over), slot(v, sec_over), fetch_out.at[1], cross_in.at[v], twin)

    def to_side(v):
        return remote(picked.at[v], landed.at[v], fetch_out.at[1], x_in.at[v], side)

    def first(v):
        step = v // PARTS
        if step == 0:

            @pl.when(mid)
            def _():
                along(v, other).start()
                along(v, outer).start()

            @pl.when(leaf)
            def _():
                along(v, inner).start()
        else:
            remote(slot(v, sec), slot(v, sec), fetch_out.at[0], line_sem(v), side).wait_recv()

            @pl.when(mid)
            def _():
                along(v, other if step == 1 else outer).start()

        across(v).start()
        to_twin(v).start()

    def second(v):
        remote(slot(v, sec_over), slot(v, sec_over), fetch_out.at[1], side_in.at[v], over).wait_recv()
        to_twin_second(v).start()

    def choose(v, sector_wanted):
        base = place[v // PARTS] * 4
        value = store[(base + 3) * PARTS + v % PARTS]
        for sector in range(3):
            value = jnp.where(sector_wanted == sector, store[(base + sector) * PARTS + v % PARTS], value)
        return value

    def third(v):
        remote(slot(v, sec_twin), slot(v, sec_twin), fetch_out.at[1], core_in.at[v], twin).wait_recv()
        remote(slot(v, sec_cross), slot(v, sec_cross), fetch_out.at[1], cross_in.at[v], twin).wait_recv()
        picked[v] = choose(v, beside)
        to_side(v).start()
        moved[pl.ds(v * band, band), :] = choose(v, wanted) * source_mask

    def perturb(half):
        span = pl.ds(half * DEPTH * rows, DEPTH * rows)

        def step(n, carry):
            lanes = pl.ds(pl.multiple_of(n * 256, 256), 256)
            value = jnp.dot(moved[span, :], blocks[:, lanes], preferred_element_type=jnp.float32)
            lane = lax.broadcasted_iota(jnp.int32, (1, 256), 1) + n * 256
            keep = jnp.where(lane < own_size, 1.0, 0.0).astype(jnp.float32).astype(jnp.bfloat16)
            left[span, lanes] = value.astype(jnp.bfloat16) * keep
            return carry

        lax.fori_loop(0, states // 256, step, 0)

    load_own.wait()
    for v in range(PARTS):
        store[(place[0] * 4 + sec) * PARTS + v] = own_ref[pl.ds(v * band, band), :]
    left[pl.ds(2 * DEPTH * rows, rows), :] = own_ref[...] * own_mask
    def run(order):
        for stage, v in order:
            (first, second, third)[stage](v)

    @pl.when(leaf)
    def _():
        run(leaf_order())

    @pl.when(mid)
    def _():
        run(mid_order())

    load_blocks.wait()
    load_guess.wait()
    perturb(0)
    for v in range(WAVES):
        to_side(v).wait_recv()
        moved[pl.ds(DEPTH * rows + v * band, band), :] = landed[v] * source_mask
    perturb(1)
    weight = jnp.full((1, kept), top_ref[0], jnp.int32).astype(jnp.float32) / jnp.full(
        (1, kept), bottom_ref[0], jnp.int32
    ).astype(jnp.float32)
    kept_mask = before(counts_ref[sec], kept, jnp.float32)

    def project(first_row, count, factor):
        span = pl.ds(first_row, count)
        value = jnp.dot(left[span, :], guess[...], preferred_element_type=jnp.float32) * factor
        top_half = value.astype(jnp.bfloat16)
        high[span, :] = top_half
        low[span, :] = (value - top_half.astype(jnp.float32)).astype(jnp.bfloat16)

    project(0, DEPTH * rows, weight * kept_mask)
    project(DEPTH * rows, DEPTH * rows, weight * kept_mask)
    project(2 * DEPTH * rows, rows, kept_mask)

    def product(n):
        lanes = pl.ds(pl.multiple_of(n * 256, 256), 256)
        dims = (((0,), (0,)), ((), ()))
        value = lax.dot_general(left[:, lanes], high[...], dims, preferred_element_type=jnp.float32)
        part_ref[lanes, :] = value + lax.dot_general(
            left[:, lanes], low[...], dims, preferred_element_type=jnp.float32
        )

    def start(source, i, target, j, lane, device):
        for n, bufs in enumerate((levels, scales)):
            remote(
                bufs[source].at[i], bufs[target].at[j], departures.at[lane, n], arrivals[target].at[j], device
            ).start()

    def arrived(target, j):
        remote(measure_ref, measure_ref, departures.at[0, 0], arrivals[target].at[j], side).wait_recv()

    def put(name, i, value):
        whole, scale = quantize(value)
        levels[name][i] = whole
        scales[name][i] = scale

    def get(name, i):
        return levels[name][i].astype(jnp.int32).astype(jnp.float32) * scales[name][i]

    def chunk_rows(half, i):
        return pl.ds(pl.multiple_of((FLOWS * half + i) * chunk, chunk), chunk)

    def value(i):
        arrived("take", i)
        return part_ref[chunk_rows(x, i), :] + get("take", i)

    def finish(i):
        start("final", i, "last", i, 0, side)
        out_ref[chunk_rows(x, i), :] = get("final", i)

    tiles = states // 256
    for n in range(tiles // 2):
        product((1 - x) * (tiles // 2) + n)
        for i in range(n * FLOWS // (tiles // 2), (n + 1) * FLOWS // (tiles // 2)):
            put("give", i, part_ref[chunk_rows(1 - x, i), :])
            start("give", i, "take", i, 0, side)
    for n in range(tiles // 2):
        product(x * (tiles // 2) + n)

    @pl.when(leaf)
    def _():
        for i in range(FLOWS):
            put("own", i, value(i))
            far = w if i % 2 == 0 else 1 - w
            start("own", i, "inner", FLOWS * far + i, 1, inner)
        for i in range(FLOWS):
            arrived("final", i)
            finish(i)

    @pl.when(mid)
    def _():
        def relay(p):
            i = 2 * p + 1 - w
            mine = value(i)
            arrived("inner", FLOWS + i)
            put("own", i, mine + get("inner", FLOWS + i))
            start("own", i, "inner", FLOWS + i, 1, other)

        def collect(p):
            i = 2 * p + w
            near = value(i)
            arrived("inner", i)
            near = near + get("inner", i)
            arrived("inner", FLOWS + i)
            put("final", i, near + get("inner", FLOWS + i))
            start("final", i, "final", i, 1, outer)
            start("final", i, "final", i, 1, other)
            finish(i)

        def forward(p):
            i = 2 * p + 1 - w
            arrived("final", i)
            start("final", i, "final", i, 1, outer)
            finish(i)

        for p in range(PAIRS + 2 * LAG):
            if p < PAIRS:
                relay(p)
            if LAG <= p < PAIRS + LAG:
                collect(p - LAG)
            if p >= 2 * LAG:
                forward(p - 2 * LAG)

    span = LANES
    blocks_count = kept // span
    tall = states // 4

    def correlate(n, carry):
        image = out_ref[pl.ds(pl.multiple_of(n * tall, tall), tall), :]
        terms = left_terms(image, 0)
        others = right_terms(image, 0)
        middle = kept // 2
        work[:middle, :] = work[:middle, :] + contract(terms[:, :middle], others, 0, 0)
        work[middle:, middle:] = work[middle:, middle:] + contract(terms[:, middle:], others[:, middle:], 0, 0)
        return carry

    diagonal = lax.broadcasted_iota(jnp.int32, (kept, kept), 0) == lax.broadcasted_iota(jnp.int32, (kept, kept), 1)
    work[...] = jnp.where(diagonal, 1.0 - kept_mask, 0.0)
    def correlate_half(half):
        def step(n, carry):
            return correlate(2 * half + n, carry)

        lax.fori_loop(0, 2, step, 0)

    correlate_half(x)
    for i in range(FLOWS):
        arrived("last", i)
        out_ref[chunk_rows(1 - x, i), :] = get("last", i)
    correlate_half(1 - x)

    def q_over(b):
        return remote(basis.at[0, b], basis.at[1, b], q_out, q_in.at[0, b], over)

    def q_twin(b):
        return remote(basis.at[0, b], basis.at[2, b], q_out, q_in.at[1, b], twin)

    def q_cross(b):
        return remote(basis.at[1, b], basis.at[3, b], q_out, q_in.at[2, b], twin)

    def pass_on(b):
        q_over(b).wait_recv()
        q_cross(b).start()

    def factor_step(b, carry):
        lanes = pl.ds(pl.multiple_of(b * span, span), span)
        inverse = eliminate_pairs(work[lanes, lanes])
        panel = contract(left_terms(inverse, 1), right_terms(work[lanes, :], 0), 1, 0)
        inverse_terms = right_terms(inverse, 1, 2)
        panel_ref[...] = right_terms(panel, 0, 2)
        near_terms[...] = left_terms(panel, 0)
        far_terms[...] = right_terms(panel, 0)

        def orthogonal(n, inner):
            some = pl.ds(pl.multiple_of(n * tall, tall), tall)
            columns = contract(left_terms(out_ref[some, lanes], 1, 2), inverse_terms, 1, 1)
            basis_full[some, :] = columns
            whole = columns.astype(jnp.bfloat16)
            basis[0, b, some, :] = whole
            basis_mid[some, :] = (columns - whole.astype(jnp.float32)).astype(jnp.bfloat16)
            return inner

        lax.fori_loop(0, 4, orthogonal, 0)
        q_over(b).start()
        q_twin(b).start()

        def update(i, inner):
            below = pl.ds(pl.multiple_of(i * span, span), span)

            def part(n, deeper):
                wide = pl.ds(pl.multiple_of(n * 2 * span, 2 * span), 2 * span)
                work[below, wide] = work[below, wide] - contract(near_terms[:, below], far_terms[:, wide], 0, 0)
                return deeper

            return lax.fori_loop(i // 2, blocks_count // 2, part, inner)

        lax.fori_loop(b + 1, blocks_count, update, 0)
        height = tile_ref.shape[0]
        mine = pl.ds(pl.multiple_of(op * height, height), height)
        tile_ref[:, lanes] = basis_full[mine, :] * float(states) ** 0.5

        def spread_out(n, inner):
            wide = pl.ds(pl.multiple_of(n * 2 * span, 2 * span), 2 * span)

            def part(m, deeper):
                some = pl.ds(pl.multiple_of(m * tall, tall), tall)
                whole = basis[0, b, some, :]
                terms = jnp.concatenate([whole, whole, basis_mid[some, :]], axis=1)
                out_ref[some, wide] = out_ref[some, wide] - contract(terms, panel_ref[:, wide], 1, 0)
                return deeper

            return lax.fori_loop(0, 4, part, inner)

        lax.fori_loop((b + 1) // 2, blocks_count // 2, spread_out, 0)

        @pl.when(b > 0)
        def _():
            pass_on(b - 1)

        return carry

    lax.fori_loop(0, blocks_count, factor_step, 0)

    def rotate(b):
        q_twin(b).wait_recv()
        q_cross(b).wait_recv()
        value = basis[0, b]
        for n, sector in enumerate((sec_over, sec_twin, sec_cross)):
            value = jnp.where(wanted == sector, basis[n + 1, b], value)
        rotated_ref[pl.ds(b * span, span), :] = contract(value, mapped[...], 0, 0)

    def apply(n, carry):
        some = pl.ds(pl.multiple_of(n * tall, tall), tall)
        columns = jnp.concatenate([basis[0, b] for b in range(blocks_count)], axis=1)
        mapped[some, :] = contract(blocks[some, :], columns, 1, 0).astype(jnp.bfloat16)
        return carry

    lax.fori_loop(0, 4, apply, 0)
    for b in range(blocks_count - 1):
        rotate(b)
    pass_on(blocks_count - 1)
    rotate(blocks_count - 1)

    def sent(ref, sem):
        remote(ref, ref, sem, x_in.at[0], side).wait_send()

    sent(basis.at[pl.ds(0, 3)], q_out)
    sent(store, fetch_out.at[1])
    for n, bufs in enumerate((levels, scales)):
        sent(bufs["inner"], departures.at[0, n])

    @pl.when(mid)
    def _():
        sent(store.at[pl.ds(0, PARTS + WAVES)], fetch_out.at[0])
        for n, bufs in enumerate((levels, scales)):
            sent(bufs["inner"], departures.at[1, n])

    @pl.when(leaf)
    def _():
        sent(store.at[pl.ds(0, PARTS)], fetch_out.at[0])
        for n, bufs in enumerate((levels, scales)):
            sent(bufs["inner"].at[pl.ds(0, FLOWS)], departures.at[1, n])


def whole_kernel(own, blocks, guess, sizes, counts, target_map, top, bottom):
    rows, states = own.shape
    kept = guess.shape[1]
    chunk = states // (2 * FLOWS)
    lengths = (FLOWS, FLOWS, FLOWS, 2 * FLOWS, FLOWS, FLOWS)
    sem = pltpu.SemaphoreType.DMA
    half = own.dtype
    total = 2 * DEPTH * rows
    pieces = kept // LANES
    scratch = [
        pltpu.VMEM((16 * PARTS, rows // PARTS, states), half),
        pltpu.VMEM((WAVES, rows // PARTS, states), half),
        pltpu.VMEM((WAVES, rows // PARTS, states), half),
        pltpu.VMEM((total, states), half),
        pltpu.VMEM((states, states), half),
        pltpu.VMEM((states, kept), half),
        pltpu.VMEM((total + rows, states), half),
        pltpu.VMEM((total + rows, kept), half),
        pltpu.VMEM((total + rows, kept), half),
    ]
    scratch += [sem((WAVES,))] * 5 + [sem((2,)), sem((8,))]
    scratch += [pltpu.VMEM((n, chunk, kept), jnp.int16) for n in lengths]
    scratch += [pltpu.VMEM((n, 1, kept), jnp.float32) for n in lengths]
    scratch += [sem((n,)) for n in (FLOWS, 2 * FLOWS, FLOWS, FLOWS)]
    scratch += [sem((2, 2)), pltpu.VMEM((1, chunk * kept // 2 + kept), jnp.float32), pltpu.VMEM((states, kept), jnp.float32)]
    scratch += [pltpu.SMEM(a.shape, jnp.int32) for a in (sizes, counts, target_map, top, bottom)]
    scratch += [
        pltpu.VMEM((rows, states), half),
        pltpu.VMEM((states, kept), jnp.float32),
        pltpu.VMEM((kept, kept), jnp.float32),
        pltpu.VMEM((6 * LANES, kept), half),
        pltpu.VMEM((6 * LANES, kept), half),
        pltpu.VMEM((4, pieces, states, LANES), half),
        pltpu.VMEM((states, LANES), half),
        pltpu.VMEM((states, LANES), jnp.float32),
        pltpu.VMEM((states, kept), half),
        pltpu.VMEM((3 * LANES, kept), half),
        sem((3, pieces)),
        sem,
    ]
    return pl.pallas_call(
        image_kernel,
        out_shape=(
            jax.ShapeDtypeStruct((states // lax.axis_size("op"), kept), jnp.float32),
            jax.ShapeDtypeStruct((kept, kept), jnp.float32),
        ),
        in_specs=[pl.BlockSpec(memory_space=pltpu.HBM)] * 8,
        out_specs=[pl.BlockSpec(memory_space=pltpu.VMEM)] * 2,
        scratch_shapes=scratch,
        compiler_params=pltpu.CompilerParams(
            collective_id=1, has_side_effects=True, vmem_limit_bytes=60 * 1024 * 1024
        ),
        name="truncate_and_rotate",
    )(sizes, counts, target_map, top, bottom, own, blocks, guess)


def body(
    wavefunction,
    op_blocks,
    basis_guess,
    sector_sizes,
    kept_counts,
    target_map,
    noise_numerator,
    noise_denominator,
):
    if lax.axis_size("op") == 2 * DEPTH and lax.axis_size("sec") == 4:
        tile, rotated = whole_kernel(
            wavefunction[0],
            op_blocks[0, 0],
            basis_guess[0],
            sector_sizes,
            kept_counts,
            target_map.T,
            noise_numerator,
            noise_denominator,
        )
        return (tile[None], rotated[None, None])
    state_count = wavefunction.shape[2]
    kept_width = basis_guess.shape[2]
    tile_rows = state_count // lax.axis_size("op")
    sec_index = lax.axis_index("sec")
    op_index = lax.axis_index("op")
    noise_weight = noise_numerator[0].astype(jnp.float32) / noise_denominator[0].astype(jnp.float32)
    sources = source_sectors(target_map)
    wanted_all = lax.dynamic_index_in_dim(sources, sec_index, 1, keepdims=False)[None, :]
    wanted = lax.dynamic_index_in_dim(wanted_all[0], op_index, 0, keepdims=False)
    states = jnp.arange(state_count, dtype=jnp.int32)
    own_size = lax.dynamic_index_in_dim(sector_sizes, sec_index, 0, keepdims=False)
    source_size = lax.dynamic_index_in_dim(sector_sizes, wanted, 0, keepdims=False)
    own_count = lax.dynamic_index_in_dim(kept_counts, sec_index, 0, keepdims=False)
    own_kept = jnp.arange(kept_width, dtype=jnp.int32) < own_count
    zero_half = jnp.zeros((), jnp.bfloat16)
    own_rows = jnp.where((states < own_size)[None, :], wavefunction[0], zero_half)
    moved = fetch_pieces(wavefunction, wanted_all)[0]
    moved = jnp.where((states < source_size)[None, :], moved, zero_half)
    blocks = op_blocks[0, 0]
    perturbed = jnp.dot(moved, blocks, preferred_element_type=jnp.float32).astype(jnp.bfloat16)
    guess = jnp.where((states < own_size)[:, None], basis_guess[0], zero_half)
    perturbed_guess = noise_weight * jnp.dot(perturbed, guess, preferred_element_type=jnp.float32)
    own_guess = jnp.dot(own_rows, guess, preferred_element_type=jnp.float32)
    part = lax.dot_general(
        jnp.concatenate([perturbed, own_rows], axis=0).astype(jnp.float32),
        jnp.concatenate([perturbed_guess, own_guess], axis=0),
        (((0,), (0,)), ((), ())),
        precision=lax.Precision.HIGH,
    )
    part = jnp.where((states < own_size)[:, None] & own_kept[None, :], part, jnp.float32(0.0))
    full_image = sum_over_op(part)
    padding = jnp.where(own_kept, jnp.float32(0.0), jnp.float32(1.0))
    correlation = dot_ta(full_image, full_image) + padding[:, None] * jnp.eye(
        kept_width, dtype=jnp.float32
    )
    inverse = inverse_factor(correlation)
    new_basis = lax.dot_general(
        full_image, inverse, (((1,), (1,)), ((), ())), precision=lax.Precision.HIGH
    )
    kept_tile = (
        lax.dynamic_slice_in_dim(new_basis, op_index * tile_rows, tile_rows, 0)
        * float(state_count) ** 0.5
    )
    basis_half = new_basis.astype(jnp.bfloat16)
    mapped = jnp.dot(blocks, basis_half, preferred_element_type=jnp.float32).astype(jnp.bfloat16)
    source_basis = fetch_sector(basis_half, wanted)
    rotated = lax.dot_general(
        source_basis, mapped, (((0,), (0,)), ((), ())), preferred_element_type=jnp.float32
    )
    return (kept_tile[None], rotated[None, None])


def solution(mesh):
    placed = (
        P("sec", "op", None),
        P("op", "sec", None, None),
        P("sec", None, None),
        P(),
        P(),
        P(),
        P(),
        P(),
    )
    return jax.shard_map(
        body,
        mesh=mesh,
        in_specs=placed,
        out_specs=(P("sec", "op", None), P("op", "sec", None, None)),
        check_vma=False,
    )
```

```python
import jax
import jax.numpy as jnp
from jax import lax
from jax.experimental import pallas as pl
from jax.experimental.pallas import tpu as pltpu
from jax.sharding import PartitionSpec as P

LANES = 128
ROWS = 8
HIGHEST = lax.Precision.HIGHEST


def dot_ta(a, b):
    return lax.dot_general(
        a, b, (((0,), (0,)), ((), ())), precision=HIGHEST, preferred_element_type=jnp.float32
    )


def dot(a, b):
    return jnp.dot(a, b, precision=HIGHEST, preferred_element_type=jnp.float32)


def eliminate_tile(tile):
    count = LANES // ROWS
    row = lax.broadcasted_iota(jnp.int32, (ROWS, LANES), 0)
    lane = lax.broadcasted_iota(jnp.int32, (ROWS, LANES), 1)
    left = [tile[ROWS * q : ROWS * (q + 1), :] for q in range(count)]
    right = [jnp.where(lane == row + ROWS * q, 1.0, 0.0).astype(jnp.float32) for q in range(count)]
    for p in range(count):
        upper, lower = left[p], right[p]
        columns = [
            jnp.broadcast_to(upper[:, ROWS * p + j : ROWS * p + j + 1], (ROWS, LANES))
            for j in range(ROWS)
        ]
        for j in range(ROWS):
            scale = lax.rsqrt(jnp.broadcast_to(columns[j][j : j + 1, :], (ROWS, LANES)))
            factor = jnp.where(row > j, columns[j] * scale, 0.0)
            for k in range(j + 1, ROWS):
                own = jnp.broadcast_to(columns[k][j : j + 1, :], (ROWS, LANES)) * scale
                columns[k] = columns[k] - factor * own
            own_upper = jnp.broadcast_to(upper[j : j + 1, :], (ROWS, LANES)) * scale
            own_lower = jnp.broadcast_to(lower[j : j + 1, :], (ROWS, LANES)) * scale
            upper = jnp.where(row == j, own_upper, upper - factor * own_upper)
            lower = jnp.where(row == j, own_lower, lower - factor * own_lower)
        right[p] = lower
        if p + 1 < count:
            change = dot_ta(upper, jnp.concatenate([upper, lower], axis=1))
            for q in range(p + 1, count):
                part = change[ROWS * q : ROWS * (q + 1), :]
                left[q] = left[q] - part[:, :LANES]
                right[q] = right[q] - part[:, LANES:]
    return jnp.concatenate(right, axis=0)


def inverse_factor_kernel(matrix_ref, out_ref, work):
    size = matrix_ref.shape[0]
    blocks = size // LANES
    work[:, :size] = matrix_ref[...]
    work[:, size:] = (
        lax.broadcasted_iota(jnp.int32, (size, size), 0)
        == lax.broadcasted_iota(jnp.int32, (size, size), 1)
    ).astype(jnp.float32)

    def step(b, carry):
        rows = pl.ds(pl.multiple_of(b * LANES, LANES), LANES)
        inverse = eliminate_tile(work[rows, rows])
        panel = dot(inverse, work[rows, :])
        work[rows, :] = panel
        out_ref[rows, :] = panel[:, size:]

        def update(i, inner):
            below = pl.ds(pl.multiple_of(i * LANES, LANES), LANES)
            work[below, :] = work[below, :] - dot_ta(work[rows, below], work[rows, :])
            return inner

        lax.fori_loop(b + 1, blocks, update, 0)
        return carry

    lax.fori_loop(0, blocks, step, 0)


def inverse_factor(matrix):
    size = matrix.shape[0]
    return pl.pallas_call(
        inverse_factor_kernel,
        out_shape=jax.ShapeDtypeStruct((size, size), jnp.float32),
        in_specs=[pl.BlockSpec(memory_space=pltpu.VMEM)],
        out_specs=pl.BlockSpec(memory_space=pltpu.VMEM),
        scratch_shapes=[pltpu.VMEM((size, 2 * size), jnp.float32)],
        compiler_params=pltpu.CompilerParams(vmem_limit_bytes=24 * 1024 * 1024),
        cost_estimate=pl.CostEstimate(flops=2 * size**3, bytes_accessed=8 * size * size, transcendentals=size),
        name="inverse_factor",
    )(matrix)


def source_sectors(target_map):
    sectors = jnp.arange(target_map.shape[1], dtype=jnp.int32)
    matches = target_map[:, :, None] == sectors[None, None, :]
    return jnp.sum(jnp.where(matches, sectors[None, :, None], 0), axis=1)


def fetch_pieces(own_slice, wanted_all):
    everyone = lax.all_gather(own_slice, "sec", axis=0, tiled=True)
    outgoing = jnp.take(everyone, wanted_all, axis=0)
    incoming = lax.all_to_all(outgoing, "op", split_axis=1, concat_axis=1, tiled=True)
    return incoming.reshape(
        incoming.shape[0], incoming.shape[1] * incoming.shape[2], incoming.shape[3]
    )


def exchange(value, axis, bit):
    count = lax.axis_size(axis)
    return lax.ppermute(value, axis, [(i, i ^ bit) for i in range(count)])


def halves(value, side):
    half = value.shape[0] // 2
    kept = lax.dynamic_slice_in_dim(value, side * half, half, 0)
    given = lax.dynamic_slice_in_dim(value, (1 - side) * half, half, 0)
    return kept, given


def sum_over_op(value):
    count = lax.axis_size("op")
    index = lax.axis_index("op")
    bits = [1 << b for b in range(count.bit_length() - 1)]
    orders = [bits, bits[1:] + bits[:1]]
    half = value.shape[0] // 2
    held = [value[:half], value[half:]]
    for step in range(len(bits)):
        for color, order in enumerate(orders):
            kept, given = halves(held[color], (index // order[step]) % 2)
            held[color] = kept + exchange(given, "op", order[step])
    for step in reversed(range(len(bits))):
        for color, order in enumerate(orders):
            own = held[color]
            other = exchange(own, "op", order[step])
            first = (index // order[step]) % 2 == 0
            held[color] = jnp.concatenate(
                [jnp.where(first, own, other), jnp.where(first, other, own)], axis=0
            )
    return jnp.concatenate(held, axis=0)


def fetch_sector(own, wanted):
    count = lax.axis_size("sec")
    offset = lax.axis_index("sec") ^ wanted
    held = {0: own}
    bit = count // 2
    while bit:
        for known in list(held):
            held[known ^ bit] = exchange(held[known], "sec", bit)
        bit //= 2
    result = own
    for known, value in held.items():
        result = jnp.where(offset == known, value, result)
    return result


MESH = pl.DeviceIdType.MESH
DEPTH = 4
PAIRS = 8
LAG = 2
AHEAD = 8
FLOWS = 2 * PAIRS
PARTS = 4
WAVES = DEPTH * PARTS


def steps(stage, step):
    return [(stage, step * PARTS + h) for h in range(PARTS)]


def mixed(*lists):
    return [item for group in zip(*lists) for item in group]


def leaf_order():
    order = steps(0, 0) + mixed(steps(1, 0), steps(0, 1)) + steps(2, 0)
    order += mixed(steps(1, 1), steps(0, 2)) + steps(2, 1) + steps(1, 2)
    return order + steps(0, 3) + steps(2, 2) + steps(1, 3) + steps(2, 3)


def mid_order():
    order = steps(0, 0) + steps(0, 1) + steps(0, 2) + steps(1, 0) + steps(2, 0) + steps(0, 3)
    return order + steps(1, 1) + mixed(steps(2, 1), steps(1, 2)) + mixed(steps(2, 2), steps(1, 3)) + steps(2, 3)


def quantize(value):
    top = jnp.maximum(jnp.max(jnp.abs(value), axis=0, keepdims=True), jnp.float32(1e-30))
    levels = jnp.round(value * (jnp.float32(32766.0) / top))
    return levels.astype(jnp.int32).astype(jnp.int16), top * jnp.float32(1.0 / 32766.0)


def remote(source, target, send, receive, device):
    return pltpu.make_async_remote_copy(
        src_ref=source,
        dst_ref=target,
        send_sem=send,
        recv_sem=receive,
        device_id=device,
        device_id_type=MESH,
    )


def greet(device):
    pl.semaphore_signal(pltpu.get_barrier_semaphore(), inc=1, device_id=device, device_id_type=MESH)


def source_of(map_ref, op, sec):
    found = jnp.int32(0)
    for sector in range(map_ref.shape[0]):
        found = jnp.where(map_ref[sector, op] == sec, sector, found)
    return found


def before(limit, width, dtype):
    lane = lax.broadcasted_iota(jnp.int32, (1, width), 1)
    return jnp.where(lane < limit, 1.0, 0.0).astype(jnp.float32).astype(dtype)


def split(value, parts):
    pieces = []
    for _ in range(parts):
        piece = value.astype(jnp.bfloat16)
        value = value - piece.astype(jnp.float32)
        pieces.append(piece)
    return pieces


def left_terms(value, axis, parts=3):
    p = split(value, parts)
    order = (p[0], p[0], p[1]) if parts == 2 else (p[0], p[0], p[1], p[0], p[2], p[1])
    return jnp.concatenate(order, axis=axis)


def right_terms(value, axis, parts=3):
    p = split(value, parts)
    order = (p[0], p[1], p[0]) if parts == 2 else (p[0], p[1], p[0], p[2], p[0], p[1])
    return jnp.concatenate(order, axis=axis)


def contract(a, b, i, j):
    return lax.dot_general(a, b, (((i,), (j,)), ((), ())), preferred_element_type=jnp.float32)


def eliminate_pairs(tile):
    count = LANES // ROWS
    row = lax.broadcasted_iota(jnp.int32, (ROWS, LANES), 0)
    lane = lax.broadcasted_iota(jnp.int32, (ROWS, LANES), 1)
    left = [tile[ROWS * q : ROWS * (q + 1), :] for q in range(count)]
    right = [jnp.where(lane == row + ROWS * q, 1.0, 0.0).astype(jnp.float32) for q in range(count)]

    def lane_of(value, j):
        return jnp.broadcast_to(value[:, j : j + 1], (ROWS, LANES))

    def row_of(value, j):
        return jnp.broadcast_to(value[j : j + 1, :], (ROWS, LANES))

    for s in range(count // 2):
        base = 2 * ROWS * s
        ua, la, ub, lb = left[2 * s], right[2 * s], left[2 * s + 1], right[2 * s + 1]
        ca = [lane_of(ua, base + j) for j in range(ROWS)]
        cb = [lane_of(ub, base + j) for j in range(2 * ROWS)]
        for j in range(ROWS):
            scale = lax.rsqrt(row_of(ca[j], j))
            fa = jnp.where(row > j, ca[j] * scale, 0.0)
            fb = cb[j] * scale
            for k in range(j + 1, ROWS):
                own = row_of(ca[k], j) * scale
                ca[k] = ca[k] - fa * own
                cb[k] = cb[k] - fb * own
            for k in range(ROWS):
                cb[ROWS + k] = cb[ROWS + k] - fb * row_of(fb, k)
            own_u = row_of(ua, j) * scale
            own_l = row_of(la, j) * scale
            ua = jnp.where(row == j, own_u, ua - fa * own_u)
            la = jnp.where(row == j, own_l, la - fa * own_l)
            ub = ub - fb * own_u
            lb = lb - fb * own_l
        cb = cb[ROWS:]
        for j in range(ROWS):
            scale = lax.rsqrt(row_of(cb[j], j))
            fb = jnp.where(row > j, cb[j] * scale, 0.0)
            for k in range(j + 1, ROWS):
                cb[k] = cb[k] - fb * (row_of(cb[k], j) * scale)
            own_u = row_of(ub, j) * scale
            own_l = row_of(lb, j) * scale
            ub = jnp.where(row == j, own_u, ub - fb * own_u)
            lb = jnp.where(row == j, own_l, lb - fb * own_l)
        right[2 * s], right[2 * s + 1] = la, lb
        if 2 * s + 2 < count:
            upper = jnp.concatenate([ua, ub], axis=0)
            lower = jnp.concatenate([la, lb], axis=0)
            both = jnp.concatenate([right_terms(upper, 0), right_terms(lower, 0)], axis=1)
            flipped = left_terms(upper, 0).T
            for first, last in ((2 * s + 2, 2 * s + 4), (2 * s + 4, count)):
                if first == last:
                    continue
                change = contract(flipped[ROWS * first : ROWS * last, :], both, 1, 0)
                for q in range(first, last):
                    part = change[ROWS * (q - first) : ROWS * (q - first + 1), :]
                    left[q] = left[q] - part[:, :LANES]
                    right[q] = right[q] - part[:, LANES:]
    return jnp.concatenate(right, axis=0)


def image_kernel(sizes_hbm, counts_hbm, map_hbm, top_hbm, bottom_hbm, own_hbm, blocks_hbm, guess_hbm, tile_ref, rotated_ref, *refs):
    rows, states = own_hbm.shape
    kept = guess_hbm.shape[1]
    chunk = states // (2 * FLOWS)
    band = rows // PARTS
    sec = lax.axis_index("sec")
    op = lax.axis_index("op")
    y, c = sec // 2, sec % 2
    z, x = op // 2, op % 2
    w = z // 2
    zz = z + w * (3 - 2 * z)
    mid = zz == 1
    leaf = jnp.logical_not(mid)
    sec_over = (1 - y) * 2 + c
    sec_twin = y * 2 + 1 - c
    sec_cross = (1 - y) * 2 + 1 - c
    twin = (sec_twin, op)
    over = (sec_over, op)
    side = (sec, z * 2 + 1 - x)
    inner = (sec, (1 + w) * 2 + x)
    outer = (sec, 6 * w + x)
    other = (sec, (3 - z) * 2 + x)

    (store, picked, landed, moved, blocks, guess, left, high, low) = refs[:9]
    (line_in, side_in, core_in, cross_in, x_in, fetch_out, load) = refs[9:16]
    refs = refs[16:]
    names = ("give", "take", "own", "inner", "final", "last")
    levels = dict(zip(names, refs[0:6]))
    scales = dict(zip(names, refs[6:12]))
    arrivals = dict(zip(("take", "inner", "final", "last"), refs[12:16]))
    departures, measure_ref, part_ref = refs[16:19]
    scalars = refs[19:24]
    own_ref, out_ref, work, near_terms, far_terms, basis, basis_mid, basis_full, mapped, panel_ref, q_in, q_out = refs[24:36]
    load_own = pltpu.make_async_copy(own_hbm, own_ref, load.at[7])
    load_own.start()
    sizes_ref, counts_ref, map_ref, top_ref, bottom_ref = scalars
    loads = [
        pltpu.make_async_copy(source, target, load.at[2 + i])
        for i, (source, target) in enumerate(zip((sizes_hbm, counts_hbm, map_hbm, top_hbm, bottom_hbm), scalars))
    ]
    for copy in loads:
        copy.start()

    load_blocks = pltpu.make_async_copy(blocks_hbm, blocks, load.at[0])
    load_guess = pltpu.make_async_copy(guess_hbm, guess, load.at[1])
    load_blocks.start()
    load_guess.start()
    barrier = pltpu.get_barrier_semaphore()
    greet(twin)
    greet(over)
    greet(side)

    @pl.when(mid)
    def _():
        greet(other)
        greet(outer)
        pl.semaphore_wait(barrier, 5)

    @pl.when(leaf)
    def _():
        greet(inner)
        pl.semaphore_wait(barrier, 4)

    for copy in loads:
        copy.wait()
    wanted = source_of(map_ref, op, sec)
    beside = source_of(map_ref, op + 1 - 2 * x, sec)
    source_mask = before(sizes_ref[wanted], states, jnp.bfloat16)
    own_size = sizes_ref[sec]
    own_mask = before(own_size, states, jnp.bfloat16)

    marks = [zz, 1 - zz, 2, 3]
    place = [q + w * (3 - 2 * q) for q in marks]

    def slot(v, sector):
        return store.at[(place[v // PARTS] * 4 + sector) * PARTS + v % PARTS]

    def piece(v):
        if v < PARTS:
            return own_ref.at[pl.ds(v * band, band)]
        return slot(v, sec)

    def line_sem(v):
        return line_in.at[place[v // PARTS] * PARTS + v % PARTS]

    def along(v, device):
        return remote(piece(v), slot(v, sec), fetch_out.at[0], line_sem(v), device)

    def across(v):
        return remote(piece(v), slot(v, sec), fetch_out.at[1], side_in.at[v], over)

    def to_twin(v):
        return remote(piece(v), slot(v, sec), fetch_out.at[1], core_in.at[v], twin)

    def to_twin_second(v):
        return remote(slot(v, sec_over), slot(v, sec_over), fetch_out.at[1], cross_in.at[v], twin)

    def to_side(v):
        return remote(picked.at[v], landed.at[v], fetch_out.at[1], x_in.at[v], side)

    def first(v):
        step = v // PARTS
        if step == 0:

            @pl.when(mid)
            def _():
                along(v, other).start()
                along(v, outer).start()

            @pl.when(leaf)
            def _():
                along(v, inner).start()
        else:
            remote(slot(v, sec), slot(v, sec), fetch_out.at[0], line_sem(v), side).wait_recv()

            @pl.when(mid)
            def _():
                along(v, other if step == 1 else outer).start()

        across(v).start()
        to_twin(v).start()

    def second(v):
        remote(slot(v, sec_over), slot(v, sec_over), fetch_out.at[1], side_in.at[v], over).wait_recv()
        to_twin_second(v).start()

    def choose(v, sector_wanted):
        base = place[v // PARTS] * 4
        value = store[(base + 3) * PARTS + v % PARTS]
        for sector in range(3):
            value = jnp.where(sector_wanted == sector, store[(base + sector) * PARTS + v % PARTS], value)
        return value

    def third(v):
        remote(slot(v, sec_twin), slot(v, sec_twin), fetch_out.at[1], core_in.at[v], twin).wait_recv()
        remote(slot(v, sec_cross), slot(v, sec_cross), fetch_out.at[1], cross_in.at[v], twin).wait_recv()
        picked[v] = choose(v, beside)
        to_side(v).start()
        moved[pl.ds(v * band, band), :] = choose(v, wanted) * source_mask

    def perturb(half):
        span = pl.ds(half * DEPTH * rows, DEPTH * rows)

        def step(n, carry):
            lanes = pl.ds(pl.multiple_of(n * 256, 256), 256)
            value = jnp.dot(moved[span, :], blocks[:, lanes], preferred_element_type=jnp.float32)
            lane = lax.broadcasted_iota(jnp.int32, (1, 256), 1) + n * 256
            keep = jnp.where(lane < own_size, 1.0, 0.0).astype(jnp.float32).astype(jnp.bfloat16)
            left[span, lanes] = value.astype(jnp.bfloat16) * keep
            return carry

        lax.fori_loop(0, states // 256, step, 0)

    load_own.wait()
    for v in range(PARTS):
        store[(place[0] * 4 + sec) * PARTS + v] = own_ref[pl.ds(v * band, band), :]
    left[pl.ds(2 * DEPTH * rows, rows), :] = own_ref[...] * own_mask
    def run(order):
        for stage, v in order:
            (first, second, third)[stage](v)

    @pl.when(leaf)
    def _():
        run(leaf_order())

    @pl.when(mid)
    def _():
        run(mid_order())

    load_blocks.wait()
    load_guess.wait()
    perturb(0)
    weight = jnp.full((1, kept), top_ref[0], jnp.int32).astype(jnp.float32) / jnp.full(
        (1, kept), bottom_ref[0], jnp.int32
    ).astype(jnp.float32)
    kept_mask = before(counts_ref[sec], kept, jnp.float32)

    def project(first_row, count, factor):
        span = pl.ds(first_row, count)
        value = jnp.dot(left[span, :], guess[...], preferred_element_type=jnp.float32) * factor
        top_half = value.astype(jnp.bfloat16)
        high[span, :] = top_half
        low[span, :] = (value - top_half.astype(jnp.float32)).astype(jnp.bfloat16)

    project(0, DEPTH * rows, weight * kept_mask)
    project(2 * DEPTH * rows, rows, kept_mask)
    for v in range(WAVES):
        to_side(v).wait_recv()
        moved[pl.ds(DEPTH * rows + v * band, band), :] = landed[v] * source_mask
    perturb(1)
    project(DEPTH * rows, DEPTH * rows, weight * kept_mask)

    def product(n):
        lanes = pl.ds(pl.multiple_of(n * 256, 256), 256)
        dims = (((0,), (0,)), ((), ()))
        value = lax.dot_general(left[:, lanes], high[...], dims, preferred_element_type=jnp.float32)
        part_ref[lanes, :] = value + lax.dot_general(
            left[:, lanes], low[...], dims, preferred_element_type=jnp.float32
        )

    def start(source, i, target, j, lane, device):
        for n, bufs in enumerate((levels, scales)):
            remote(
                bufs[source].at[i], bufs[target].at[j], departures.at[lane, n], arrivals[target].at[j], device
            ).start()

    def arrived(target, j):
        remote(measure_ref, measure_ref, departures.at[0, 0], arrivals[target].at[j], side).wait_recv()

    def put(name, i, value):
        whole, scale = quantize(value)
        levels[name][i] = whole
        scales[name][i] = scale

    def get(name, i):
        return levels[name][i].astype(jnp.int32).astype(jnp.float32) * scales[name][i]

    def chunk_rows(half, i):
        return pl.ds(pl.multiple_of((FLOWS * half + i) * chunk, chunk), chunk)

    def value(i):
        arrived("take", i)
        return part_ref[chunk_rows(x, i), :] + get("take", i)

    def finish(i):
        start("final", i, "last", i, 0, side)
        out_ref[chunk_rows(x, i), :] = get("final", i)

    def give(i):
        put("give", i, part_ref[chunk_rows(1 - x, i), :])
        start("give", i, "take", i, 0, side)

    tiles = states // 256
    for n in range(tiles // 2):
        product((1 - x) * (tiles // 2) + n)
        if n == 0:
            for i in range(AHEAD):
                give(i)
    for n in range(tiles // 2):
        product(x * (tiles // 2) + n)

    span = LANES
    blocks_count = kept // span
    tall = states // 4

    def correlate(n, carry):
        image = out_ref[pl.ds(pl.multiple_of(n * tall, tall), tall), :]
        terms = left_terms(image, 0)
        others = right_terms(image, 0)
        middle = kept // 2
        work[:middle, :] = work[:middle, :] + contract(terms[:, :middle], others, 0, 0)
        work[middle:, middle:] = work[middle:, middle:] + contract(terms[:, middle:], others[:, middle:], 0, 0)
        return carry

    diagonal = lax.broadcasted_iota(jnp.int32, (kept, kept), 0) == lax.broadcasted_iota(jnp.int32, (kept, kept), 1)
    work[...] = jnp.where(diagonal, 1.0 - kept_mask, 0.0)

    @pl.when(leaf)
    def _():
        for i in range(FLOWS):
            if i + AHEAD < FLOWS:
                give(i + AHEAD)
            put("own", i, value(i))
            far = w if i % 2 == 0 else 1 - w
            start("own", i, "inner", FLOWS * far + i, 1, inner)
        for i in range(FLOWS):
            arrived("final", i)
            finish(i)
            if i == FLOWS // 2 + 1:
                correlate(2 * x, 0)

    @pl.when(mid)
    def _():
        def relay(p):
            i = 2 * p + 1 - w
            mine = value(i)
            arrived("inner", FLOWS + i)
            put("own", i, mine + get("inner", FLOWS + i))
            start("own", i, "inner", FLOWS + i, 1, other)

        def collect(p):
            i = 2 * p + w
            near = value(i)
            arrived("inner", i)
            near = near + get("inner", i)
            arrived("inner", FLOWS + i)
            put("final", i, near + get("inner", FLOWS + i))
            start("final", i, "final", i, 1, outer)
            start("final", i, "final", i, 1, other)
            finish(i)

        def forward(p):
            i = 2 * p + 1 - w
            arrived("final", i)
            start("final", i, "final", i, 1, outer)
            finish(i)

        for p in range(PAIRS + 2 * LAG):
            if p < PAIRS:
                for i in range(2 * p + AHEAD, min(2 * p + AHEAD + 2, FLOWS)):
                    give(i)
                relay(p)
            if LAG <= p < PAIRS + LAG:
                collect(p - LAG)
            if p >= 2 * LAG:
                forward(p - 2 * LAG)
            if p == PAIRS // 2 + 2 * LAG:
                correlate(2 * x, 0)


    correlate(2 * x + 1, 0)
    for n in range(2):
        for i in range(n * FLOWS // 2, (n + 1) * FLOWS // 2):
            arrived("last", i)
            out_ref[chunk_rows(1 - x, i), :] = get("last", i)
        correlate(2 * (1 - x) + n, 0)

    def q_over(b):
        return remote(basis.at[0, b], basis.at[1, b], q_out, q_in.at[0, b], over)

    def q_twin(b):
        return remote(basis.at[0, b], basis.at[2, b], q_out, q_in.at[1, b], twin)

    def q_cross(b):
        return remote(basis.at[1, b], basis.at[3, b], q_out, q_in.at[2, b], twin)

    def pass_on(b):
        q_over(b).wait_recv()
        q_cross(b).start()

    def factor_step(b, carry):
        lanes = pl.ds(pl.multiple_of(b * span, span), span)
        inverse = eliminate_pairs(work[lanes, lanes])
        panel = contract(left_terms(inverse, 1), right_terms(work[lanes, :], 0), 1, 0)
        inverse_terms = right_terms(inverse, 1, 2)
        panel_ref[...] = right_terms(panel, 0, 2)
        near_terms[...] = left_terms(panel, 0)
        far_terms[...] = right_terms(panel, 0)

        def orthogonal(n, inner):
            some = pl.ds(pl.multiple_of(n * tall, tall), tall)
            columns = contract(left_terms(out_ref[some, lanes], 1, 2), inverse_terms, 1, 1)
            basis_full[some, :] = columns
            whole = columns.astype(jnp.bfloat16)
            basis[0, b, some, :] = whole
            basis_mid[some, :] = (columns - whole.astype(jnp.float32)).astype(jnp.bfloat16)
            return inner

        lax.fori_loop(0, 4, orthogonal, 0)
        q_over(b).start()
        q_twin(b).start()

        def update(i, inner):
            below = pl.ds(pl.multiple_of(i * span, span), span)

            def part(n, deeper):
                wide = pl.ds(pl.multiple_of(n * 2 * span, 2 * span), 2 * span)
                work[below, wide] = work[below, wide] - contract(near_terms[:, below], far_terms[:, wide], 0, 0)
                return deeper

            return lax.fori_loop(i // 2, blocks_count // 2, part, inner)

        lax.fori_loop(b + 1, blocks_count, update, 0)
        height = tile_ref.shape[0]
        mine = pl.ds(pl.multiple_of(op * height, height), height)
        tile_ref[:, lanes] = basis_full[mine, :] * float(states) ** 0.5

        def spread_out(n, inner):
            wide = pl.ds(pl.multiple_of(n * 2 * span, 2 * span), 2 * span)

            def part(m, deeper):
                some = pl.ds(pl.multiple_of(m * tall, tall), tall)
                whole = basis[0, b, some, :]
                terms = jnp.concatenate([whole, whole, basis_mid[some, :]], axis=1)
                out_ref[some, wide] = out_ref[some, wide] - contract(terms, panel_ref[:, wide], 1, 0)
                return deeper

            return lax.fori_loop(0, 4, part, inner)

        lax.fori_loop((b + 1) // 2, blocks_count // 2, spread_out, 0)

        @pl.when(b > 0)
        def _():
            pass_on(b - 1)

        return carry

    lax.fori_loop(0, blocks_count, factor_step, 0)

    def rotate(b):
        q_twin(b).wait_recv()
        q_cross(b).wait_recv()
        value = basis[0, b]
        for n, sector in enumerate((sec_over, sec_twin, sec_cross)):
            value = jnp.where(wanted == sector, basis[n + 1, b], value)
        rotated_ref[pl.ds(b * span, span), :] = contract(value, mapped[...], 0, 0)

    def apply(n, carry):
        some = pl.ds(pl.multiple_of(n * tall, tall), tall)
        columns = jnp.concatenate([basis[0, b] for b in range(blocks_count)], axis=1)
        mapped[some, :] = contract(blocks[some, :], columns, 1, 0).astype(jnp.bfloat16)
        return carry

    lax.fori_loop(0, 4, apply, 0)
    for b in range(blocks_count - 1):
        rotate(b)
    pass_on(blocks_count - 1)
    rotate(blocks_count - 1)

    def sent(ref, sem):
        remote(ref, ref, sem, x_in.at[0], side).wait_send()

    sent(basis.at[pl.ds(0, 3)], q_out)
    sent(store, fetch_out.at[1])
    for n, bufs in enumerate((levels, scales)):
        sent(bufs["inner"], departures.at[0, n])

    @pl.when(mid)
    def _():
        sent(store.at[pl.ds(0, PARTS + WAVES)], fetch_out.at[0])
        for n, bufs in enumerate((levels, scales)):
            sent(bufs["inner"], departures.at[1, n])

    @pl.when(leaf)
    def _():
        sent(store.at[pl.ds(0, PARTS)], fetch_out.at[0])
        for n, bufs in enumerate((levels, scales)):
            sent(bufs["inner"].at[pl.ds(0, FLOWS)], departures.at[1, n])


def publish_kernel(tile_ref, rotated_ref, tile_out, rotated_out, done):
    copies = [
        pltpu.make_async_copy(source, target, done.at[i])
        for i, (source, target) in enumerate(((tile_ref, tile_out), (rotated_ref, rotated_out)))
    ]
    for copy in copies:
        copy.start()
    for copy in copies:
        copy.wait()


def publish(tile, rotated):
    return pl.pallas_call(
        publish_kernel,
        out_shape=tuple(jax.ShapeDtypeStruct(a.shape, a.dtype) for a in (tile, rotated)),
        in_specs=[pl.BlockSpec(memory_space=pltpu.VMEM)] * 2,
        out_specs=(pl.BlockSpec(memory_space=pl.ANY),) * 2,
        scratch_shapes=[pltpu.SemaphoreType.DMA((2,))],
        compiler_params=pltpu.CompilerParams(vmem_limit_bytes=2 * 1024 * 1024),
        name="publish",
    )(tile, rotated)


def whole_kernel(own, blocks, guess, sizes, counts, target_map, top, bottom):
    rows, states = own.shape
    kept = guess.shape[1]
    chunk = states // (2 * FLOWS)
    lengths = (FLOWS, FLOWS, FLOWS, 2 * FLOWS, FLOWS, FLOWS)
    sem = pltpu.SemaphoreType.DMA
    half = own.dtype
    total = 2 * DEPTH * rows
    pieces = kept // LANES
    scratch = [
        pltpu.VMEM((16 * PARTS, rows // PARTS, states), half),
        pltpu.VMEM((WAVES, rows // PARTS, states), half),
        pltpu.VMEM((WAVES, rows // PARTS, states), half),
        pltpu.VMEM((total, states), half),
        pltpu.VMEM((states, states), half),
        pltpu.VMEM((states, kept), half),
        pltpu.VMEM((total + rows, states), half),
        pltpu.VMEM((total + rows, kept), half),
        pltpu.VMEM((total + rows, kept), half),
    ]
    scratch += [sem((WAVES,))] * 5 + [sem((2,)), sem((8,))]
    scratch += [pltpu.VMEM((n, chunk, kept), jnp.int16) for n in lengths]
    scratch += [pltpu.VMEM((n, 1, kept), jnp.float32) for n in lengths]
    scratch += [sem((n,)) for n in (FLOWS, 2 * FLOWS, FLOWS, FLOWS)]
    scratch += [sem((2, 2)), pltpu.VMEM((1, chunk * kept // 2 + kept), jnp.float32), pltpu.VMEM((states, kept), jnp.float32)]
    scratch += [pltpu.SMEM(a.shape, jnp.int32) for a in (sizes, counts, target_map, top, bottom)]
    scratch += [
        pltpu.VMEM((rows, states), half),
        pltpu.VMEM((states, kept), jnp.float32),
        pltpu.VMEM((kept, kept), jnp.float32),
        pltpu.VMEM((6 * LANES, kept), half),
        pltpu.VMEM((6 * LANES, kept), half),
        pltpu.VMEM((4, pieces, states, LANES), half),
        pltpu.VMEM((states, LANES), half),
        pltpu.VMEM((states, LANES), jnp.float32),
        pltpu.VMEM((states, kept), half),
        pltpu.VMEM((3 * LANES, kept), half),
        sem((3, pieces)),
        sem,
    ]
    return pl.pallas_call(
        image_kernel,
        out_shape=(
            pltpu.VMEM((states // lax.axis_size("op"), kept), jnp.float32),
            pltpu.VMEM((kept, kept), jnp.float32),
        ),
        in_specs=[pl.BlockSpec(memory_space=pltpu.HBM)] * 8,
        out_specs=[pl.BlockSpec(memory_space=pltpu.VMEM)] * 2,
        scratch_shapes=scratch,
        compiler_params=pltpu.CompilerParams(
            collective_id=1, has_side_effects=True, vmem_limit_bytes=60 * 1024 * 1024
        ),
        name="truncate_and_rotate",
    )(sizes, counts, target_map, top, bottom, own, blocks, guess)


def body(
    wavefunction,
    op_blocks,
    basis_guess,
    sector_sizes,
    kept_counts,
    target_map,
    noise_numerator,
    noise_denominator,
):
    if lax.axis_size("op") == 2 * DEPTH and lax.axis_size("sec") == 4:
        tile, rotated = whole_kernel(
            wavefunction[0],
            op_blocks[0, 0],
            basis_guess[0],
            sector_sizes,
            kept_counts,
            target_map.T,
            noise_numerator,
            noise_denominator,
        )
        tile, rotated = publish(tile, rotated)
        return (tile[None], rotated[None, None])
    state_count = wavefunction.shape[2]
    kept_width = basis_guess.shape[2]
    tile_rows = state_count // lax.axis_size("op")
    sec_index = lax.axis_index("sec")
    op_index = lax.axis_index("op")
    noise_weight = noise_numerator[0].astype(jnp.float32) / noise_denominator[0].astype(jnp.float32)
    sources = source_sectors(target_map)
    wanted_all = lax.dynamic_index_in_dim(sources, sec_index, 1, keepdims=False)[None, :]
    wanted = lax.dynamic_index_in_dim(wanted_all[0], op_index, 0, keepdims=False)
    states = jnp.arange(state_count, dtype=jnp.int32)
    own_size = lax.dynamic_index_in_dim(sector_sizes, sec_index, 0, keepdims=False)
    source_size = lax.dynamic_index_in_dim(sector_sizes, wanted, 0, keepdims=False)
    own_count = lax.dynamic_index_in_dim(kept_counts, sec_index, 0, keepdims=False)
    own_kept = jnp.arange(kept_width, dtype=jnp.int32) < own_count
    zero_half = jnp.zeros((), jnp.bfloat16)
    own_rows = jnp.where((states < own_size)[None, :], wavefunction[0], zero_half)
    moved = fetch_pieces(wavefunction, wanted_all)[0]
    moved = jnp.where((states < source_size)[None, :], moved, zero_half)
    blocks = op_blocks[0, 0]
    perturbed = jnp.dot(moved, blocks, preferred_element_type=jnp.float32).astype(jnp.bfloat16)
    guess = jnp.where((states < own_size)[:, None], basis_guess[0], zero_half)
    perturbed_guess = noise_weight * jnp.dot(perturbed, guess, preferred_element_type=jnp.float32)
    own_guess = jnp.dot(own_rows, guess, preferred_element_type=jnp.float32)
    part = lax.dot_general(
        jnp.concatenate([perturbed, own_rows], axis=0).astype(jnp.float32),
        jnp.concatenate([perturbed_guess, own_guess], axis=0),
        (((0,), (0,)), ((), ())),
        precision=lax.Precision.HIGH,
    )
    part = jnp.where((states < own_size)[:, None] & own_kept[None, :], part, jnp.float32(0.0))
    full_image = sum_over_op(part)
    padding = jnp.where(own_kept, jnp.float32(0.0), jnp.float32(1.0))
    correlation = dot_ta(full_image, full_image) + padding[:, None] * jnp.eye(
        kept_width, dtype=jnp.float32
    )
    inverse = inverse_factor(correlation)
    new_basis = lax.dot_general(
        full_image, inverse, (((1,), (1,)), ((), ())), precision=lax.Precision.HIGH
    )
    kept_tile = (
        lax.dynamic_slice_in_dim(new_basis, op_index * tile_rows, tile_rows, 0)
        * float(state_count) ** 0.5
    )
    basis_half = new_basis.astype(jnp.bfloat16)
    mapped = jnp.dot(blocks, basis_half, preferred_element_type=jnp.float32).astype(jnp.bfloat16)
    source_basis = fetch_sector(basis_half, wanted)
    rotated = lax.dot_general(
        source_basis, mapped, (((0,), (0,)), ((), ())), preferred_element_type=jnp.float32
    )
    return (kept_tile[None], rotated[None, None])


def solution(mesh):
    placed = (
        P("sec", "op", None),
        P("op", "sec", None, None),
        P("sec", None, None),
        P(),
        P(),
        P(),
        P(),
        P(),
    )
    return jax.shard_map(
        body,
        mesh=mesh,
        in_specs=placed,
        out_specs=(P("sec", "op", None), P("op", "sec", None, None)),
        check_vma=False,
    )
```

```python
import functools

import jax
import jax.numpy as jnp
from jax import lax
from jax.experimental import pallas as pl
from jax.experimental.pallas import tpu as pltpu
from jax.sharding import PartitionSpec as P

LANES = 128
ROWS = 8
HIGHEST = lax.Precision.HIGHEST


def dot_ta(a, b):
    return lax.dot_general(
        a, b, (((0,), (0,)), ((), ())), precision=HIGHEST, preferred_element_type=jnp.float32
    )


def dot(a, b):
    return jnp.dot(a, b, precision=HIGHEST, preferred_element_type=jnp.float32)


def eliminate_tile(tile):
    count = LANES // ROWS
    row = lax.broadcasted_iota(jnp.int32, (ROWS, LANES), 0)
    lane = lax.broadcasted_iota(jnp.int32, (ROWS, LANES), 1)
    left = [tile[ROWS * q : ROWS * (q + 1), :] for q in range(count)]
    right = [jnp.where(lane == row + ROWS * q, 1.0, 0.0).astype(jnp.float32) for q in range(count)]
    for p in range(count):
        upper, lower = left[p], right[p]
        columns = [
            jnp.broadcast_to(upper[:, ROWS * p + j : ROWS * p + j + 1], (ROWS, LANES))
            for j in range(ROWS)
        ]
        for j in range(ROWS):
            scale = lax.rsqrt(jnp.broadcast_to(columns[j][j : j + 1, :], (ROWS, LANES)))
            factor = jnp.where(row > j, columns[j] * scale, 0.0)
            for k in range(j + 1, ROWS):
                own = jnp.broadcast_to(columns[k][j : j + 1, :], (ROWS, LANES)) * scale
                columns[k] = columns[k] - factor * own
            own_upper = jnp.broadcast_to(upper[j : j + 1, :], (ROWS, LANES)) * scale
            own_lower = jnp.broadcast_to(lower[j : j + 1, :], (ROWS, LANES)) * scale
            upper = jnp.where(row == j, own_upper, upper - factor * own_upper)
            lower = jnp.where(row == j, own_lower, lower - factor * own_lower)
        right[p] = lower
        if p + 1 < count:
            change = dot_ta(upper, jnp.concatenate([upper, lower], axis=1))
            for q in range(p + 1, count):
                part = change[ROWS * q : ROWS * (q + 1), :]
                left[q] = left[q] - part[:, :LANES]
                right[q] = right[q] - part[:, LANES:]
    return jnp.concatenate(right, axis=0)


def inverse_factor_kernel(matrix_ref, out_ref, work):
    size = matrix_ref.shape[0]
    blocks = size // LANES
    work[:, :size] = matrix_ref[...]
    work[:, size:] = (
        lax.broadcasted_iota(jnp.int32, (size, size), 0)
        == lax.broadcasted_iota(jnp.int32, (size, size), 1)
    ).astype(jnp.float32)

    def step(b, carry):
        rows = pl.ds(pl.multiple_of(b * LANES, LANES), LANES)
        inverse = eliminate_tile(work[rows, rows])
        panel = dot(inverse, work[rows, :])
        work[rows, :] = panel
        out_ref[rows, :] = panel[:, size:]

        def update(i, inner):
            below = pl.ds(pl.multiple_of(i * LANES, LANES), LANES)
            work[below, :] = work[below, :] - dot_ta(work[rows, below], work[rows, :])
            return inner

        lax.fori_loop(b + 1, blocks, update, 0)
        return carry

    lax.fori_loop(0, blocks, step, 0)


def inverse_factor(matrix):
    size = matrix.shape[0]
    return pl.pallas_call(
        inverse_factor_kernel,
        out_shape=jax.ShapeDtypeStruct((size, size), jnp.float32),
        in_specs=[pl.BlockSpec(memory_space=pltpu.VMEM)],
        out_specs=pl.BlockSpec(memory_space=pltpu.VMEM),
        scratch_shapes=[pltpu.VMEM((size, 2 * size), jnp.float32)],
        compiler_params=pltpu.CompilerParams(vmem_limit_bytes=24 * 1024 * 1024),
        cost_estimate=pl.CostEstimate(flops=2 * size**3, bytes_accessed=8 * size * size, transcendentals=size),
        name="inverse_factor",
    )(matrix)


def source_sectors(target_map):
    sectors = jnp.arange(target_map.shape[1], dtype=jnp.int32)
    matches = target_map[:, :, None] == sectors[None, None, :]
    return jnp.sum(jnp.where(matches, sectors[None, :, None], 0), axis=1)


def fetch_pieces(own_slice, wanted_all):
    everyone = lax.all_gather(own_slice, "sec", axis=0, tiled=True)
    outgoing = jnp.take(everyone, wanted_all, axis=0)
    incoming = lax.all_to_all(outgoing, "op", split_axis=1, concat_axis=1, tiled=True)
    return incoming.reshape(
        incoming.shape[0], incoming.shape[1] * incoming.shape[2], incoming.shape[3]
    )


def exchange(value, axis, bit):
    count = lax.axis_size(axis)
    return lax.ppermute(value, axis, [(i, i ^ bit) for i in range(count)])


def halves(value, side):
    half = value.shape[0] // 2
    kept = lax.dynamic_slice_in_dim(value, side * half, half, 0)
    given = lax.dynamic_slice_in_dim(value, (1 - side) * half, half, 0)
    return kept, given


def sum_over_op(value):
    count = lax.axis_size("op")
    index = lax.axis_index("op")
    bits = [1 << b for b in range(count.bit_length() - 1)]
    orders = [bits, bits[1:] + bits[:1]]
    half = value.shape[0] // 2
    held = [value[:half], value[half:]]
    for step in range(len(bits)):
        for color, order in enumerate(orders):
            kept, given = halves(held[color], (index // order[step]) % 2)
            held[color] = kept + exchange(given, "op", order[step])
    for step in reversed(range(len(bits))):
        for color, order in enumerate(orders):
            own = held[color]
            other = exchange(own, "op", order[step])
            first = (index // order[step]) % 2 == 0
            held[color] = jnp.concatenate(
                [jnp.where(first, own, other), jnp.where(first, other, own)], axis=0
            )
    return jnp.concatenate(held, axis=0)


def fetch_sector(own, wanted):
    count = lax.axis_size("sec")
    offset = lax.axis_index("sec") ^ wanted
    held = {0: own}
    bit = count // 2
    while bit:
        for known in list(held):
            held[known ^ bit] = exchange(held[known], "sec", bit)
        bit //= 2
    result = own
    for known, value in held.items():
        result = jnp.where(offset == known, value, result)
    return result


MESH = pl.DeviceIdType.MESH
DEPTH = 4
PAIRS = 8
LAG = 2
AHEAD = 8
FLOWS = 2 * PAIRS
PARTS = 4
WAVES = DEPTH * PARTS


def steps(stage, step):
    return [(stage, step * PARTS + h) for h in range(PARTS)]


def mixed(*lists):
    return [item for group in zip(*lists) for item in group]


def leaf_order():
    order = steps(0, 0) + mixed(steps(1, 0), steps(0, 1)) + steps(2, 0)
    order += mixed(steps(1, 1), steps(0, 2)) + steps(2, 1) + steps(1, 2)
    return order + steps(0, 3) + steps(2, 2) + steps(1, 3) + steps(2, 3)


def mid_order():
    order = steps(0, 0) + steps(0, 1) + steps(0, 2) + steps(1, 0) + steps(2, 0) + steps(0, 3)
    return order + steps(1, 1) + mixed(steps(2, 1), steps(1, 2)) + mixed(steps(2, 2), steps(1, 3)) + steps(2, 3)


def quantize(value):
    top = jnp.maximum(jnp.max(jnp.abs(value), axis=0, keepdims=True), jnp.float32(1e-30))
    levels = jnp.round(value * (jnp.float32(32766.0) / top))
    return levels.astype(jnp.int32).astype(jnp.int16), top * jnp.float32(1.0 / 32766.0)


def remote(source, target, send, receive, device):
    return pltpu.make_async_remote_copy(
        src_ref=source,
        dst_ref=target,
        send_sem=send,
        recv_sem=receive,
        device_id=device,
        device_id_type=MESH,
    )


def greet(device):
    pl.semaphore_signal(pltpu.get_barrier_semaphore(), inc=1, device_id=device, device_id_type=MESH)


def source_of(map_ref, op, sec):
    found = jnp.int32(0)
    for sector in range(map_ref.shape[0]):
        found = jnp.where(map_ref[sector, op] == sec, sector, found)
    return found


def before(limit, width, dtype):
    lane = lax.broadcasted_iota(jnp.int32, (1, width), 1)
    return jnp.where(lane < limit, 1.0, 0.0).astype(jnp.float32).astype(dtype)


def split(value, parts):
    pieces = []
    for _ in range(parts):
        piece = value.astype(jnp.bfloat16)
        value = value - piece.astype(jnp.float32)
        pieces.append(piece)
    return pieces


def left_terms(value, axis, parts=3):
    p = split(value, parts)
    order = (p[0], p[0], p[1]) if parts == 2 else (p[0], p[0], p[1], p[0], p[2], p[1])
    return jnp.concatenate(order, axis=axis)


def right_terms(value, axis, parts=3):
    p = split(value, parts)
    order = (p[0], p[1], p[0]) if parts == 2 else (p[0], p[1], p[0], p[2], p[0], p[1])
    return jnp.concatenate(order, axis=axis)


def contract(a, b, i, j):
    return lax.dot_general(a, b, (((i,), (j,)), ((), ())), preferred_element_type=jnp.float32)


def eliminate_pairs(tile, beside=()):
    count = LANES // ROWS
    row = lax.broadcasted_iota(jnp.int32, (ROWS, LANES), 0)
    lane = lax.broadcasted_iota(jnp.int32, (ROWS, LANES), 1)
    left = [tile[ROWS * q : ROWS * (q + 1), :] for q in range(count)]
    right = [jnp.where(lane == row + ROWS * q, 1.0, 0.0).astype(jnp.float32) for q in range(count)]

    def lane_of(value, j):
        return jnp.broadcast_to(value[:, j : j + 1], (ROWS, LANES))

    def row_of(value, j):
        return jnp.broadcast_to(value[j : j + 1, :], (ROWS, LANES))

    for s in range(count // 2):
        for extra in beside[s :: count // 2]:
            extra()
        base = 2 * ROWS * s
        ua, la, ub, lb = left[2 * s], right[2 * s], left[2 * s + 1], right[2 * s + 1]
        ca = [lane_of(ua, base + j) for j in range(ROWS)]
        cb = [lane_of(ub, base + j) for j in range(2 * ROWS)]
        for j in range(ROWS):
            scale = lax.rsqrt(row_of(ca[j], j))
            fa = jnp.where(row > j, ca[j] * scale, 0.0)
            fb = cb[j] * scale
            for k in range(j + 1, ROWS):
                own = row_of(ca[k], j) * scale
                ca[k] = ca[k] - fa * own
                cb[k] = cb[k] - fb * own
            for k in range(ROWS):
                cb[ROWS + k] = cb[ROWS + k] - fb * row_of(fb, k)
            own_u = row_of(ua, j) * scale
            own_l = row_of(la, j) * scale
            ua = jnp.where(row == j, own_u, ua - fa * own_u)
            la = jnp.where(row == j, own_l, la - fa * own_l)
            ub = ub - fb * own_u
            lb = lb - fb * own_l
        cb = cb[ROWS:]
        for j in range(ROWS):
            scale = lax.rsqrt(row_of(cb[j], j))
            fb = jnp.where(row > j, cb[j] * scale, 0.0)
            for k in range(j + 1, ROWS):
                cb[k] = cb[k] - fb * (row_of(cb[k], j) * scale)
            own_u = row_of(ub, j) * scale
            own_l = row_of(lb, j) * scale
            ub = jnp.where(row == j, own_u, ub - fb * own_u)
            lb = jnp.where(row == j, own_l, lb - fb * own_l)
        right[2 * s], right[2 * s + 1] = la, lb
        if 2 * s + 2 < count:
            upper = jnp.concatenate([ua, ub], axis=0)
            lower = jnp.concatenate([la, lb], axis=0)
            both = jnp.concatenate([right_terms(upper, 0), right_terms(lower, 0)], axis=1)
            flipped = left_terms(upper, 0).T
            for first, last in ((2 * s + 2, 2 * s + 4), (2 * s + 4, count)):
                if first == last:
                    continue
                change = contract(flipped[ROWS * first : ROWS * last, :], both, 1, 0)
                for q in range(first, last):
                    part = change[ROWS * (q - first) : ROWS * (q - first + 1), :]
                    left[q] = left[q] - part[:, :LANES]
                    right[q] = right[q] - part[:, LANES:]
    return jnp.concatenate(right, axis=0)


def image_kernel(sizes_hbm, counts_hbm, map_hbm, top_hbm, bottom_hbm, own_hbm, blocks_hbm, guess_hbm, tile_ref, rotated_ref, *refs):
    rows, states = own_hbm.shape
    kept = guess_hbm.shape[1]
    chunk = states // (2 * FLOWS)
    band = rows // PARTS
    sec = lax.axis_index("sec")
    op = lax.axis_index("op")
    y, c = sec // 2, sec % 2
    z, x = op // 2, op % 2
    w = z // 2
    zz = z + w * (3 - 2 * z)
    mid = zz == 1
    leaf = jnp.logical_not(mid)
    sec_over = (1 - y) * 2 + c
    sec_twin = y * 2 + 1 - c
    sec_cross = (1 - y) * 2 + 1 - c
    twin = (sec_twin, op)
    over = (sec_over, op)
    side = (sec, z * 2 + 1 - x)
    inner = (sec, (1 + w) * 2 + x)
    outer = (sec, 6 * w + x)
    other = (sec, (3 - z) * 2 + x)

    (store, picked, landed, moved, blocks, guess, left, high, low) = refs[:9]
    (line_in, side_in, core_in, x_in, fetch_out, load) = refs[9:15]
    refs = refs[15:]
    names = ("give", "take", "own", "inner", "final", "last")
    levels = dict(zip(names, refs[0:6]))
    scales = dict(zip(names, refs[6:12]))
    arrivals = dict(zip(("take", "inner", "final", "last"), refs[12:16]))
    departures, measure_ref, part_ref = refs[16:19]
    scalars = refs[19:24]
    own_ref, out_ref, work, near_terms, far_terms, basis, basis_mid, basis_full, mapped, panel_ref, inverse_ref, q_in, q_out = refs[24:37]
    load_own = pltpu.make_async_copy(own_hbm, own_ref, load.at[7])
    load_own.start()
    sizes_ref, counts_ref, map_ref, top_ref, bottom_ref = scalars
    loads = [
        pltpu.make_async_copy(source, target, load.at[2 + i])
        for i, (source, target) in enumerate(zip((sizes_hbm, counts_hbm, map_hbm, top_hbm, bottom_hbm), scalars))
    ]
    for copy in loads:
        copy.start()

    load_blocks = pltpu.make_async_copy(blocks_hbm, blocks, load.at[0])
    load_guess = pltpu.make_async_copy(guess_hbm, guess, load.at[1])
    load_blocks.start()
    load_guess.start()
    barrier = pltpu.get_barrier_semaphore()
    greet(twin)
    greet(over)
    greet(side)

    @pl.when(mid)
    def _():
        greet(other)
        greet(outer)
        pl.semaphore_wait(barrier, 5)

    @pl.when(leaf)
    def _():
        greet(inner)
        pl.semaphore_wait(barrier, 4)

    for copy in loads:
        copy.wait()
    wanted = source_of(map_ref, op, sec)
    beside = source_of(map_ref, op + 1 - 2 * x, sec)
    source_mask = before(sizes_ref[wanted], states, jnp.bfloat16)
    own_size = sizes_ref[sec]
    own_mask = before(own_size, states, jnp.bfloat16)

    marks = [zz, 1 - zz, 2, 3]
    place = [q + w * (3 - 2 * q) for q in marks]

    def slot(v, sector):
        return store.at[(place[v // PARTS] * 4 + sector) * PARTS + v % PARTS]

    def piece(v):
        if v < PARTS:
            return own_ref.at[pl.ds(v * band, band)]
        return slot(v, sec)

    def line_sem(v):
        return line_in.at[place[v // PARTS] * PARTS + v % PARTS]

    def along(v, device):
        return remote(piece(v), slot(v, sec), fetch_out.at[0], line_sem(v), device)

    def across(v):
        return remote(piece(v), slot(v, sec), fetch_out.at[1], side_in.at[v], over)

    def to_twin(v):
        return remote(piece(v), slot(v, sec), fetch_out.at[1], core_in.at[v], twin)

    def to_twin_second(v):
        return remote(slot(v, sec_over), slot(v, sec_over), fetch_out.at[1], core_in.at[v], twin)

    def to_side(v):
        return remote(picked.at[v], landed.at[v], fetch_out.at[1], x_in.at[v], side)

    def first(v):
        step = v // PARTS
        if step == 0:

            @pl.when(mid)
            def _():
                along(v, other).start()
                along(v, outer).start()

            @pl.when(leaf)
            def _():
                along(v, inner).start()
        else:
            remote(slot(v, sec), slot(v, sec), fetch_out.at[0], line_sem(v), side).wait_recv()

            @pl.when(mid)
            def _():
                along(v, other if step == 1 else outer).start()

        across(v).start()
        to_twin(v).start()

    def second(v):
        remote(slot(v, sec_over), slot(v, sec_over), fetch_out.at[1], side_in.at[v], over).wait_recv()
        to_twin_second(v).start()

    def choose(v, sector_wanted):
        base = place[v // PARTS] * 4
        value = store[(base + 3) * PARTS + v % PARTS]
        for sector in range(3):
            value = jnp.where(sector_wanted == sector, store[(base + sector) * PARTS + v % PARTS], value)
        return value

    def third(v):
        both = store.at[pl.ds(0, 2)]
        remote(both, both, fetch_out.at[1], core_in.at[v], twin).wait_recv()
        picked[v] = choose(v, beside)
        to_side(v).start()
        moved[pl.ds(v * band, band), :] = choose(v, wanted) * source_mask

    def perturb(first_row, count):
        span = pl.ds(first_row, count)

        def step(n, carry):
            lanes = pl.ds(pl.multiple_of(n * 256, 256), 256)
            value = jnp.dot(moved[span, :], blocks[:, lanes], preferred_element_type=jnp.float32)
            lane = lax.broadcasted_iota(jnp.int32, (1, 256), 1) + n * 256
            keep = jnp.where(lane < own_size, 1.0, 0.0).astype(jnp.float32).astype(jnp.bfloat16)
            left[span, lanes] = value.astype(jnp.bfloat16) * keep
            return carry

        lax.fori_loop(0, states // 256, step, 0)

    load_own.wait()
    for v in range(PARTS):
        store[(place[0] * 4 + sec) * PARTS + v] = own_ref[pl.ds(v * band, band), :]
    left[pl.ds(2 * DEPTH * rows, rows), :] = own_ref[...] * own_mask
    def run(order):
        for stage, v in order:
            (first, second, third)[stage](v)

    @pl.when(leaf)
    def _():
        run(leaf_order())

    @pl.when(mid)
    def _():
        run(mid_order())

    load_blocks.wait()
    load_guess.wait()
    perturb(0, DEPTH * rows)
    weight = jnp.full((1, kept), top_ref[0], jnp.int32).astype(jnp.float32) / jnp.full(
        (1, kept), bottom_ref[0], jnp.int32
    ).astype(jnp.float32)
    kept_mask = before(counts_ref[sec], kept, jnp.float32)

    def project(first_row, count, factor):
        span = pl.ds(first_row, count)
        value = jnp.dot(left[span, :], guess[...], preferred_element_type=jnp.float32) * factor
        top_half = value.astype(jnp.bfloat16)
        high[span, :] = top_half
        low[span, :] = (value - top_half.astype(jnp.float32)).astype(jnp.bfloat16)

    project(0, DEPTH * rows, weight * kept_mask)
    project(2 * DEPTH * rows, rows, kept_mask)
    for early, late in ((0, WAVES - PARTS), (WAVES - PARTS, WAVES)):
        for v in range(early, late):
            to_side(v).wait_recv()
            moved[pl.ds(DEPTH * rows + v * band, band), :] = landed[v] * source_mask
        perturb(DEPTH * rows + early * band, (late - early) * band)
        project(DEPTH * rows + early * band, (late - early) * band, weight * kept_mask)

    def product(n):
        lanes = pl.ds(pl.multiple_of(n * 256, 256), 256)
        dims = (((0,), (0,)), ((), ()))
        value = lax.dot_general(left[:, lanes], high[...], dims, preferred_element_type=jnp.float32)
        part_ref[lanes, :] = value + lax.dot_general(
            left[:, lanes], low[...], dims, preferred_element_type=jnp.float32
        )

    def start(source, i, target, j, lane, device, flag=None):
        flag = arrivals[target].at[j if flag is None else flag]
        for n, bufs in enumerate((levels, scales)):
            remote(bufs[source].at[i], bufs[target].at[j], departures.at[lane, n], flag, device).start()

    def arrived(target, j, ref=measure_ref.at[0]):
        remote(ref, ref, departures.at[0, 0], arrivals[target].at[j], side).wait_recv()

    def put(name, i, value):
        whole, scale = quantize(value)
        levels[name][i] = whole
        scales[name][i] = scale

    def get(name, i):
        return levels[name][i].astype(jnp.int32).astype(jnp.float32) * scales[name][i]

    def chunk_rows(half, i):
        return pl.ds(pl.multiple_of((FLOWS * half + i) * chunk, chunk), chunk)

    def value(i):
        arrived("take", i)
        return part_ref[chunk_rows(x, i), :] + get("take", i)

    def finish(i):
        start("final", i, "last", i, 0, side)
        out_ref[chunk_rows(x, i), :] = get("final", i)

    def give(i):
        put("give", i, part_ref[chunk_rows(1 - x, i), :])
        start("give", i, "take", i, 0, side)

    tiles = states // 256
    for n in range(tiles // 2):
        product((1 - x) * (tiles // 2) + n)
        if n == 0:
            for i in range(AHEAD):
                give(i)
    for n in range(tiles // 2):
        product(x * (tiles // 2) + n)

    span = LANES
    blocks_count = kept // span
    tall = states // 4

    def correlate(n, carry):
        image = out_ref[pl.ds(pl.multiple_of(n * tall, tall), tall), :]
        terms = left_terms(image, 0)
        others = right_terms(image, 0)
        middle = kept // 2
        work[:middle, :] = work[:middle, :] + contract(terms[:, :middle], others, 0, 0)
        work[middle:, middle:] = work[middle:, middle:] + contract(terms[:, middle:], others[:, middle:], 0, 0)
        return carry

    diagonal = lax.broadcasted_iota(jnp.int32, (kept, kept), 0) == lax.broadcasted_iota(jnp.int32, (kept, kept), 1)
    work[...] = jnp.where(diagonal, 1.0 - kept_mask, 0.0)

    @pl.when(leaf)
    def _():
        for i in range(FLOWS):
            if i + AHEAD < FLOWS:
                give(i + AHEAD)
            put("own", i, value(i))
            far = w if i % 2 == 0 else 1 - w
            start("own", i, "inner", FLOWS * far + i, 1, inner, i)
        for i in range(FLOWS):
            arrived("final", i)
            finish(i)
            if i == FLOWS // 2 + 1:
                correlate(2 * x, 0)

    @pl.when(mid)
    def _():
        def relay(p):
            i = 2 * p + 1 - w
            mine = value(i)
            arrived("inner", i)
            put("own", i, mine + get("inner", FLOWS + i))
            start("own", i, "inner", FLOWS + i, 1, other, i)

        def collect(p):
            i = 2 * p + w
            near = value(i)
            arrived("inner", i, measure_ref)
            put("final", i, near + get("inner", i) + get("inner", FLOWS + i))
            start("final", i, "final", i, 1, outer)
            start("final", i, "final", i, 1, other)
            finish(i)

        def forward(p):
            i = 2 * p + 1 - w
            arrived("final", i)
            start("final", i, "final", i, 1, outer)
            finish(i)

        for p in range(PAIRS + 2 * LAG):
            if p < PAIRS:
                for i in range(2 * p + AHEAD, min(2 * p + AHEAD + 2, FLOWS)):
                    give(i)
                relay(p)
            if LAG <= p < PAIRS + LAG:
                collect(p - LAG)
            if p >= 2 * LAG:
                forward(p - 2 * LAG)
            if p == PAIRS // 2 + 2 * LAG:
                correlate(2 * x, 0)


    correlate(2 * x + 1, 0)
    for n in range(2):
        for i in range(n * FLOWS // 2, (n + 1) * FLOWS // 2):
            arrived("last", i)
            out_ref[chunk_rows(1 - x, i), :] = get("last", i)
        correlate(2 * (1 - x) + n, 0)

    def q_over(b):
        return remote(basis.at[0, b], basis.at[1, b], q_out, q_in.at[0, b], over)

    def q_twin(b):
        return remote(basis.at[0, b], basis.at[2, b], q_out, q_in.at[1, b], twin)

    def q_cross(b):
        return remote(basis.at[1, b], basis.at[3, b], q_out, q_in.at[2, b], twin)

    def half_of(which):
        return pl.ds(pl.multiple_of(which * (states // 2), states // 2), states // 2)

    def q_half(b, ref, which, i, device):
        some = half_of(which)
        return remote(basis.at[ref, b, some], basis.at[1, b, some], q_out, q_in.at[i, b], device)

    def pass_half(b):
        q_half(b, 0, x, 0, over).wait_recv()
        q_half(b, 1, x, 3, side).start()

    def pass_on(b):
        q_half(b, 1, 1 - x, 3, side).wait_recv()
        q_cross(b).start()

    def update(b, i):
        below = pl.ds(pl.multiple_of(i * span, span), span)

        def part(n, deeper):
            wide = pl.ds(pl.multiple_of(n * 2 * span, 2 * span), 2 * span)
            work[below, wide] = work[below, wide] - contract(near_terms[:, below], far_terms[:, wide], 0, 0)
            return deeper

        lax.fori_loop(i // 2, blocks_count // 2, part, 0)

    def factor_step(b, carry):
        lanes = pl.ds(pl.multiple_of(b * span, span), span)
        inverse = inverse_ref[...]
        panel = contract(left_terms(inverse, 1), right_terms(work[lanes, :], 0), 1, 0)
        inverse_terms = right_terms(inverse, 1, 2)
        panel_ref[...] = right_terms(panel, 0, 2)
        near_terms[...] = left_terms(panel, 0)
        far_terms[...] = right_terms(panel, 0)

        def orthogonal(n, inner):
            some = pl.ds(pl.multiple_of(n * tall, tall), tall)
            columns = contract(left_terms(out_ref[some, lanes], 1, 2), inverse_terms, 1, 1)
            basis_full[some, :] = columns
            whole = columns.astype(jnp.bfloat16)
            basis[0, b, some, :] = whole
            basis_mid[some, :] = (columns - whole.astype(jnp.float32)).astype(jnp.bfloat16)

            @pl.when(b + 1 == blocks_count)
            def _():
                remote(basis.at[0, b, some], basis.at[1, b, some], q_out, q_in.at[0, b], over).start()

            return inner

        lax.fori_loop(0, 4, orthogonal, 0)
        @pl.when(b + 1 < blocks_count)
        def _():
            q_half(b, 0, x, 0, over).start()

        q_twin(b).start()
        height = tile_ref.shape[0]
        mine = pl.ds(pl.multiple_of(op * height, height), height)
        tile_ref[:, lanes] = basis_full[mine, :] * float(states) ** 0.5

        @pl.when(b + 1 < blocks_count)
        def _():
            update(b, b + 1)

            def spread_out(m, n):
                some = pl.ds(m * tall, tall)
                wide = pl.ds(n * 2 * span, 2 * span)
                whole = basis[0, b, some, :]
                terms = jnp.concatenate([whole, whole, basis_mid[some, :]], axis=1)
                out_ref[some, wide] = out_ref[some, wide] - contract(terms, panel_ref[:, wide], 1, 0)

            following = pl.ds(pl.multiple_of((b + 1) * span, span), span)
            beside = [functools.partial(spread_out, m, n) for n in range(kept // (2 * span)) for m in range(4)]

            def late_update(ahead):
                valid = jnp.where(b + ahead < blocks_count, 1.0, 0.0).astype(jnp.float32)
                below = pl.ds(pl.multiple_of(jnp.minimum(b + ahead, blocks_count - 1) * span, span), span)
                wide = pl.ds(kept // 2, kept // 2)
                work[below, wide] = work[below, wide] - valid * contract(
                    near_terms[:, below], far_terms[:, wide], 0, 0
                )

            beside += [functools.partial(late_update, ahead) for ahead in range(2, blocks_count)]
            inverse_ref[...] = eliminate_pairs(work[following, following], beside)

        @pl.when(b > 0)
        def _():
            pass_half(b - 1)

        @pl.when((b > 1) & (b + 1 < blocks_count))
        def _():
            pass_on(b - 2)

        return carry

    inverse_ref[...] = eliminate_pairs(work[pl.ds(0, span), pl.ds(0, span)])
    lax.fori_loop(0, blocks_count, factor_step, 0)

    def rotate(b):
        q_twin(b).wait_recv()
        q_cross(b).wait_recv()
        value = basis[0, b]
        for n, sector in enumerate((sec_over, sec_twin, sec_cross)):
            value = jnp.where(wanted == sector, basis[n + 1, b], value)
        rotated_ref[pl.ds(b * span, span), :] = contract(value, mapped[...], 0, 0)

    def apply(n, carry):
        some = pl.ds(pl.multiple_of(n * tall, tall), tall)
        columns = jnp.concatenate([basis[0, b] for b in range(blocks_count)], axis=1)
        mapped[some, :] = contract(blocks[some, :], columns, 1, 0).astype(jnp.bfloat16)
        return carry

    lax.fori_loop(0, 4, apply, 0)
    pass_on(blocks_count - 3)
    for b in range(blocks_count - 2):
        rotate(b)
    pass_on(blocks_count - 2)
    rotate(blocks_count - 2)
    q_over(blocks_count - 1).wait_recv()
    q_cross(blocks_count - 1).start()
    rotate(blocks_count - 1)

    def sent(ref, sem):
        remote(ref, ref, sem, x_in.at[0], side).wait_send()

    sent(basis.at[pl.ds(0, 3)], q_out)
    sent(store, fetch_out.at[1])
    for n, bufs in enumerate((levels, scales)):
        sent(bufs["inner"], departures.at[0, n])

    @pl.when(mid)
    def _():
        sent(store.at[pl.ds(0, PARTS + WAVES)], fetch_out.at[0])
        for n, bufs in enumerate((levels, scales)):
            sent(bufs["inner"], departures.at[1, n])

    @pl.when(leaf)
    def _():
        sent(store.at[pl.ds(0, PARTS)], fetch_out.at[0])
        for n, bufs in enumerate((levels, scales)):
            sent(bufs["inner"].at[pl.ds(0, FLOWS)], departures.at[1, n])


def publish_kernel(tile_ref, rotated_ref, tile_out, rotated_out, done):
    copies = [
        pltpu.make_async_copy(source, target, done.at[i])
        for i, (source, target) in enumerate(((tile_ref, tile_out), (rotated_ref, rotated_out)))
    ]
    for copy in copies:
        copy.start()
    for copy in copies:
        copy.wait()


def publish(tile, rotated):
    return pl.pallas_call(
        publish_kernel,
        out_shape=tuple(jax.ShapeDtypeStruct(a.shape, a.dtype) for a in (tile, rotated)),
        in_specs=[pl.BlockSpec(memory_space=pltpu.VMEM)] * 2,
        out_specs=(pl.BlockSpec(memory_space=pl.ANY),) * 2,
        scratch_shapes=[pltpu.SemaphoreType.DMA((2,))],
        compiler_params=pltpu.CompilerParams(vmem_limit_bytes=2 * 1024 * 1024),
        name="publish",
    )(tile, rotated)


def whole_kernel(own, blocks, guess, sizes, counts, target_map, top, bottom):
    rows, states = own.shape
    kept = guess.shape[1]
    chunk = states // (2 * FLOWS)
    lengths = (FLOWS, FLOWS, FLOWS, 2 * FLOWS, FLOWS, FLOWS)
    sem = pltpu.SemaphoreType.DMA
    half = own.dtype
    total = 2 * DEPTH * rows
    pieces = kept // LANES
    scratch = [
        pltpu.VMEM((16 * PARTS, rows // PARTS, states), half),
        pltpu.VMEM((WAVES, rows // PARTS, states), half),
        pltpu.VMEM((WAVES, rows // PARTS, states), half),
        pltpu.VMEM((total, states), half),
        pltpu.VMEM((states, states), half),
        pltpu.VMEM((states, kept), half),
        pltpu.VMEM((total + rows, states), half),
        pltpu.VMEM((total + rows, kept), half),
        pltpu.VMEM((total + rows, kept), half),
    ]
    scratch += [sem((WAVES,))] * 4 + [sem((2,)), sem((8,))]
    scratch += [pltpu.VMEM((n, chunk, kept), jnp.int16) for n in lengths]
    scratch += [pltpu.VMEM((n, 1, kept), jnp.float32) for n in lengths]
    scratch += [sem((n,)) for n in (FLOWS, FLOWS, FLOWS, FLOWS)]
    scratch += [sem((2, 2)), pltpu.VMEM((2, 1, chunk * kept // 2 + kept), jnp.float32), pltpu.VMEM((states, kept), jnp.float32)]
    scratch += [pltpu.SMEM(a.shape, jnp.int32) for a in (sizes, counts, target_map, top, bottom)]
    scratch += [
        pltpu.VMEM((rows, states), half),
        pltpu.VMEM((states, kept), jnp.float32),
        pltpu.VMEM((kept, kept), jnp.float32),
        pltpu.VMEM((6 * LANES, kept), half),
        pltpu.VMEM((6 * LANES, kept), half),
        pltpu.VMEM((4, pieces, states, LANES), half),
        pltpu.VMEM((states, LANES), half),
        pltpu.VMEM((states, LANES), jnp.float32),
        pltpu.VMEM((states, kept), half),
        pltpu.VMEM((3 * LANES, kept), half),
        pltpu.VMEM((LANES, LANES), jnp.float32),
        sem((4, pieces)),
        sem,
    ]
    return pl.pallas_call(
        image_kernel,
        out_shape=(
            pltpu.VMEM((states // lax.axis_size("op"), kept), jnp.float32),
            pltpu.VMEM((kept, kept), jnp.float32),
        ),
        in_specs=[pl.BlockSpec(memory_space=pltpu.HBM)] * 8,
        out_specs=[pl.BlockSpec(memory_space=pltpu.VMEM)] * 2,
        scratch_shapes=scratch,
        compiler_params=pltpu.CompilerParams(
            collective_id=1, has_side_effects=True, vmem_limit_bytes=60 * 1024 * 1024
        ),
        name="truncate_and_rotate",
    )(sizes, counts, target_map, top, bottom, own, blocks, guess)


def body(
    wavefunction,
    op_blocks,
    basis_guess,
    sector_sizes,
    kept_counts,
    target_map,
    noise_numerator,
    noise_denominator,
):
    if lax.axis_size("op") == 2 * DEPTH and lax.axis_size("sec") == 4:
        tile, rotated = whole_kernel(
            wavefunction[0],
            op_blocks[0, 0],
            basis_guess[0],
            sector_sizes,
            kept_counts,
            target_map.T,
            noise_numerator,
            noise_denominator,
        )
        tile, rotated = publish(tile, rotated)
        return (tile[None], rotated[None, None])
    state_count = wavefunction.shape[2]
    kept_width = basis_guess.shape[2]
    tile_rows = state_count // lax.axis_size("op")
    sec_index = lax.axis_index("sec")
    op_index = lax.axis_index("op")
    noise_weight = noise_numerator[0].astype(jnp.float32) / noise_denominator[0].astype(jnp.float32)
    sources = source_sectors(target_map)
    wanted_all = lax.dynamic_index_in_dim(sources, sec_index, 1, keepdims=False)[None, :]
    wanted = lax.dynamic_index_in_dim(wanted_all[0], op_index, 0, keepdims=False)
    states = jnp.arange(state_count, dtype=jnp.int32)
    own_size = lax.dynamic_index_in_dim(sector_sizes, sec_index, 0, keepdims=False)
    source_size = lax.dynamic_index_in_dim(sector_sizes, wanted, 0, keepdims=False)
    own_count = lax.dynamic_index_in_dim(kept_counts, sec_index, 0, keepdims=False)
    own_kept = jnp.arange(kept_width, dtype=jnp.int32) < own_count
    zero_half = jnp.zeros((), jnp.bfloat16)
    own_rows = jnp.where((states < own_size)[None, :], wavefunction[0], zero_half)
    moved = fetch_pieces(wavefunction, wanted_all)[0]
    moved = jnp.where((states < source_size)[None, :], moved, zero_half)
    blocks = op_blocks[0, 0]
    perturbed = jnp.dot(moved, blocks, preferred_element_type=jnp.float32).astype(jnp.bfloat16)
    guess = jnp.where((states < own_size)[:, None], basis_guess[0], zero_half)
    perturbed_guess = noise_weight * jnp.dot(perturbed, guess, preferred_element_type=jnp.float32)
    own_guess = jnp.dot(own_rows, guess, preferred_element_type=jnp.float32)
    part = lax.dot_general(
        jnp.concatenate([perturbed, own_rows], axis=0).astype(jnp.float32),
        jnp.concatenate([perturbed_guess, own_guess], axis=0),
        (((0,), (0,)), ((), ())),
        precision=lax.Precision.HIGH,
    )
    part = jnp.where((states < own_size)[:, None] & own_kept[None, :], part, jnp.float32(0.0))
    full_image = sum_over_op(part)
    padding = jnp.where(own_kept, jnp.float32(0.0), jnp.float32(1.0))
    correlation = dot_ta(full_image, full_image) + padding[:, None] * jnp.eye(
        kept_width, dtype=jnp.float32
    )
    inverse = inverse_factor(correlation)
    new_basis = lax.dot_general(
        full_image, inverse, (((1,), (1,)), ((), ())), precision=lax.Precision.HIGH
    )
    kept_tile = (
        lax.dynamic_slice_in_dim(new_basis, op_index * tile_rows, tile_rows, 0)
        * float(state_count) ** 0.5
    )
    basis_half = new_basis.astype(jnp.bfloat16)
    mapped = jnp.dot(blocks, basis_half, preferred_element_type=jnp.float32).astype(jnp.bfloat16)
    source_basis = fetch_sector(basis_half, wanted)
    rotated = lax.dot_general(
        source_basis, mapped, (((0,), (0,)), ((), ())), preferred_element_type=jnp.float32
    )
    return (kept_tile[None], rotated[None, None])


def solution(mesh):
    placed = (
        P("sec", "op", None),
        P("op", "sec", None, None),
        P("sec", None, None),
        P(),
        P(),
        P(),
        P(),
        P(),
    )
    return jax.shard_map(
        body,
        mesh=mesh,
        in_specs=placed,
        out_specs=(P("sec", "op", None), P("op", "sec", None, None)),
        check_vma=False,
    )
```

```python
import functools

import jax
import jax.numpy as jnp
from jax import lax
from jax.experimental import pallas as pl
from jax.experimental.pallas import tpu as pltpu
from jax.sharding import PartitionSpec as P

LANES = 128
ROWS = 8
HIGHEST = lax.Precision.HIGHEST


def dot_ta(a, b):
    return lax.dot_general(
        a, b, (((0,), (0,)), ((), ())), precision=HIGHEST, preferred_element_type=jnp.float32
    )


def dot(a, b):
    return jnp.dot(a, b, precision=HIGHEST, preferred_element_type=jnp.float32)


def eliminate_tile(tile):
    count = LANES // ROWS
    row = lax.broadcasted_iota(jnp.int32, (ROWS, LANES), 0)
    lane = lax.broadcasted_iota(jnp.int32, (ROWS, LANES), 1)
    left = [tile[ROWS * q : ROWS * (q + 1), :] for q in range(count)]
    right = [jnp.where(lane == row + ROWS * q, 1.0, 0.0).astype(jnp.float32) for q in range(count)]
    for p in range(count):
        upper, lower = left[p], right[p]
        columns = [
            jnp.broadcast_to(upper[:, ROWS * p + j : ROWS * p + j + 1], (ROWS, LANES))
            for j in range(ROWS)
        ]
        for j in range(ROWS):
            scale = lax.rsqrt(jnp.broadcast_to(columns[j][j : j + 1, :], (ROWS, LANES)))
            factor = jnp.where(row > j, columns[j] * scale, 0.0)
            for k in range(j + 1, ROWS):
                own = jnp.broadcast_to(columns[k][j : j + 1, :], (ROWS, LANES)) * scale
                columns[k] = columns[k] - factor * own
            own_upper = jnp.broadcast_to(upper[j : j + 1, :], (ROWS, LANES)) * scale
            own_lower = jnp.broadcast_to(lower[j : j + 1, :], (ROWS, LANES)) * scale
            upper = jnp.where(row == j, own_upper, upper - factor * own_upper)
            lower = jnp.where(row == j, own_lower, lower - factor * own_lower)
        right[p] = lower
        if p + 1 < count:
            change = dot_ta(upper, jnp.concatenate([upper, lower], axis=1))
            for q in range(p + 1, count):
                part = change[ROWS * q : ROWS * (q + 1), :]
                left[q] = left[q] - part[:, :LANES]
                right[q] = right[q] - part[:, LANES:]
    return jnp.concatenate(right, axis=0)


def inverse_factor_kernel(matrix_ref, out_ref, work):
    size = matrix_ref.shape[0]
    blocks = size // LANES
    work[:, :size] = matrix_ref[...]
    work[:, size:] = (
        lax.broadcasted_iota(jnp.int32, (size, size), 0)
        == lax.broadcasted_iota(jnp.int32, (size, size), 1)
    ).astype(jnp.float32)

    def step(b, carry):
        rows = pl.ds(pl.multiple_of(b * LANES, LANES), LANES)
        inverse = eliminate_tile(work[rows, rows])
        panel = dot(inverse, work[rows, :])
        work[rows, :] = panel
        out_ref[rows, :] = panel[:, size:]

        def update(i, inner):
            below = pl.ds(pl.multiple_of(i * LANES, LANES), LANES)
            work[below, :] = work[below, :] - dot_ta(work[rows, below], work[rows, :])
            return inner

        lax.fori_loop(b + 1, blocks, update, 0)
        return carry

    lax.fori_loop(0, blocks, step, 0)


def inverse_factor(matrix):
    size = matrix.shape[0]
    return pl.pallas_call(
        inverse_factor_kernel,
        out_shape=jax.ShapeDtypeStruct((size, size), jnp.float32),
        in_specs=[pl.BlockSpec(memory_space=pltpu.VMEM)],
        out_specs=pl.BlockSpec(memory_space=pltpu.VMEM),
        scratch_shapes=[pltpu.VMEM((size, 2 * size), jnp.float32)],
        compiler_params=pltpu.CompilerParams(vmem_limit_bytes=24 * 1024 * 1024),
        cost_estimate=pl.CostEstimate(flops=2 * size**3, bytes_accessed=8 * size * size, transcendentals=size),
        name="inverse_factor",
    )(matrix)


def source_sectors(target_map):
    sectors = jnp.arange(target_map.shape[1], dtype=jnp.int32)
    matches = target_map[:, :, None] == sectors[None, None, :]
    return jnp.sum(jnp.where(matches, sectors[None, :, None], 0), axis=1)


def fetch_pieces(own_slice, wanted_all):
    everyone = lax.all_gather(own_slice, "sec", axis=0, tiled=True)
    outgoing = jnp.take(everyone, wanted_all, axis=0)
    incoming = lax.all_to_all(outgoing, "op", split_axis=1, concat_axis=1, tiled=True)
    return incoming.reshape(
        incoming.shape[0], incoming.shape[1] * incoming.shape[2], incoming.shape[3]
    )


def exchange(value, axis, bit):
    count = lax.axis_size(axis)
    return lax.ppermute(value, axis, [(i, i ^ bit) for i in range(count)])


def halves(value, side):
    half = value.shape[0] // 2
    kept = lax.dynamic_slice_in_dim(value, side * half, half, 0)
    given = lax.dynamic_slice_in_dim(value, (1 - side) * half, half, 0)
    return kept, given


def sum_over_op(value):
    count = lax.axis_size("op")
    index = lax.axis_index("op")
    bits = [1 << b for b in range(count.bit_length() - 1)]
    orders = [bits, bits[1:] + bits[:1]]
    half = value.shape[0] // 2
    held = [value[:half], value[half:]]
    for step in range(len(bits)):
        for color, order in enumerate(orders):
            kept, given = halves(held[color], (index // order[step]) % 2)
            held[color] = kept + exchange(given, "op", order[step])
    for step in reversed(range(len(bits))):
        for color, order in enumerate(orders):
            own = held[color]
            other = exchange(own, "op", order[step])
            first = (index // order[step]) % 2 == 0
            held[color] = jnp.concatenate(
                [jnp.where(first, own, other), jnp.where(first, other, own)], axis=0
            )
    return jnp.concatenate(held, axis=0)


def fetch_sector(own, wanted):
    count = lax.axis_size("sec")
    offset = lax.axis_index("sec") ^ wanted
    held = {0: own}
    bit = count // 2
    while bit:
        for known in list(held):
            held[known ^ bit] = exchange(held[known], "sec", bit)
        bit //= 2
    result = own
    for known, value in held.items():
        result = jnp.where(offset == known, value, result)
    return result


MESH = pl.DeviceIdType.MESH
DEPTH = 4
PAIRS = 8
LAG = 2
AHEAD = 8
FLOWS = 2 * PAIRS
PARTS = 4
WAVES = DEPTH * PARTS


def steps(stage, step):
    return [(stage, step * PARTS + h) for h in range(PARTS)]


def mixed(*lists):
    return [item for group in zip(*lists) for item in group]


def leaf_order():
    order = steps(0, 0) + mixed(steps(1, 0), steps(0, 1)) + steps(2, 0)
    order += mixed(steps(1, 1), steps(0, 2)) + steps(2, 1) + steps(1, 2)
    return order + steps(0, 3) + steps(2, 2) + steps(1, 3) + steps(2, 3)


def mid_order():
    order = steps(0, 0) + steps(0, 1) + steps(0, 2) + steps(1, 0) + steps(2, 0) + steps(0, 3)
    return order + steps(1, 1) + mixed(steps(2, 1), steps(1, 2)) + mixed(steps(2, 2), steps(1, 3)) + steps(2, 3)


def quantize(value):
    top = jnp.maximum(jnp.max(jnp.abs(value), axis=0, keepdims=True), jnp.float32(1e-30))
    levels = jnp.round(value * (jnp.float32(32766.0) / top))
    return levels.astype(jnp.int32).astype(jnp.int16), top * jnp.float32(1.0 / 32766.0)


def remote(source, target, send, receive, device):
    return pltpu.make_async_remote_copy(
        src_ref=source,
        dst_ref=target,
        send_sem=send,
        recv_sem=receive,
        device_id=device,
        device_id_type=MESH,
    )


def greet(device):
    pl.semaphore_signal(pltpu.get_barrier_semaphore(), inc=1, device_id=device, device_id_type=MESH)


def source_of(map_ref, op, sec):
    found = jnp.int32(0)
    for sector in range(map_ref.shape[0]):
        found = jnp.where(map_ref[sector, op] == sec, sector, found)
    return found


def before(limit, width, dtype):
    lane = lax.broadcasted_iota(jnp.int32, (1, width), 1)
    return jnp.where(lane < limit, 1.0, 0.0).astype(jnp.float32).astype(dtype)


def split(value, parts):
    pieces = []
    for _ in range(parts):
        piece = value.astype(jnp.bfloat16)
        value = value - piece.astype(jnp.float32)
        pieces.append(piece)
    return pieces


def left_terms(value, axis, parts=3):
    p = split(value, parts)
    order = (p[0], p[0], p[1]) if parts == 2 else (p[0], p[0], p[1], p[0], p[2], p[1])
    return jnp.concatenate(order, axis=axis)


def right_terms(value, axis, parts=3):
    p = split(value, parts)
    order = (p[0], p[1], p[0]) if parts == 2 else (p[0], p[1], p[0], p[2], p[0], p[1])
    return jnp.concatenate(order, axis=axis)


def contract(a, b, i, j):
    return lax.dot_general(a, b, (((i,), (j,)), ((), ())), preferred_element_type=jnp.float32)


def eliminate_pairs(tile, beside=()):
    count = LANES // ROWS
    row = lax.broadcasted_iota(jnp.int32, (ROWS, LANES), 0)
    lane = lax.broadcasted_iota(jnp.int32, (ROWS, LANES), 1)
    left = [tile[ROWS * q : ROWS * (q + 1), :] for q in range(count)]
    right = [jnp.where(lane == row + ROWS * q, 1.0, 0.0).astype(jnp.float32) for q in range(count)]

    def lane_of(value, j):
        return jnp.broadcast_to(value[:, j : j + 1], (ROWS, LANES))

    def row_of(value, j):
        return jnp.broadcast_to(value[j : j + 1, :], (ROWS, LANES))

    for s in range(count // 2):
        for extra in beside[s :: count // 2]:
            extra()
        base = 2 * ROWS * s
        ua, la, ub, lb = left[2 * s], right[2 * s], left[2 * s + 1], right[2 * s + 1]
        ca = [lane_of(ua, base + j) for j in range(ROWS)]
        cb = [lane_of(ub, base + j) for j in range(2 * ROWS)]
        for j in range(ROWS):
            scale = lax.rsqrt(row_of(ca[j], j))
            fa = jnp.where(row > j, ca[j] * scale, 0.0)
            fb = cb[j] * scale
            for k in range(j + 1, ROWS):
                own = row_of(ca[k], j) * scale
                ca[k] = ca[k] - fa * own
                cb[k] = cb[k] - fb * own
            for k in range(ROWS):
                cb[ROWS + k] = cb[ROWS + k] - fb * row_of(fb, k)
            own_u = row_of(ua, j) * scale
            own_l = row_of(la, j) * scale
            ua = jnp.where(row == j, own_u, ua - fa * own_u)
            la = jnp.where(row == j, own_l, la - fa * own_l)
            ub = ub - fb * own_u
            lb = lb - fb * own_l
        cb = cb[ROWS:]
        for j in range(ROWS):
            scale = lax.rsqrt(row_of(cb[j], j))
            fb = jnp.where(row > j, cb[j] * scale, 0.0)
            for k in range(j + 1, ROWS):
                cb[k] = cb[k] - fb * (row_of(cb[k], j) * scale)
            own_u = row_of(ub, j) * scale
            own_l = row_of(lb, j) * scale
            ub = jnp.where(row == j, own_u, ub - fb * own_u)
            lb = jnp.where(row == j, own_l, lb - fb * own_l)
        right[2 * s], right[2 * s + 1] = la, lb
        if 2 * s + 2 < count:
            upper = jnp.concatenate([ua, ub], axis=0)
            lower = jnp.concatenate([la, lb], axis=0)
            both = jnp.concatenate([right_terms(upper, 0), right_terms(lower, 0)], axis=1)
            flipped = left_terms(upper, 0).T
            for first, last in ((2 * s + 2, 2 * s + 4), (2 * s + 4, count)):
                if first == last:
                    continue
                change = contract(flipped[ROWS * first : ROWS * last, :], both, 1, 0)
                for q in range(first, last):
                    part = change[ROWS * (q - first) : ROWS * (q - first + 1), :]
                    left[q] = left[q] - part[:, :LANES]
                    right[q] = right[q] - part[:, LANES:]
    return jnp.concatenate(right, axis=0)


def image_kernel(sizes_hbm, counts_hbm, map_hbm, top_hbm, bottom_hbm, own_hbm, blocks_hbm, guess_hbm, tile_ref, rotated_ref, *refs):
    rows, states = own_hbm.shape
    kept = guess_hbm.shape[1]
    chunk = states // (2 * FLOWS)
    band = rows // PARTS
    sec = lax.axis_index("sec")
    op = lax.axis_index("op")
    y, c = sec // 2, sec % 2
    z, x = op // 2, op % 2
    w = z // 2
    zz = z + w * (3 - 2 * z)
    mid = zz == 1
    leaf = jnp.logical_not(mid)
    sec_over = (1 - y) * 2 + c
    sec_twin = y * 2 + 1 - c
    sec_cross = (1 - y) * 2 + 1 - c
    twin = (sec_twin, op)
    over = (sec_over, op)
    side = (sec, z * 2 + 1 - x)
    inner = (sec, (1 + w) * 2 + x)
    outer = (sec, 6 * w + x)
    other = (sec, (3 - z) * 2 + x)

    (store, picked, landed, moved, blocks, guess, left, high, low) = refs[:9]
    (line_in, side_in, core_in, x_in, fetch_out, load) = refs[9:15]
    refs = refs[15:]
    names = ("give", "take", "own", "inner", "final", "last")
    levels = dict(zip(names, refs[0:6]))
    scales = dict(zip(names, refs[6:12]))
    arrivals = dict(zip(("take", "inner", "final", "last"), refs[12:16]))
    departures, measure_ref, part_ref = refs[16:19]
    scalars = refs[19:24]
    own_ref, out_ref, work, near_terms, far_terms, basis, basis_mid, basis_full, mapped, panel_ref, inverse_ref, q_in, q_out = refs[24:37]
    load_own = pltpu.make_async_copy(own_hbm, own_ref, load.at[7])
    load_own.start()
    sizes_ref, counts_ref, map_ref, top_ref, bottom_ref = scalars
    loads = [
        pltpu.make_async_copy(source, target, load.at[2 + i])
        for i, (source, target) in enumerate(zip((sizes_hbm, counts_hbm, map_hbm, top_hbm, bottom_hbm), scalars))
    ]
    for copy in loads:
        copy.start()

    load_blocks = pltpu.make_async_copy(blocks_hbm, blocks, load.at[0])
    load_guess = pltpu.make_async_copy(guess_hbm, guess, load.at[1])
    load_blocks.start()
    load_guess.start()
    barrier = pltpu.get_barrier_semaphore()
    greet(twin)
    greet(over)
    greet(side)

    @pl.when(mid)
    def _():
        greet(other)
        greet(outer)
        pl.semaphore_wait(barrier, 5)

    @pl.when(leaf)
    def _():
        greet(inner)
        pl.semaphore_wait(barrier, 4)

    for copy in loads:
        copy.wait()
    wanted = source_of(map_ref, op, sec)
    beside = source_of(map_ref, op + 1 - 2 * x, sec)
    source_mask = before(sizes_ref[wanted], states, jnp.bfloat16)
    own_size = sizes_ref[sec]
    own_mask = before(own_size, states, jnp.bfloat16)

    marks = [zz, 1 - zz, 2, 3]
    place = [q + w * (3 - 2 * q) for q in marks]

    def slot(v, sector):
        return store.at[(place[v // PARTS] * 4 + sector) * PARTS + v % PARTS]

    def piece(v):
        if v < PARTS:
            return own_ref.at[pl.ds(v * band, band)]
        return slot(v, sec)

    def line_sem(v):
        return line_in.at[place[v // PARTS] * PARTS + v % PARTS]

    def along(v, device):
        return remote(piece(v), slot(v, sec), fetch_out.at[0], line_sem(v), device)

    def across(v):
        return remote(piece(v), slot(v, sec), fetch_out.at[1], side_in.at[v], over)

    def to_twin(v):
        return remote(piece(v), slot(v, sec), fetch_out.at[1], core_in.at[v], twin)

    def to_twin_second(v):
        return remote(slot(v, sec_over), slot(v, sec_over), fetch_out.at[1], core_in.at[v], twin)

    def to_side(v):
        return remote(picked.at[v], landed.at[v], fetch_out.at[1], x_in.at[v], side)

    def first(v):
        step = v // PARTS
        if step == 0:

            @pl.when(mid)
            def _():
                along(v, other).start()
                along(v, outer).start()

            @pl.when(leaf)
            def _():
                along(v, inner).start()
        else:
            remote(slot(v, sec), slot(v, sec), fetch_out.at[0], line_sem(v), side).wait_recv()

            @pl.when(mid)
            def _():
                along(v, other if step == 1 else outer).start()

        across(v).start()
        to_twin(v).start()

    def second(v):
        remote(slot(v, sec_over), slot(v, sec_over), fetch_out.at[1], side_in.at[v], over).wait_recv()
        to_twin_second(v).start()

    def choose(v, sector_wanted):
        base = place[v // PARTS] * 4
        value = store[(base + 3) * PARTS + v % PARTS]
        for sector in range(3):
            value = jnp.where(sector_wanted == sector, store[(base + sector) * PARTS + v % PARTS], value)
        return value

    def third(v):
        both = store.at[pl.ds(0, 2)]
        remote(both, both, fetch_out.at[1], core_in.at[v], twin).wait_recv()
        picked[v] = choose(v, beside)
        to_side(v).start()
        moved[pl.ds(v * band, band), :] = choose(v, wanted) * source_mask

    def perturb(first_row, count):
        span = pl.ds(first_row, count)

        def step(n, carry):
            lanes = pl.ds(pl.multiple_of(n * 256, 256), 256)
            value = jnp.dot(moved[span, :], blocks[:, lanes], preferred_element_type=jnp.float32)
            lane = lax.broadcasted_iota(jnp.int32, (1, 256), 1) + n * 256
            keep = jnp.where(lane < own_size, 1.0, 0.0).astype(jnp.float32).astype(jnp.bfloat16)
            left[span, lanes] = value.astype(jnp.bfloat16) * keep
            return carry

        lax.fori_loop(0, states // 256, step, 0)

    load_own.wait()
    for v in range(PARTS):
        store[(place[0] * 4 + sec) * PARTS + v] = own_ref[pl.ds(v * band, band), :]
    left[pl.ds(2 * DEPTH * rows, rows), :] = own_ref[...] * own_mask
    def run(order):
        for stage, v in order:
            (first, second, third)[stage](v)

    @pl.when(leaf)
    def _():
        run(leaf_order())

    @pl.when(mid)
    def _():
        run(mid_order())

    load_blocks.wait()
    load_guess.wait()
    perturb(0, DEPTH * rows)
    weight = jnp.full((1, kept), top_ref[0], jnp.int32).astype(jnp.float32) / jnp.full(
        (1, kept), bottom_ref[0], jnp.int32
    ).astype(jnp.float32)
    kept_mask = before(counts_ref[sec], kept, jnp.float32)

    def project(first_row, count, factor):
        span = pl.ds(first_row, count)
        value = jnp.dot(left[span, :], guess[...], preferred_element_type=jnp.float32) * factor
        top_half = value.astype(jnp.bfloat16)
        high[span, :] = top_half
        low[span, :] = (value - top_half.astype(jnp.float32)).astype(jnp.bfloat16)

    project(0, DEPTH * rows, weight * kept_mask)
    project(2 * DEPTH * rows, rows, kept_mask)
    for early, late in ((0, WAVES - PARTS), (WAVES - PARTS, WAVES)):
        for v in range(early, late):
            to_side(v).wait_recv()
            moved[pl.ds(DEPTH * rows + v * band, band), :] = landed[v] * source_mask
        perturb(DEPTH * rows + early * band, (late - early) * band)
        project(DEPTH * rows + early * band, (late - early) * band, weight * kept_mask)

    def product(n):
        lanes = pl.ds(pl.multiple_of(n * 256, 256), 256)
        dims = (((0,), (0,)), ((), ()))
        value = lax.dot_general(left[:, lanes], high[...], dims, preferred_element_type=jnp.float32)
        part_ref[lanes, :] = value + lax.dot_general(
            left[:, lanes], low[...], dims, preferred_element_type=jnp.float32
        )

    def start(source, i, target, j, lane, device, flag=None):
        flag = arrivals[target].at[j if flag is None else flag]
        for n, bufs in enumerate((levels, scales)):
            remote(bufs[source].at[i], bufs[target].at[j], departures.at[lane, n], flag, device).start()

    def arrived(target, j, ref=measure_ref.at[0]):
        remote(ref, ref, departures.at[0, 0], arrivals[target].at[j], side).wait_recv()

    def put(name, i, value):
        whole, scale = quantize(value)
        levels[name][i] = whole
        scales[name][i] = scale

    def get(name, i):
        return levels[name][i].astype(jnp.int32).astype(jnp.float32) * scales[name][i]

    def chunk_rows(half, i):
        return pl.ds(pl.multiple_of((FLOWS * half + i) * chunk, chunk), chunk)

    def value(i):
        arrived("take", i)
        return part_ref[chunk_rows(x, i), :] + get("take", i)

    def finish(i):
        start("final", i, "last", i, 0, side)
        out_ref[chunk_rows(x, i), :] = get("final", i)

    def give(i):
        put("give", i, part_ref[chunk_rows(1 - x, i), :])
        start("give", i, "take", i, 0, side)

    tiles = states // 256
    for n in range(tiles // 2):
        product((1 - x) * (tiles // 2) + n)
        if n == 0:
            for i in range(AHEAD):
                give(i)
    for n in range(tiles // 2):
        product(x * (tiles // 2) + n)

    span = LANES
    blocks_count = kept // span
    tall = states // 4

    def correlate(n, carry):
        image = out_ref[pl.ds(pl.multiple_of(n * tall, tall), tall), :]
        terms = left_terms(image, 0)
        others = right_terms(image, 0)
        middle = kept // 2
        work[:middle, :] = work[:middle, :] + contract(terms[:, :middle], others, 0, 0)
        work[middle:, middle:] = work[middle:, middle:] + contract(terms[:, middle:], others[:, middle:], 0, 0)
        return carry

    diagonal = lax.broadcasted_iota(jnp.int32, (kept, kept), 0) == lax.broadcasted_iota(jnp.int32, (kept, kept), 1)
    work[...] = jnp.where(diagonal, 1.0 - kept_mask, 0.0)

    @pl.when(leaf)
    def _():
        for i in range(FLOWS):
            if i + AHEAD < FLOWS:
                give(i + AHEAD)
            put("own", i, value(i))
            far = w if i % 2 == 0 else 1 - w
            start("own", i, "inner", FLOWS * far + i, 1, inner, i)
        for i in range(FLOWS):
            arrived("final", i)
            finish(i)
            if i == FLOWS // 2 + 1:
                correlate(2 * x, 0)

    @pl.when(mid)
    def _():
        def relay(p):
            i = 2 * p + 1 - w
            mine = value(i)
            arrived("inner", i)
            put("own", i, mine + get("inner", FLOWS + i))
            start("own", i, "inner", FLOWS + i, 1, other, i)

        def collect(p):
            i = 2 * p + w
            near = value(i)
            arrived("inner", i, measure_ref)
            put("final", i, near + get("inner", i) + get("inner", FLOWS + i))
            start("final", i, "final", i, 1, outer)
            start("final", i, "final", i, 1, other)
            finish(i)

        def forward(p):
            i = 2 * p + 1 - w
            arrived("final", i)
            start("final", i, "final", i, 1, outer)
            finish(i)

        for p in range(PAIRS + 2 * LAG):
            if p < PAIRS:
                for i in range(2 * p + AHEAD, min(2 * p + AHEAD + 2, FLOWS)):
                    give(i)
                relay(p)
            if LAG <= p < PAIRS + LAG:
                collect(p - LAG)
            if p >= 2 * LAG:
                forward(p - 2 * LAG)
            if p == PAIRS // 2 + 2 * LAG:
                correlate(2 * x, 0)


    correlate(2 * x + 1, 0)
    for n in range(2):
        for i in range(n * FLOWS // 2, (n + 1) * FLOWS // 2):
            arrived("last", i)
            out_ref[chunk_rows(1 - x, i), :] = get("last", i)
        correlate(2 * (1 - x) + n, 0)

    def q_over(b):
        return remote(basis.at[0, b], basis.at[1, b], q_out, q_in.at[0, b], over)

    def q_twin(b):
        return remote(basis.at[0, b], basis.at[2, b], q_out, q_in.at[1, b], twin)

    def q_cross(b):
        return remote(basis.at[1, b], basis.at[3, b], q_out, q_in.at[2, b], twin)

    def half_of(which):
        return pl.ds(pl.multiple_of(which * (states // 2), states // 2), states // 2)

    def q_half(b, ref, which, i, device):
        some = half_of(which)
        return remote(basis.at[ref, b, some], basis.at[1, b, some], q_out, q_in.at[i, b], device)

    def pass_half(b):
        q_half(b, 0, x, 0, over).wait_recv()
        q_half(b, 1, x, 3, side).start()

    def pass_on(b):
        q_half(b, 1, 1 - x, 3, side).wait_recv()
        q_cross(b).start()

    def update(b, i):
        below = pl.ds(pl.multiple_of(i * span, span), span)

        def part(n, deeper):
            wide = pl.ds(pl.multiple_of(n * 2 * span, 2 * span), 2 * span)
            work[below, wide] = work[below, wide] - contract(near_terms[:, below], far_terms[:, wide], 0, 0)
            return deeper

        lax.fori_loop(i // 2, blocks_count // 2, part, 0)

    def factor_step(b, carry):
        lanes = pl.ds(pl.multiple_of(b * span, span), span)
        inverse = inverse_ref[...]
        panel = contract(left_terms(inverse, 1), right_terms(work[lanes, :], 0), 1, 0)
        inverse_terms = right_terms(inverse, 1, 2)
        panel_ref[...] = right_terms(panel, 0, 2)
        near_terms[...] = left_terms(panel, 0)
        far_terms[...] = right_terms(panel, 0)

        def orthogonal(n, inner):
            some = pl.ds(pl.multiple_of(n * tall, tall), tall)
            columns = contract(left_terms(out_ref[some, lanes], 1, 2), inverse_terms, 1, 1)
            basis_full[some, :] = columns
            whole = columns.astype(jnp.bfloat16)
            basis[0, b, some, :] = whole
            basis_mid[some, :] = (columns - whole.astype(jnp.float32)).astype(jnp.bfloat16)
            return inner

        lax.fori_loop(0, 4, orthogonal, 0)
        @pl.when(b + 1 < blocks_count)
        def _():
            q_half(b, 0, x, 0, over).start()

        @pl.when(b + 1 == blocks_count)
        def _():
            q_over(b).start()

        q_twin(b).start()
        height = tile_ref.shape[0]
        mine = pl.ds(pl.multiple_of(op * height, height), height)
        tile_ref[:, lanes] = basis_full[mine, :] * float(states) ** 0.5

        @pl.when(b + 1 < blocks_count)
        def _():
            update(b, b + 1)

            def spread_out(m, n):
                some = pl.ds(m * tall, tall)
                wide = pl.ds(n * 2 * span, 2 * span)
                whole = basis[0, b, some, :]
                terms = jnp.concatenate([whole, whole, basis_mid[some, :]], axis=1)
                out_ref[some, wide] = out_ref[some, wide] - contract(terms, panel_ref[:, wide], 1, 0)

            following = pl.ds(pl.multiple_of((b + 1) * span, span), span)
            beside = [functools.partial(spread_out, m, n) for n in range(kept // (2 * span)) for m in range(4)]

            def late_update(ahead):
                valid = jnp.where(b + ahead < blocks_count, 1.0, 0.0).astype(jnp.float32)
                below = pl.ds(pl.multiple_of(jnp.minimum(b + ahead, blocks_count - 1) * span, span), span)
                wide = pl.ds(kept // 2, kept // 2)
                work[below, wide] = work[below, wide] - valid * contract(
                    near_terms[:, below], far_terms[:, wide], 0, 0
                )

            beside += [functools.partial(late_update, ahead) for ahead in range(2, blocks_count)]
            inverse_ref[...] = eliminate_pairs(work[following, following], beside)

        @pl.when(b > 0)
        def _():
            pass_half(b - 1)

        @pl.when((b > 1) & (b + 1 < blocks_count))
        def _():
            pass_on(b - 2)

        return carry

    inverse_ref[...] = eliminate_pairs(work[pl.ds(0, span), pl.ds(0, span)])
    lax.fori_loop(0, blocks_count, factor_step, 0)

    def rotate(b):
        q_twin(b).wait_recv()
        q_cross(b).wait_recv()
        value = basis[0, b]
        for n, sector in enumerate((sec_over, sec_twin, sec_cross)):
            value = jnp.where(wanted == sector, basis[n + 1, b], value)
        rotated_ref[pl.ds(b * span, span), :] = contract(value, mapped[...], 0, 0)

    def apply(n, carry):
        some = pl.ds(pl.multiple_of(n * tall, tall), tall)
        columns = jnp.concatenate([basis[0, b] for b in range(blocks_count)], axis=1)
        mapped[some, :] = contract(blocks[some, :], columns, 1, 0).astype(jnp.bfloat16)
        return carry

    lax.fori_loop(0, 4, apply, 0)
    pass_on(blocks_count - 3)
    for b in range(blocks_count - 2):
        rotate(b)
    pass_on(blocks_count - 2)
    rotate(blocks_count - 2)
    q_over(blocks_count - 1).wait_recv()
    q_cross(blocks_count - 1).start()
    rotate(blocks_count - 1)

    def sent(ref, sem):
        remote(ref, ref, sem, x_in.at[0], side).wait_send()

    sent(basis.at[pl.ds(0, 3)], q_out)
    sent(store, fetch_out.at[1])
    for n, bufs in enumerate((levels, scales)):
        sent(bufs["inner"], departures.at[0, n])

    @pl.when(mid)
    def _():
        sent(store.at[pl.ds(0, PARTS + WAVES)], fetch_out.at[0])
        for n, bufs in enumerate((levels, scales)):
            sent(bufs["inner"], departures.at[1, n])

    @pl.when(leaf)
    def _():
        sent(store.at[pl.ds(0, PARTS)], fetch_out.at[0])
        for n, bufs in enumerate((levels, scales)):
            sent(bufs["inner"].at[pl.ds(0, FLOWS)], departures.at[1, n])


def publish_kernel(tile_ref, rotated_ref, tile_out, rotated_out, done):
    copies = [
        pltpu.make_async_copy(source, target, done.at[i])
        for i, (source, target) in enumerate(((tile_ref, tile_out), (rotated_ref, rotated_out)))
    ]
    for copy in copies:
        copy.start()
    for copy in copies:
        copy.wait()


def publish(tile, rotated):
    return pl.pallas_call(
        publish_kernel,
        out_shape=tuple(jax.ShapeDtypeStruct(a.shape, a.dtype) for a in (tile, rotated)),
        in_specs=[pl.BlockSpec(memory_space=pltpu.VMEM)] * 2,
        out_specs=(pl.BlockSpec(memory_space=pl.ANY),) * 2,
        scratch_shapes=[pltpu.SemaphoreType.DMA((2,))],
        compiler_params=pltpu.CompilerParams(vmem_limit_bytes=2 * 1024 * 1024),
        name="publish",
    )(tile, rotated)


def whole_kernel(own, blocks, guess, sizes, counts, target_map, top, bottom):
    rows, states = own.shape
    kept = guess.shape[1]
    chunk = states // (2 * FLOWS)
    lengths = (FLOWS, FLOWS, FLOWS, 2 * FLOWS, FLOWS, FLOWS)
    sem = pltpu.SemaphoreType.DMA
    half = own.dtype
    total = 2 * DEPTH * rows
    pieces = kept // LANES
    scratch = [
        pltpu.VMEM((16 * PARTS, rows // PARTS, states), half),
        pltpu.VMEM((WAVES, rows // PARTS, states), half),
        pltpu.VMEM((WAVES, rows // PARTS, states), half),
        pltpu.VMEM((total, states), half),
        pltpu.VMEM((states, states), half),
        pltpu.VMEM((states, kept), half),
        pltpu.VMEM((total + rows, states), half),
        pltpu.VMEM((total + rows, kept), half),
        pltpu.VMEM((total + rows, kept), half),
    ]
    scratch += [sem((WAVES,))] * 4 + [sem((2,)), sem((8,))]
    scratch += [pltpu.VMEM((n, chunk, kept), jnp.int16) for n in lengths]
    scratch += [pltpu.VMEM((n, 1, kept), jnp.float32) for n in lengths]
    scratch += [sem((n,)) for n in (FLOWS, FLOWS, FLOWS, FLOWS)]
    scratch += [sem((2, 2)), pltpu.VMEM((2, 1, chunk * kept // 2 + kept), jnp.float32), pltpu.VMEM((states, kept), jnp.float32)]
    scratch += [pltpu.SMEM(a.shape, jnp.int32) for a in (sizes, counts, target_map, top, bottom)]
    scratch += [
        pltpu.VMEM((rows, states), half),
        pltpu.VMEM((states, kept), jnp.float32),
        pltpu.VMEM((kept, kept), jnp.float32),
        pltpu.VMEM((6 * LANES, kept), half),
        pltpu.VMEM((6 * LANES, kept), half),
        pltpu.VMEM((4, pieces, states, LANES), half),
        pltpu.VMEM((states, LANES), half),
        pltpu.VMEM((states, LANES), jnp.float32),
        pltpu.VMEM((states, kept), half),
        pltpu.VMEM((3 * LANES, kept), half),
        pltpu.VMEM((LANES, LANES), jnp.float32),
        sem((4, pieces)),
        sem,
    ]
    return pl.pallas_call(
        image_kernel,
        out_shape=(
            pltpu.VMEM((states // lax.axis_size("op"), kept), jnp.float32),
            pltpu.VMEM((kept, kept), jnp.float32),
        ),
        in_specs=[pl.BlockSpec(memory_space=pltpu.HBM)] * 8,
        out_specs=[pl.BlockSpec(memory_space=pltpu.VMEM)] * 2,
        scratch_shapes=scratch,
        compiler_params=pltpu.CompilerParams(
            collective_id=1, has_side_effects=True, vmem_limit_bytes=60 * 1024 * 1024
        ),
        name="truncate_and_rotate",
    )(sizes, counts, target_map, top, bottom, own, blocks, guess)


def body(
    wavefunction,
    op_blocks,
    basis_guess,
    sector_sizes,
    kept_counts,
    target_map,
    noise_numerator,
    noise_denominator,
):
    if lax.axis_size("op") == 2 * DEPTH and lax.axis_size("sec") == 4:
        tile, rotated = whole_kernel(
            wavefunction[0],
            op_blocks[0, 0],
            basis_guess[0],
            sector_sizes,
            kept_counts,
            target_map.T,
            noise_numerator,
            noise_denominator,
        )
        tile, rotated = publish(tile, rotated)
        return (tile[None], rotated[None, None])
    state_count = wavefunction.shape[2]
    kept_width = basis_guess.shape[2]
    tile_rows = state_count // lax.axis_size("op")
    sec_index = lax.axis_index("sec")
    op_index = lax.axis_index("op")
    noise_weight = noise_numerator[0].astype(jnp.float32) / noise_denominator[0].astype(jnp.float32)
    sources = source_sectors(target_map)
    wanted_all = lax.dynamic_index_in_dim(sources, sec_index, 1, keepdims=False)[None, :]
    wanted = lax.dynamic_index_in_dim(wanted_all[0], op_index, 0, keepdims=False)
    states = jnp.arange(state_count, dtype=jnp.int32)
    own_size = lax.dynamic_index_in_dim(sector_sizes, sec_index, 0, keepdims=False)
    source_size = lax.dynamic_index_in_dim(sector_sizes, wanted, 0, keepdims=False)
    own_count = lax.dynamic_index_in_dim(kept_counts, sec_index, 0, keepdims=False)
    own_kept = jnp.arange(kept_width, dtype=jnp.int32) < own_count
    zero_half = jnp.zeros((), jnp.bfloat16)
    own_rows = jnp.where((states < own_size)[None, :], wavefunction[0], zero_half)
    moved = fetch_pieces(wavefunction, wanted_all)[0]
    moved = jnp.where((states < source_size)[None, :], moved, zero_half)
    blocks = op_blocks[0, 0]
    perturbed = jnp.dot(moved, blocks, preferred_element_type=jnp.float32).astype(jnp.bfloat16)
    guess = jnp.where((states < own_size)[:, None], basis_guess[0], zero_half)
    perturbed_guess = noise_weight * jnp.dot(perturbed, guess, preferred_element_type=jnp.float32)
    own_guess = jnp.dot(own_rows, guess, preferred_element_type=jnp.float32)
    part = lax.dot_general(
        jnp.concatenate([perturbed, own_rows], axis=0).astype(jnp.float32),
        jnp.concatenate([perturbed_guess, own_guess], axis=0),
        (((0,), (0,)), ((), ())),
        precision=lax.Precision.HIGH,
    )
    part = jnp.where((states < own_size)[:, None] & own_kept[None, :], part, jnp.float32(0.0))
    full_image = sum_over_op(part)
    padding = jnp.where(own_kept, jnp.float32(0.0), jnp.float32(1.0))
    correlation = dot_ta(full_image, full_image) + padding[:, None] * jnp.eye(
        kept_width, dtype=jnp.float32
    )
    inverse = inverse_factor(correlation)
    new_basis = lax.dot_general(
        full_image, inverse, (((1,), (1,)), ((), ())), precision=lax.Precision.HIGH
    )
    kept_tile = (
        lax.dynamic_slice_in_dim(new_basis, op_index * tile_rows, tile_rows, 0)
        * float(state_count) ** 0.5
    )
    basis_half = new_basis.astype(jnp.bfloat16)
    mapped = jnp.dot(blocks, basis_half, preferred_element_type=jnp.float32).astype(jnp.bfloat16)
    source_basis = fetch_sector(basis_half, wanted)
    rotated = lax.dot_general(
        source_basis, mapped, (((0,), (0,)), ((), ())), preferred_element_type=jnp.float32
    )
    return (kept_tile[None], rotated[None, None])


def solution(mesh):
    placed = (
        P("sec", "op", None),
        P("op", "sec", None, None),
        P("sec", None, None),
        P(),
        P(),
        P(),
        P(),
        P(),
    )
    return jax.shard_map(
        body,
        mesh=mesh,
        in_specs=placed,
        out_specs=(P("sec", "op", None), P("op", "sec", None, None)),
        check_vma=False,
    )
```

```python
import functools

import jax
import jax.numpy as jnp
from jax import lax
from jax.experimental import pallas as pl
from jax.experimental.pallas import tpu as pltpu
from jax.sharding import PartitionSpec as P

LANES = 128
ROWS = 8
HIGHEST = lax.Precision.HIGHEST


def dot_ta(a, b):
    return lax.dot_general(
        a, b, (((0,), (0,)), ((), ())), precision=HIGHEST, preferred_element_type=jnp.float32
    )


def dot(a, b):
    return jnp.dot(a, b, precision=HIGHEST, preferred_element_type=jnp.float32)


def eliminate_tile(tile):
    count = LANES // ROWS
    row = lax.broadcasted_iota(jnp.int32, (ROWS, LANES), 0)
    lane = lax.broadcasted_iota(jnp.int32, (ROWS, LANES), 1)
    left = [tile[ROWS * q : ROWS * (q + 1), :] for q in range(count)]
    right = [jnp.where(lane == row + ROWS * q, 1.0, 0.0).astype(jnp.float32) for q in range(count)]
    for p in range(count):
        upper, lower = left[p], right[p]
        columns = [
            jnp.broadcast_to(upper[:, ROWS * p + j : ROWS * p + j + 1], (ROWS, LANES))
            for j in range(ROWS)
        ]
        for j in range(ROWS):
            scale = lax.rsqrt(jnp.broadcast_to(columns[j][j : j + 1, :], (ROWS, LANES)))
            factor = jnp.where(row > j, columns[j] * scale, 0.0)
            for k in range(j + 1, ROWS):
                own = jnp.broadcast_to(columns[k][j : j + 1, :], (ROWS, LANES)) * scale
                columns[k] = columns[k] - factor * own
            own_upper = jnp.broadcast_to(upper[j : j + 1, :], (ROWS, LANES)) * scale
            own_lower = jnp.broadcast_to(lower[j : j + 1, :], (ROWS, LANES)) * scale
            upper = jnp.where(row == j, own_upper, upper - factor * own_upper)
            lower = jnp.where(row == j, own_lower, lower - factor * own_lower)
        right[p] = lower
        if p + 1 < count:
            change = dot_ta(upper, jnp.concatenate([upper, lower], axis=1))
            for q in range(p + 1, count):
                part = change[ROWS * q : ROWS * (q + 1), :]
                left[q] = left[q] - part[:, :LANES]
                right[q] = right[q] - part[:, LANES:]
    return jnp.concatenate(right, axis=0)


def inverse_factor_kernel(matrix_ref, out_ref, work):
    size = matrix_ref.shape[0]
    blocks = size // LANES
    work[:, :size] = matrix_ref[...]
    work[:, size:] = (
        lax.broadcasted_iota(jnp.int32, (size, size), 0)
        == lax.broadcasted_iota(jnp.int32, (size, size), 1)
    ).astype(jnp.float32)

    def step(b, carry):
        rows = pl.ds(pl.multiple_of(b * LANES, LANES), LANES)
        inverse = eliminate_tile(work[rows, rows])
        panel = dot(inverse, work[rows, :])
        work[rows, :] = panel
        out_ref[rows, :] = panel[:, size:]

        def update(i, inner):
            below = pl.ds(pl.multiple_of(i * LANES, LANES), LANES)
            work[below, :] = work[below, :] - dot_ta(work[rows, below], work[rows, :])
            return inner

        lax.fori_loop(b + 1, blocks, update, 0)
        return carry

    lax.fori_loop(0, blocks, step, 0)


def inverse_factor(matrix):
    size = matrix.shape[0]
    return pl.pallas_call(
        inverse_factor_kernel,
        out_shape=jax.ShapeDtypeStruct((size, size), jnp.float32),
        in_specs=[pl.BlockSpec(memory_space=pltpu.VMEM)],
        out_specs=pl.BlockSpec(memory_space=pltpu.VMEM),
        scratch_shapes=[pltpu.VMEM((size, 2 * size), jnp.float32)],
        compiler_params=pltpu.CompilerParams(vmem_limit_bytes=24 * 1024 * 1024),
        cost_estimate=pl.CostEstimate(flops=2 * size**3, bytes_accessed=8 * size * size, transcendentals=size),
        name="inverse_factor",
    )(matrix)


def source_sectors(target_map):
    sectors = jnp.arange(target_map.shape[1], dtype=jnp.int32)
    matches = target_map[:, :, None] == sectors[None, None, :]
    return jnp.sum(jnp.where(matches, sectors[None, :, None], 0), axis=1)


def fetch_pieces(own_slice, wanted_all):
    everyone = lax.all_gather(own_slice, "sec", axis=0, tiled=True)
    outgoing = jnp.take(everyone, wanted_all, axis=0)
    incoming = lax.all_to_all(outgoing, "op", split_axis=1, concat_axis=1, tiled=True)
    return incoming.reshape(
        incoming.shape[0], incoming.shape[1] * incoming.shape[2], incoming.shape[3]
    )


def exchange(value, axis, bit):
    count = lax.axis_size(axis)
    return lax.ppermute(value, axis, [(i, i ^ bit) for i in range(count)])


def halves(value, side):
    half = value.shape[0] // 2
    kept = lax.dynamic_slice_in_dim(value, side * half, half, 0)
    given = lax.dynamic_slice_in_dim(value, (1 - side) * half, half, 0)
    return kept, given


def sum_over_op(value):
    count = lax.axis_size("op")
    index = lax.axis_index("op")
    bits = [1 << b for b in range(count.bit_length() - 1)]
    orders = [bits, bits[1:] + bits[:1]]
    half = value.shape[0] // 2
    held = [value[:half], value[half:]]
    for step in range(len(bits)):
        for color, order in enumerate(orders):
            kept, given = halves(held[color], (index // order[step]) % 2)
            held[color] = kept + exchange(given, "op", order[step])
    for step in reversed(range(len(bits))):
        for color, order in enumerate(orders):
            own = held[color]
            other = exchange(own, "op", order[step])
            first = (index // order[step]) % 2 == 0
            held[color] = jnp.concatenate(
                [jnp.where(first, own, other), jnp.where(first, other, own)], axis=0
            )
    return jnp.concatenate(held, axis=0)


def fetch_sector(own, wanted):
    count = lax.axis_size("sec")
    offset = lax.axis_index("sec") ^ wanted
    held = {0: own}
    bit = count // 2
    while bit:
        for known in list(held):
            held[known ^ bit] = exchange(held[known], "sec", bit)
        bit //= 2
    result = own
    for known, value in held.items():
        result = jnp.where(offset == known, value, result)
    return result


MESH = pl.DeviceIdType.MESH
DEPTH = 4
PAIRS = 8
LAG = 2
AHEAD = 8
FLOWS = 2 * PAIRS
PARTS = 4
WAVES = DEPTH * PARTS


def steps(stage, step):
    return [(stage, step * PARTS + h) for h in range(PARTS)]


def mixed(*lists):
    return [item for group in zip(*lists) for item in group]


def leaf_order():
    order = steps(0, 0) + mixed(steps(1, 0), steps(0, 1)) + steps(2, 0)
    order += mixed(steps(1, 1), steps(0, 2)) + steps(2, 1) + steps(1, 2)
    return order + steps(0, 3) + steps(2, 2) + steps(1, 3) + steps(2, 3)


def mid_order():
    order = steps(0, 0) + steps(0, 1) + steps(0, 2) + steps(1, 0) + steps(2, 0) + steps(0, 3)
    return order + steps(1, 1) + mixed(steps(2, 1), steps(1, 2)) + mixed(steps(2, 2), steps(1, 3)) + steps(2, 3)


def quantize(value):
    top = jnp.maximum(jnp.max(jnp.abs(value), axis=0, keepdims=True), jnp.float32(1e-30))
    levels = jnp.round(value * (jnp.float32(32766.0) / top))
    return levels.astype(jnp.int32).astype(jnp.int16), top * jnp.float32(1.0 / 32766.0)


def remote(source, target, send, receive, device):
    return pltpu.make_async_remote_copy(
        src_ref=source,
        dst_ref=target,
        send_sem=send,
        recv_sem=receive,
        device_id=device,
        device_id_type=MESH,
    )


def greet(device):
    pl.semaphore_signal(pltpu.get_barrier_semaphore(), inc=1, device_id=device, device_id_type=MESH)


def source_of(map_ref, op, sec):
    found = jnp.int32(0)
    for sector in range(map_ref.shape[0]):
        found = jnp.where(map_ref[sector, op] == sec, sector, found)
    return found


def before(limit, width, dtype):
    lane = lax.broadcasted_iota(jnp.int32, (1, width), 1)
    return jnp.where(lane < limit, 1.0, 0.0).astype(jnp.float32).astype(dtype)


def split(value, parts):
    pieces = []
    for _ in range(parts):
        piece = value.astype(jnp.bfloat16)
        value = value - piece.astype(jnp.float32)
        pieces.append(piece)
    return pieces


def left_terms(value, axis, parts=3):
    p = split(value, parts)
    order = (p[0], p[0], p[1]) if parts == 2 else (p[0], p[0], p[1], p[0], p[2], p[1])
    return jnp.concatenate(order, axis=axis)


def right_terms(value, axis, parts=3):
    p = split(value, parts)
    order = (p[0], p[1], p[0]) if parts == 2 else (p[0], p[1], p[0], p[2], p[0], p[1])
    return jnp.concatenate(order, axis=axis)


def contract(a, b, i, j):
    return lax.dot_general(a, b, (((i,), (j,)), ((), ())), preferred_element_type=jnp.float32)


def eliminate_pairs(tile, beside=()):
    count = LANES // ROWS
    row = lax.broadcasted_iota(jnp.int32, (ROWS, LANES), 0)
    lane = lax.broadcasted_iota(jnp.int32, (ROWS, LANES), 1)
    left = [tile[ROWS * q : ROWS * (q + 1), :] for q in range(count)]
    right = [jnp.where(lane == row + ROWS * q, 1.0, 0.0).astype(jnp.float32) for q in range(count)]

    def lane_of(value, j):
        return jnp.broadcast_to(value[:, j : j + 1], (ROWS, LANES))

    def row_of(value, j):
        return jnp.broadcast_to(value[j : j + 1, :], (ROWS, LANES))

    for s in range(count // 2):
        for extra in beside[s :: count // 2]:
            extra()
        base = 2 * ROWS * s
        ua, la, ub, lb = left[2 * s], right[2 * s], left[2 * s + 1], right[2 * s + 1]
        ca = [lane_of(ua, base + j) for j in range(ROWS)]
        cb = [lane_of(ub, base + j) for j in range(2 * ROWS)]
        for j in range(ROWS):
            scale = lax.rsqrt(row_of(ca[j], j))
            fa = jnp.where(row > j, ca[j] * scale, 0.0)
            fb = cb[j] * scale
            for k in range(j + 1, ROWS):
                own = row_of(ca[k], j) * scale
                ca[k] = ca[k] - fa * own
                cb[k] = cb[k] - fb * own
            for k in range(ROWS):
                cb[ROWS + k] = cb[ROWS + k] - fb * row_of(fb, k)
            own_u = row_of(ua, j) * scale
            own_l = row_of(la, j) * scale
            ua = jnp.where(row == j, own_u, ua - fa * own_u)
            la = jnp.where(row == j, own_l, la - fa * own_l)
            ub = ub - fb * own_u
            lb = lb - fb * own_l
        cb = cb[ROWS:]
        for j in range(ROWS):
            scale = lax.rsqrt(row_of(cb[j], j))
            fb = jnp.where(row > j, cb[j] * scale, 0.0)
            for k in range(j + 1, ROWS):
                cb[k] = cb[k] - fb * (row_of(cb[k], j) * scale)
            own_u = row_of(ub, j) * scale
            own_l = row_of(lb, j) * scale
            ub = jnp.where(row == j, own_u, ub - fb * own_u)
            lb = jnp.where(row == j, own_l, lb - fb * own_l)
        right[2 * s], right[2 * s + 1] = la, lb
        if 2 * s + 2 < count:
            upper = jnp.concatenate([ua, ub], axis=0)
            lower = jnp.concatenate([la, lb], axis=0)
            both = jnp.concatenate([right_terms(upper, 0), right_terms(lower, 0)], axis=1)
            flipped = left_terms(upper, 0).T
            for first, last in ((2 * s + 2, 2 * s + 4), (2 * s + 4, count)):
                if first == last:
                    continue
                change = contract(flipped[ROWS * first : ROWS * last, :], both, 1, 0)
                for q in range(first, last):
                    part = change[ROWS * (q - first) : ROWS * (q - first + 1), :]
                    left[q] = left[q] - part[:, :LANES]
                    right[q] = right[q] - part[:, LANES:]
    return jnp.concatenate(right, axis=0)


def image_kernel(sizes_hbm, counts_hbm, map_hbm, top_hbm, bottom_hbm, own_hbm, blocks_hbm, guess_hbm, tile_ref, rotated_ref, *refs):
    rows, states = own_hbm.shape
    kept = guess_hbm.shape[1]
    chunk = states // (2 * FLOWS)
    band = rows // PARTS
    sec = lax.axis_index("sec")
    op = lax.axis_index("op")
    y, c = sec // 2, sec % 2
    z, x = op // 2, op % 2
    w = z // 2
    zz = z + w * (3 - 2 * z)
    mid = zz == 1
    leaf = jnp.logical_not(mid)
    sec_over = (1 - y) * 2 + c
    sec_twin = y * 2 + 1 - c
    sec_cross = (1 - y) * 2 + 1 - c
    twin = (sec_twin, op)
    over = (sec_over, op)
    side = (sec, z * 2 + 1 - x)
    inner = (sec, (1 + w) * 2 + x)
    outer = (sec, 6 * w + x)
    other = (sec, (3 - z) * 2 + x)

    (store, picked, landed, moved, blocks, guess, left, high, low) = refs[:9]
    (line_in, side_in, core_in, x_in, fetch_out, load) = refs[9:15]
    refs = refs[15:]
    names = ("give", "take", "own", "inner", "final", "last")
    levels = dict(zip(names, refs[0:6]))
    scales = dict(zip(names, refs[6:12]))
    arrivals = dict(zip(("take", "inner", "final", "last"), refs[12:16]))
    departures, measure_ref, part_ref = refs[16:19]
    scalars = refs[19:24]
    own_ref, out_ref, work, near_terms, far_terms, basis, basis_mid, basis_full, mapped, panel_ref, inverse_ref, q_in, q_out = refs[24:37]
    load_own = pltpu.make_async_copy(own_hbm, own_ref, load.at[7])
    load_own.start()
    sizes_ref, counts_ref, map_ref, top_ref, bottom_ref = scalars
    loads = [
        pltpu.make_async_copy(source, target, load.at[2 + i])
        for i, (source, target) in enumerate(zip((sizes_hbm, counts_hbm, map_hbm, top_hbm, bottom_hbm), scalars))
    ]
    for copy in loads:
        copy.start()

    load_blocks = pltpu.make_async_copy(blocks_hbm, blocks, load.at[0])
    load_guess = pltpu.make_async_copy(guess_hbm, guess, load.at[1])
    load_blocks.start()
    load_guess.start()
    barrier = pltpu.get_barrier_semaphore()
    greet(twin)
    greet(over)
    greet(side)

    @pl.when(mid)
    def _():
        greet(other)
        greet(outer)
        pl.semaphore_wait(barrier, 5)

    @pl.when(leaf)
    def _():
        greet(inner)
        pl.semaphore_wait(barrier, 4)

    for copy in loads:
        copy.wait()
    wanted = source_of(map_ref, op, sec)
    beside = source_of(map_ref, op + 1 - 2 * x, sec)
    source_mask = before(sizes_ref[wanted], states, jnp.bfloat16)
    own_size = sizes_ref[sec]
    own_mask = before(own_size, states, jnp.bfloat16)

    marks = [zz, 1 - zz, 2, 3]
    place = [q + w * (3 - 2 * q) for q in marks]

    def slot(v, sector):
        return store.at[(place[v // PARTS] * 4 + sector) * PARTS + v % PARTS]

    def piece(v):
        if v < PARTS:
            return own_ref.at[pl.ds(v * band, band)]
        return slot(v, sec)

    def line_sem(v):
        return line_in.at[place[v // PARTS] * PARTS + v % PARTS]

    def along(v, device):
        return remote(piece(v), slot(v, sec), fetch_out.at[0], line_sem(v), device)

    def across(v):
        return remote(piece(v), slot(v, sec), fetch_out.at[1], side_in.at[v], over)

    def to_twin(v):
        return remote(piece(v), slot(v, sec), fetch_out.at[1], core_in.at[v], twin)

    def to_twin_second(v):
        return remote(slot(v, sec_over), slot(v, sec_over), fetch_out.at[1], core_in.at[v], twin)

    def to_side(v):
        return remote(picked.at[v], landed.at[v], fetch_out.at[1], x_in.at[v], side)

    def first(v):
        step = v // PARTS
        if step == 0:

            @pl.when(mid)
            def _():
                along(v, other).start()
                along(v, outer).start()

            @pl.when(leaf)
            def _():
                along(v, inner).start()
        else:
            remote(slot(v, sec), slot(v, sec), fetch_out.at[0], line_sem(v), side).wait_recv()

            @pl.when(mid)
            def _():
                along(v, other if step == 1 else outer).start()

        across(v).start()
        to_twin(v).start()

    def second(v):
        remote(slot(v, sec_over), slot(v, sec_over), fetch_out.at[1], side_in.at[v], over).wait_recv()
        to_twin_second(v).start()

    def choose(v, sector_wanted):
        base = place[v // PARTS] * 4
        value = store[(base + 3) * PARTS + v % PARTS]
        for sector in range(3):
            value = jnp.where(sector_wanted == sector, store[(base + sector) * PARTS + v % PARTS], value)
        return value

    def third(v):
        both = store.at[pl.ds(0, 2)]
        remote(both, both, fetch_out.at[1], core_in.at[v], twin).wait_recv()
        picked[v] = choose(v, beside)
        to_side(v).start()
        moved[pl.ds(v * band, band), :] = choose(v, wanted) * source_mask

    def perturb(first_row, count):
        span = pl.ds(first_row, count)

        def step(n, carry):
            lanes = pl.ds(pl.multiple_of(n * 256, 256), 256)
            value = jnp.dot(moved[span, :], blocks[:, lanes], preferred_element_type=jnp.float32)
            lane = lax.broadcasted_iota(jnp.int32, (1, 256), 1) + n * 256
            keep = jnp.where(lane < own_size, 1.0, 0.0).astype(jnp.float32).astype(jnp.bfloat16)
            left[span, lanes] = value.astype(jnp.bfloat16) * keep
            return carry

        lax.fori_loop(0, states // 256, step, 0)

    load_own.wait()
    for v in range(PARTS):
        store[(place[0] * 4 + sec) * PARTS + v] = own_ref[pl.ds(v * band, band), :]
    left[pl.ds(2 * DEPTH * rows, rows), :] = own_ref[...] * own_mask
    def run(order):
        for stage, v in order:
            (first, second, third)[stage](v)

    @pl.when(leaf)
    def _():
        run(leaf_order())

    @pl.when(mid)
    def _():
        run(mid_order())

    load_blocks.wait()
    load_guess.wait()
    perturb(0, DEPTH * rows)
    weight = jnp.full((1, kept), top_ref[0], jnp.int32).astype(jnp.float32) / jnp.full(
        (1, kept), bottom_ref[0], jnp.int32
    ).astype(jnp.float32)
    kept_mask = before(counts_ref[sec], kept, jnp.float32)

    def project(first_row, count, factor):
        span = pl.ds(first_row, count)
        value = jnp.dot(left[span, :], guess[...], preferred_element_type=jnp.float32) * factor
        top_half = value.astype(jnp.bfloat16)
        high[span, :] = top_half
        low[span, :] = (value - top_half.astype(jnp.float32)).astype(jnp.bfloat16)

    project(0, DEPTH * rows, weight * kept_mask)
    project(2 * DEPTH * rows, rows, kept_mask)
    for early, late in ((0, WAVES - PARTS), (WAVES - PARTS, WAVES)):
        for v in range(early, late):
            to_side(v).wait_recv()
            moved[pl.ds(DEPTH * rows + v * band, band), :] = landed[v] * source_mask
        perturb(DEPTH * rows + early * band, (late - early) * band)
        project(DEPTH * rows + early * band, (late - early) * band, weight * kept_mask)

    def product(n):
        lanes = pl.ds(pl.multiple_of(n * 256, 256), 256)
        dims = (((0,), (0,)), ((), ()))
        value = lax.dot_general(left[:, lanes], high[...], dims, preferred_element_type=jnp.float32)
        part_ref[lanes, :] = value + lax.dot_general(
            left[:, lanes], low[...], dims, preferred_element_type=jnp.float32
        )

    def start(source, i, target, j, lane, device, flag=None):
        flag = arrivals[target].at[j if flag is None else flag]
        for n, bufs in enumerate((levels, scales)):
            remote(bufs[source].at[i], bufs[target].at[j], departures.at[lane, n], flag, device).start()

    def arrived(target, j, ref=measure_ref.at[0]):
        remote(ref, ref, departures.at[0, 0], arrivals[target].at[j], side).wait_recv()

    def put(name, i, value):
        whole, scale = quantize(value)
        levels[name][i] = whole
        scales[name][i] = scale

    def get(name, i):
        return levels[name][i].astype(jnp.int32).astype(jnp.float32) * scales[name][i]

    def chunk_rows(half, i):
        return pl.ds(pl.multiple_of((FLOWS * half + i) * chunk, chunk), chunk)

    def value(i):
        arrived("take", i)
        return part_ref[chunk_rows(x, i), :] + get("take", i)

    def finish(i):
        start("final", i, "last", i, 0, side)
        out_ref[chunk_rows(x, i), :] = get("final", i)

    def give(i):
        put("give", i, part_ref[chunk_rows(1 - x, i), :])
        start("give", i, "take", i, 0, side)

    tiles = states // 256
    for n in range(tiles // 2):
        product((1 - x) * (tiles // 2) + n)
        if n == 0:
            for i in range(AHEAD):
                give(i)
    for n in range(tiles // 2):
        product(x * (tiles // 2) + n)

    span = LANES
    blocks_count = kept // span
    tall = states // 4

    def correlate(n, carry):
        image = out_ref[pl.ds(pl.multiple_of(n * tall, tall), tall), :]
        terms = left_terms(image, 0)
        others = right_terms(image, 0)
        middle = kept // 2
        work[:middle, :] = work[:middle, :] + contract(terms[:, :middle], others, 0, 0)
        work[middle:, middle:] = work[middle:, middle:] + contract(terms[:, middle:], others[:, middle:], 0, 0)
        return carry

    diagonal = lax.broadcasted_iota(jnp.int32, (kept, kept), 0) == lax.broadcasted_iota(jnp.int32, (kept, kept), 1)
    work[...] = jnp.where(diagonal, 1.0 - kept_mask, 0.0)

    @pl.when(leaf)
    def _():
        for i in range(FLOWS):
            if i + AHEAD < FLOWS:
                give(i + AHEAD)
            put("own", i, value(i))
            far = w if i % 2 == 0 else 1 - w
            start("own", i, "inner", FLOWS * far + i, 1, inner, i)
        for i in range(FLOWS):
            arrived("final", i)
            finish(i)
            if i == FLOWS // 2 + 1:
                correlate(2 * x, 0)

    @pl.when(mid)
    def _():
        def relay(p):
            i = 2 * p + 1 - w
            mine = value(i)
            arrived("inner", i)
            put("own", i, mine + get("inner", FLOWS + i))
            start("own", i, "inner", FLOWS + i, 1, other, i)

        def collect(p):
            i = 2 * p + w
            near = value(i)
            arrived("inner", i, measure_ref)
            put("final", i, near + get("inner", i) + get("inner", FLOWS + i))
            start("final", i, "final", i, 1, outer)
            start("final", i, "final", i, 1, other)
            finish(i)

        def forward(p):
            i = 2 * p + 1 - w
            arrived("final", i)
            start("final", i, "final", i, 1, outer)
            finish(i)

        for p in range(PAIRS + 2 * LAG):
            if p < PAIRS:
                for i in range(2 * p + AHEAD, min(2 * p + AHEAD + 2, FLOWS)):
                    give(i)
                relay(p)
            if LAG <= p < PAIRS + LAG:
                collect(p - LAG)
            if p >= 2 * LAG:
                forward(p - 2 * LAG)
            if p == PAIRS // 2 + 2 * LAG:
                correlate(2 * x, 0)


    correlate(2 * x + 1, 0)
    for n in range(2):
        for i in range(n * FLOWS // 2, (n + 1) * FLOWS // 2):
            arrived("last", i)
            out_ref[chunk_rows(1 - x, i), :] = get("last", i)
        correlate(2 * (1 - x) + n, 0)

    def q_over(b):
        return remote(basis.at[0, b], basis.at[1, b], q_out, q_in.at[0, b], over)

    def q_twin(b):
        return remote(basis.at[0, b], basis.at[2, b], q_out, q_in.at[1, b], twin)

    def q_cross(b):
        return remote(basis.at[1, b], basis.at[3, b], q_out, q_in.at[2, b], twin)

    def half_of(which):
        return pl.ds(pl.multiple_of(which * (states // 2), states // 2), states // 2)

    def q_half(b, ref, which, i, device):
        some = half_of(which)
        return remote(basis.at[ref, b, some], basis.at[1, b, some], q_out, q_in.at[i, b], device)

    def pass_half(b):
        q_half(b, 0, x, 0, over).wait_recv()
        q_half(b, 1, x, 3, side).start()

    def pass_on(b):
        q_half(b, 1, 1 - x, 3, side).wait_recv()
        q_cross(b).start()

    def update(b, i):
        below = pl.ds(pl.multiple_of(i * span, span), span)

        def part(n, deeper):
            wide = pl.ds(pl.multiple_of(n * 2 * span, 2 * span), 2 * span)
            work[below, wide] = work[below, wide] - contract(near_terms[:, below], far_terms[:, wide], 0, 0)
            return deeper

        lax.fori_loop(i // 2, blocks_count // 2, part, 0)

    def factor_step(b, carry):
        lanes = pl.ds(pl.multiple_of(b * span, span), span)
        inverse = inverse_ref[...]
        panel = contract(left_terms(inverse, 1), right_terms(work[lanes, :], 0), 1, 0)
        inverse_terms = right_terms(inverse, 1, 2)
        panel_ref[...] = right_terms(panel, 0, 2)
        near_terms[...] = left_terms(panel, 0)
        far_terms[...] = right_terms(panel, 0)

        def orthogonal(n, inner):
            some = pl.ds(pl.multiple_of(n * tall, tall), tall)
            columns = contract(left_terms(out_ref[some, lanes], 1, 2), inverse_terms, 1, 1)
            basis_full[some, :] = columns
            whole = columns.astype(jnp.bfloat16)
            basis[0, b, some, :] = whole
            basis_mid[some, :] = (columns - whole.astype(jnp.float32)).astype(jnp.bfloat16)
            return inner

        lax.fori_loop(0, 4, orthogonal, 0)
        @pl.when(b + 1 < blocks_count)
        def _():
            q_half(b, 0, x, 0, over).start()

        @pl.when(b + 1 == blocks_count)
        def _():
            q_over(b).start()

        q_twin(b).start()
        height = tile_ref.shape[0]
        mine = pl.ds(pl.multiple_of(op * height, height), height)
        tile_ref[:, lanes] = basis_full[mine, :] * float(states) ** 0.5

        @pl.when(b + 1 < blocks_count)
        def _():
            update(b, b + 1)

            def spread_out(m, n):
                some = pl.ds(m * tall, tall)
                wide = pl.ds(n * 2 * span, 2 * span)
                whole = basis[0, b, some, :]
                terms = jnp.concatenate([whole, whole, basis_mid[some, :]], axis=1)
                out_ref[some, wide] = out_ref[some, wide] - contract(terms, panel_ref[:, wide], 1, 0)

            following = pl.ds(pl.multiple_of((b + 1) * span, span), span)
            beside = [functools.partial(spread_out, m, n) for n in range(kept // (2 * span)) for m in range(4)]

            def late_update(ahead):
                valid = jnp.where(b + ahead < blocks_count, 1.0, 0.0).astype(jnp.float32)
                below = pl.ds(pl.multiple_of(jnp.minimum(b + ahead, blocks_count - 1) * span, span), span)
                wide = pl.ds(kept // 2, kept // 2)
                work[below, wide] = work[below, wide] - valid * contract(
                    near_terms[:, below], far_terms[:, wide], 0, 0
                )

            beside += [functools.partial(late_update, ahead) for ahead in range(2, blocks_count)]
            inverse_ref[...] = eliminate_pairs(work[following, following], beside)

        @pl.when(b > 0)
        def _():
            pass_half(b - 1)

        @pl.when((b > 1) & (b + 1 < blocks_count))
        def _():
            pass_on(b - 2)

        return carry

    inverse_ref[...] = eliminate_pairs(work[pl.ds(0, span), pl.ds(0, span)])
    lax.fori_loop(0, blocks_count, factor_step, 0)

    def rotate(b):
        q_twin(b).wait_recv()
        q_cross(b).wait_recv()
        value = basis[0, b]
        for n, sector in enumerate((sec_over, sec_twin, sec_cross)):
            value = jnp.where(wanted == sector, basis[n + 1, b], value)
        rotated_ref[pl.ds(b * span, span), :] = contract(value, mapped[...], 0, 0)

    def apply(n, carry):
        some = pl.ds(pl.multiple_of(n * tall, tall), tall)
        columns = jnp.concatenate([basis[0, b] for b in range(blocks_count)], axis=1)
        mapped[some, :] = contract(blocks[some, :], columns, 1, 0).astype(jnp.bfloat16)
        return carry

    lax.fori_loop(0, 4, apply, 0)
    pass_on(blocks_count - 3)
    for b in range(blocks_count - 2):
        rotate(b)
    pass_on(blocks_count - 2)
    q_over(blocks_count - 1).wait_recv()
    q_cross(blocks_count - 1).start()
    rotate(blocks_count - 2)
    rotate(blocks_count - 1)

    def sent(ref, sem):
        remote(ref, ref, sem, x_in.at[0], side).wait_send()

    sent(basis.at[pl.ds(0, 3)], q_out)
    sent(store, fetch_out.at[1])
    for n, bufs in enumerate((levels, scales)):
        sent(bufs["inner"], departures.at[0, n])

    @pl.when(mid)
    def _():
        sent(store.at[pl.ds(0, PARTS + WAVES)], fetch_out.at[0])
        for n, bufs in enumerate((levels, scales)):
            sent(bufs["inner"], departures.at[1, n])

    @pl.when(leaf)
    def _():
        sent(store.at[pl.ds(0, PARTS)], fetch_out.at[0])
        for n, bufs in enumerate((levels, scales)):
            sent(bufs["inner"].at[pl.ds(0, FLOWS)], departures.at[1, n])


def publish_kernel(tile_ref, rotated_ref, tile_out, rotated_out, done):
    copies = [
        pltpu.make_async_copy(source, target, done.at[i])
        for i, (source, target) in enumerate(((tile_ref, tile_out), (rotated_ref, rotated_out)))
    ]
    for copy in copies:
        copy.start()
    for copy in copies:
        copy.wait()


def publish(tile, rotated):
    return pl.pallas_call(
        publish_kernel,
        out_shape=tuple(jax.ShapeDtypeStruct(a.shape, a.dtype) for a in (tile, rotated)),
        in_specs=[pl.BlockSpec(memory_space=pltpu.VMEM)] * 2,
        out_specs=(pl.BlockSpec(memory_space=pl.ANY),) * 2,
        scratch_shapes=[pltpu.SemaphoreType.DMA((2,))],
        compiler_params=pltpu.CompilerParams(vmem_limit_bytes=2 * 1024 * 1024),
        name="publish",
    )(tile, rotated)


def whole_kernel(own, blocks, guess, sizes, counts, target_map, top, bottom):
    rows, states = own.shape
    kept = guess.shape[1]
    chunk = states // (2 * FLOWS)
    lengths = (FLOWS, FLOWS, FLOWS, 2 * FLOWS, FLOWS, FLOWS)
    sem = pltpu.SemaphoreType.DMA
    half = own.dtype
    total = 2 * DEPTH * rows
    pieces = kept // LANES
    scratch = [
        pltpu.VMEM((16 * PARTS, rows // PARTS, states), half),
        pltpu.VMEM((WAVES, rows // PARTS, states), half),
        pltpu.VMEM((WAVES, rows // PARTS, states), half),
        pltpu.VMEM((total, states), half),
        pltpu.VMEM((states, states), half),
        pltpu.VMEM((states, kept), half),
        pltpu.VMEM((total + rows, states), half),
        pltpu.VMEM((total + rows, kept), half),
        pltpu.VMEM((total + rows, kept), half),
    ]
    scratch += [sem((WAVES,))] * 4 + [sem((2,)), sem((8,))]
    scratch += [pltpu.VMEM((n, chunk, kept), jnp.int16) for n in lengths]
    scratch += [pltpu.VMEM((n, 1, kept), jnp.float32) for n in lengths]
    scratch += [sem((n,)) for n in (FLOWS, FLOWS, FLOWS, FLOWS)]
    scratch += [sem((2, 2)), pltpu.VMEM((2, 1, chunk * kept // 2 + kept), jnp.float32), pltpu.VMEM((states, kept), jnp.float32)]
    scratch += [pltpu.SMEM(a.shape, jnp.int32) for a in (sizes, counts, target_map, top, bottom)]
    scratch += [
        pltpu.VMEM((rows, states), half),
        pltpu.VMEM((states, kept), jnp.float32),
        pltpu.VMEM((kept, kept), jnp.float32),
        pltpu.VMEM((6 * LANES, kept), half),
        pltpu.VMEM((6 * LANES, kept), half),
        pltpu.VMEM((4, pieces, states, LANES), half),
        pltpu.VMEM((states, LANES), half),
        pltpu.VMEM((states, LANES), jnp.float32),
        pltpu.VMEM((states, kept), half),
        pltpu.VMEM((3 * LANES, kept), half),
        pltpu.VMEM((LANES, LANES), jnp.float32),
        sem((4, pieces)),
        sem,
    ]
    return pl.pallas_call(
        image_kernel,
        out_shape=(
            pltpu.VMEM((states // lax.axis_size("op"), kept), jnp.float32),
            pltpu.VMEM((kept, kept), jnp.float32),
        ),
        in_specs=[pl.BlockSpec(memory_space=pltpu.HBM)] * 8,
        out_specs=[pl.BlockSpec(memory_space=pltpu.VMEM)] * 2,
        scratch_shapes=scratch,
        compiler_params=pltpu.CompilerParams(
            collective_id=1, has_side_effects=True, vmem_limit_bytes=60 * 1024 * 1024
        ),
        name="truncate_and_rotate",
    )(sizes, counts, target_map, top, bottom, own, blocks, guess)


def body(
    wavefunction,
    op_blocks,
    basis_guess,
    sector_sizes,
    kept_counts,
    target_map,
    noise_numerator,
    noise_denominator,
):
    if lax.axis_size("op") == 2 * DEPTH and lax.axis_size("sec") == 4:
        tile, rotated = whole_kernel(
            wavefunction[0],
            op_blocks[0, 0],
            basis_guess[0],
            sector_sizes,
            kept_counts,
            target_map.T,
            noise_numerator,
            noise_denominator,
        )
        tile, rotated = publish(tile, rotated)
        return (tile[None], rotated[None, None])
    state_count = wavefunction.shape[2]
    kept_width = basis_guess.shape[2]
    tile_rows = state_count // lax.axis_size("op")
    sec_index = lax.axis_index("sec")
    op_index = lax.axis_index("op")
    noise_weight = noise_numerator[0].astype(jnp.float32) / noise_denominator[0].astype(jnp.float32)
    sources = source_sectors(target_map)
    wanted_all = lax.dynamic_index_in_dim(sources, sec_index, 1, keepdims=False)[None, :]
    wanted = lax.dynamic_index_in_dim(wanted_all[0], op_index, 0, keepdims=False)
    states = jnp.arange(state_count, dtype=jnp.int32)
    own_size = lax.dynamic_index_in_dim(sector_sizes, sec_index, 0, keepdims=False)
    source_size = lax.dynamic_index_in_dim(sector_sizes, wanted, 0, keepdims=False)
    own_count = lax.dynamic_index_in_dim(kept_counts, sec_index, 0, keepdims=False)
    own_kept = jnp.arange(kept_width, dtype=jnp.int32) < own_count
    zero_half = jnp.zeros((), jnp.bfloat16)
    own_rows = jnp.where((states < own_size)[None, :], wavefunction[0], zero_half)
    moved = fetch_pieces(wavefunction, wanted_all)[0]
    moved = jnp.where((states < source_size)[None, :], moved, zero_half)
    blocks = op_blocks[0, 0]
    perturbed = jnp.dot(moved, blocks, preferred_element_type=jnp.float32).astype(jnp.bfloat16)
    guess = jnp.where((states < own_size)[:, None], basis_guess[0], zero_half)
    perturbed_guess = noise_weight * jnp.dot(perturbed, guess, preferred_element_type=jnp.float32)
    own_guess = jnp.dot(own_rows, guess, preferred_element_type=jnp.float32)
    part = lax.dot_general(
        jnp.concatenate([perturbed, own_rows], axis=0).astype(jnp.float32),
        jnp.concatenate([perturbed_guess, own_guess], axis=0),
        (((0,), (0,)), ((), ())),
        precision=lax.Precision.HIGH,
    )
    part = jnp.where((states < own_size)[:, None] & own_kept[None, :], part, jnp.float32(0.0))
    full_image = sum_over_op(part)
    padding = jnp.where(own_kept, jnp.float32(0.0), jnp.float32(1.0))
    correlation = dot_ta(full_image, full_image) + padding[:, None] * jnp.eye(
        kept_width, dtype=jnp.float32
    )
    inverse = inverse_factor(correlation)
    new_basis = lax.dot_general(
        full_image, inverse, (((1,), (1,)), ((), ())), precision=lax.Precision.HIGH
    )
    kept_tile = (
        lax.dynamic_slice_in_dim(new_basis, op_index * tile_rows, tile_rows, 0)
        * float(state_count) ** 0.5
    )
    basis_half = new_basis.astype(jnp.bfloat16)
    mapped = jnp.dot(blocks, basis_half, preferred_element_type=jnp.float32).astype(jnp.bfloat16)
    source_basis = fetch_sector(basis_half, wanted)
    rotated = lax.dot_general(
        source_basis, mapped, (((0,), (0,)), ((), ())), preferred_element_type=jnp.float32
    )
    return (kept_tile[None], rotated[None, None])


def solution(mesh):
    placed = (
        P("sec", "op", None),
        P("op", "sec", None, None),
        P("sec", None, None),
        P(),
        P(),
        P(),
        P(),
        P(),
    )
    return jax.shard_map(
        body,
        mesh=mesh,
        in_specs=placed,
        out_specs=(P("sec", "op", None), P("op", "sec", None, None)),
        check_vma=False,
    )
```
